32 devices in a mesh: batch: 2 (over x), w: 4 (over z), h: 4 (over y, core).
Axes of the slice: x: 2, y: 2, z: 4, core: 2. Of those that a mesh axis runs over, the one named last changes fastest.
Arguments:
- images: bfloat16 [32, 1024, 512, 4], P('batch', 'h', 'w'), parts along dimension 0
- down_w1: bfloat16 [3, 3, 4, 32], replicated
- down_b1: float32 [32], replicated
- refine_w1: bfloat16 [3, 3, 32, 32], replicated
- refine_b1: float32 [32], replicated
- down_w2: bfloat16 [3, 3, 32, 64], replicated
- down_b2: float32 [64], replicated
- refine_w2: bfloat16 [3, 3, 64, 64], replicated
- refine_b2: float32 [64], replicated
- down_w3: bfloat16 [3, 3, 64, 128], replicated
- down_b3: float32 [128], replicated
- refine_w3: bfloat16 [3, 3, 128, 128], replicated
- refine_b3: float32 [128], replicated
Outputs:
- output: bfloat16 [32, 128, 64, 128], P('batch', 'h', 'w'), parts along dimension 0
There are 2 independent parts. The reference program is written for one: setup_inputs(seed, part) draws one part's arguments, and reference() takes and returns one part's arrays. A program takes and returns all parts, laid end to end along the dimension named above; an argument that names none is the same for every part.
All inputs are finite; a program needn't handle non-finite values.
Results may differ from the reference program's by a relative error of at most 0.00187565.
Values are sent between devices in bfloat16 or wider.
A program may use at most 1 GiB of HBM per device.

```python
import jax
import jax.numpy as jnp
from jax import lax

BATCH = 16
IMG_H = 1024
IMG_W = 512
CIN = 4
WIDTH = 32

DIM_NUMS = ('NHWC', 'HWIO', 'NHWC')


def conv_weight(rng_key, chan_in, chan_out):
    weight_scale = (2.0 / (9 * chan_in)) ** 0.5
    raw_draw = jax.random.normal(rng_key, (3, 3, chan_in, chan_out), jnp.float32)
    return (raw_draw * weight_scale).astype(jnp.bfloat16)


def setup_inputs(seed: int = 0, part: int = 0) -> dict:
    image_key = jax.random.fold_in(jax.random.key(seed), part)
    key_list = jax.random.split(jax.random.key(seed + 1), 12)
    widths = [CIN, WIDTH, 2 * WIDTH, 4 * WIDTH]
    images = jax.random.normal(image_key, (BATCH, IMG_H, IMG_W, CIN), jnp.float32)
    arrays = {'images': images.astype(jnp.bfloat16)}
    for stage_num in range(3):
        chan_in = widths[stage_num]
        chan_out = widths[stage_num + 1]
        suffix = str(stage_num + 1)
        arrays['down_w' + suffix] = conv_weight(key_list[4 * stage_num], chan_in, chan_out)
        arrays['down_b' + suffix] = 0.3 * jax.random.normal(key_list[4 * stage_num + 1], (chan_out,), jnp.float32)
        arrays['refine_w' + suffix] = conv_weight(key_list[4 * stage_num + 2], chan_out, chan_out)
        arrays['refine_b' + suffix] = 0.3 * jax.random.normal(key_list[4 * stage_num + 3], (chan_out,), jnp.float32)
    return arrays


def periodic_conv(current, weight, bias_vec, stride):
    padded = jnp.pad(current, ((1, 1), (1, 1), (0, 0)), mode='wrap')
    conv_out = lax.conv_general_dilated(padded[None].astype(jnp.float32), weight.astype(jnp.float32), (stride, stride), 'VALID', dimension_numbers=DIM_NUMS)
    return jnp.maximum(conv_out[0] + bias_vec, 0.0).astype(jnp.bfloat16)


def reference(images, down_w1, down_b1, refine_w1, refine_b1, down_w2, down_b2, refine_w2, refine_b2, down_w3, down_b3, refine_w3, refine_b3):
    stages = [(down_w1, down_b1, refine_w1, refine_b1), (down_w2, down_b2, refine_w2, refine_b2), (down_w3, down_b3, refine_w3, refine_b3)]

    def encode_image(one_image):
        current = one_image
        for down_w, down_b, refine_w, refine_b in stages:
            current = periodic_conv(current, down_w, down_b, 2)
            current = periodic_conv(current, refine_w, refine_b, 1)
        return current

    return lax.map(encode_image, images)
```

```python
import functools

import jax
import jax.numpy as jnp
import numpy as np
from jax import lax
from jax.experimental import pallas as pl
from jax.experimental.pallas import tpu as pltpu
from jax.sharding import PartitionSpec as P

BF = jnp.bfloat16
F32 = jnp.float32
N = 16
G = 16
MESH = pl.DeviceIdType.MESH


def first_weight_selector():
    sel = np.zeros((8, 256, 36), np.float32)
    for j in range(8):
        for c in range(4):
            for wi in range(16):
                b = wi - 2 * j + 1
                if 0 <= b <= 2:
                    for hi in range(2):
                        sel[j, hi * 64 + c * 16 + wi, ((hi + 1) * 3 + b) * 4 + c] = 1
                    sel[j, 128 + 64 + c * 16 + wi, (0 * 3 + b) * 4 + c] = 1
            if j == 0:
                for a, wi in ((1, 15), (2, 14), (0, 13)):
                    sel[j, 128 + c * 16 + wi, (a * 3) * 4 + c] = 1
    return sel.reshape(8 * 256, 36)


def roll(v, shift):
    shift %= 128
    return v if shift == 0 else pltpu.roll(v, shift, v.ndim - 1)


def flat(v):
    return v.reshape(-1, 128)


def build_weight(big, w, k_blocks, stride):
    cin, cout = w.shape[2], w.shape[3]
    ncols = 128 // cout
    zero = jnp.zeros((cin, cout), BF)
    for kp, pos in enumerate(k_blocks):
        for orow in range(2):
            pieces = []
            for j in range(ncols):
                piece = zero
                if pos is not None:
                    a, b = pos[0] - stride * orow, pos[1] - stride * j + 1
                    if 0 <= a <= 2 and 0 <= b <= 2:
                        piece = w[a, b]
                pieces.append(piece)
            big[kp * cin:(kp + 1) * cin, orow * 128:(orow + 1) * 128] = (
                pieces[0] if ncols == 1 else jnp.concatenate(pieces, axis=1))


REFINE1_K = ([(ir, ic) for ir in range(4) for ic in range(4)]
             + [p for e in (0, 2) for p in ((e, 4), (e + 1, -1), (e + 1, 4), (e, -1))])
REFINE2_K = ([(ir, ic) for ir in range(4) for ic in range(2)]
             + [p for ir in range(4) for p in ((ir, 2), (ir, -1))])
REFINE3_K = [(ir, ic) for ir in range(4) for ic in (-1, 0, 1)]
DOWN2_K = ([(ir, ic) for ir in range(5) for ic in range(4)]
           + [p for e in (0, 2) for p in (None, (e + 1, -1), None, (e, -1))]
           + [None, None, None, (4, -1)])
DOWN3_K = ([(ir, ic) for ir in range(5) for ic in range(2)]
           + [p for e in (0, 2) for p in ((e + 1, -1), (e, -1))] + [None, (4, -1)])


def tiled_bias(b):
    reps = 128 // b.shape[1]
    return jnp.concatenate([b[...]] * (2 * reps), axis=1)


def emit(res, bias, dst, row0, pairs, g0, ng):
    val = jnp.maximum(res + bias, 0.0).astype(BF).reshape(pairs, ng, N, 256)
    for p in range(pairs):
        for half in range(2):
            dst(row0 + 2 * p + half, g0, ng, val[p, :, :, half * 128:(half + 1) * 128])


def refine_lhs(stage, src, row0, g0, ng):
    def own(h):
        return flat(src[row0 + h, pl.ds(1 + g0, ng)])

    def left(h):
        return flat(src[row0 + h, pl.ds(g0, ng)])

    def right(h):
        return flat(src[row0 + h, pl.ds(2 + g0, ng)])

    def edge(h):
        return jnp.concatenate([right(h)[:, :64], left(h)[:, 64:]], axis=1)

    if stage == 3:
        return [f(h) for h in range(4) for f in (left, own, right)]
    if stage == 2:
        return [own(h) for h in range(4)] + [edge(h) for h in range(4)]
    ks = [own(h) for h in range(4)]
    for h in (0, 2):
        f0, f1 = edge(h), roll(edge(h + 1), 64)
        ks.append(jnp.concatenate([f0[:, :32], f1[:, 32:96], f0[:, 96:]], axis=1))
    return ks


def down_lhs(src, row0, g0, ng):
    def own(h):
        return flat(src[2 * row0 + h, pl.ds(1 + g0, ng)])

    def left(h):
        return flat(src[2 * row0 + h, pl.ds(g0, ng)])

    ks = [own(h) for h in range(5)]
    for h in (0, 2):
        ks.append(jnp.concatenate([roll(left(h + 1), 64)[:, :64], left(h)[:, 64:]], axis=1))
    return ks + [left(4)]


def conv_rows(lhs, weight, bias, dst, row_lo, row_hi, g0, ng, pairs):
    steps = (row_hi - row_lo) // (2 * pairs)

    def step(i, carry):
        row0 = row_lo + i * (2 * pairs)
        per_pair = [lhs(row0 + 2 * p, g0, ng) for p in range(pairs)]
        ks = [jnp.concatenate(part, axis=0) if pairs > 1 else part[0] for part in zip(*per_pair)]
        res = jnp.dot(jnp.concatenate(ks, axis=1), weight[...], preferred_element_type=F32)
        emit(res, bias, dst, row0, pairs, g0, ng)
        return carry

    lax.fori_loop(0, steps, step, 0)


def pack_cols(stage, buf, rows, right_edge):
    col = buf[pl.ds(1, rows), G if right_edge else 1]
    per = 4 if stage == 1 else 2
    width = 128 // per
    col = col.reshape(rows // per, per, N, 128)
    base = 128 - width if right_edge else 0
    parts = []
    for k in range(per):
        v = roll(flat(col[:, k]), k * width - base)
        parts.append(v[:, k * width:(k + 1) * width])
    return jnp.concatenate(parts, axis=1).reshape(rows // per, N, 128)


def unpack_cols(stage, buf, rows, packed, left_halo):
    per = 4 if stage == 1 else 2
    width = 128 // per
    base = 128 - width if left_halo else 0
    g = 0 if left_halo else G + 1
    for k in range(per):
        v = roll(flat(packed[...]), base - k * width).reshape(rows // per, N, 128)
        for i in range(rows // per):
            buf[1 + i * per + k, g] = v[i]


def kernel(h_count, w_count, rows1, x, sel, dw1, db1, rw1, rb1, dw2, db2, rw2, rb2, dw3, db3, rw3, rb3, out,
           pv, y1, z1, y2, z2, y3, bw1, br1, bw2, br2, bw3, br3,
           send_x, recv_x, send_c, recv_c, send_sem, recv_sem):
    rows2, rows3 = rows1 // 2, rows1 // 4
    me_h, me_w = lax.axis_index('h'), lax.axis_index('w')

    def device(dh, dw):
        return {'h': lax.rem(me_h + dh + h_count, h_count), 'w': lax.rem(me_w + dw + w_count, w_count)}

    barrier = pltpu.get_barrier_semaphore()
    others = [(dh, dw) for dh in (-1, 0, 1) for dw in (-1, 0, 1) if dh or dw]
    for dh, dw in others:
        pl.semaphore_signal(barrier, inc=1, device_id=device(dh, dw), device_id_type=MESH)

    def copies(e, buf, rows, ng, both, send_col, recv_col):
        last = rows
        table = [
            (buf.at[last, pl.ds(1, ng)], buf.at[0, pl.ds(1, ng)], (1, 0)),
            (send_col[0], recv_col[0], (0, 1)),
            (buf.at[last, ng], buf.at[0, 0], (1, 1)),
        ]
        if both:
            table += [
                (buf.at[1, pl.ds(1, ng)], buf.at[last + 1, pl.ds(1, ng)], (-1, 0)),
                (send_col[1], recv_col[1], (0, -1)),
                (buf.at[last, 1], buf.at[0, ng + 1], (1, -1)),
                (buf.at[1, ng], buf.at[last + 1, 0], (-1, 1)),
                (buf.at[1, 1], buf.at[last + 1, ng + 1], (-1, -1)),
            ]
        return [
            pltpu.make_async_remote_copy(
                src_ref=src, dst_ref=dst, send_sem=send_sem.at[e, d], recv_sem=recv_sem.at[e, d],
                device_id=device(*direction), device_id_type=MESH)
            for d, (src, dst, direction) in enumerate(table)
        ]

    def exchange(e, stage, buf, rows, both):
        if stage == 3:
            send_col = [buf.at[pl.ds(1, rows), G], buf.at[pl.ds(1, rows), 1]]
            recv_col = [buf.at[pl.ds(1, rows), 0], buf.at[pl.ds(1, rows), G + 1]]
        else:
            send_col = [send_c.at[e, 0], send_c.at[e, 1]]
            recv_col = [recv_c.at[e, 0], recv_c.at[e, 1]]
            send_c[e, 0] = pack_cols(stage, buf, rows, True)
            if both:
                send_c[e, 1] = pack_cols(stage, buf, rows, False)
        todo = copies(e, buf, rows, G, both, send_col, recv_col)
        for c in todo:
            c.start()
        for c in todo:
            c.wait()
        if stage != 3:
            unpack_cols(stage, buf, rows, recv_c.at[e, 0], True)
            if both:
                unpack_cols(stage, buf, rows, recv_c.at[e, 1], False)

    picked = jnp.dot(sel[...], dw1[...], preferred_element_type=F32).astype(BF)
    bw1[...] = jnp.concatenate([picked[j * 256:(j + 1) * 256] for j in range(8)], axis=1)
    build_weight(br1, rw1, REFINE1_K, 1)
    build_weight(bw2, dw2, DOWN2_K, 2)
    build_weight(br2, rw2, REFINE2_K, 1)
    build_weight(bw3, dw3, DOWN3_K, 2)
    build_weight(br3, rw3, REFINE3_K, 1)

    lane = lax.broadcasted_iota(jnp.int16, (N, 128), 1)

    def swap(v, dist, blocks):
        mask = (lane & dist) == 0
        new = list(v)
        for i in range(8):
            if not i & blocks:
                a, b = v[i], v[i + blocks]
                new[i] = jnp.where(mask, a, roll(b, dist))
                new[i + blocks] = jnp.where(mask, roll(a, -dist), b)
        return new

    def to_pairs(i, carry):
        t = jnp.transpose(x[:, pl.ds(i * 16, 16), :], (1, 0, 2))
        for p in range(2):
            v = [t[p * 8 + k] for k in range(8)]
            for dist, blocks in ((64, 4), (32, 2), (16, 1)):
                v = swap(v, dist, blocks)
            for q in range(8):
                pv[1 + 2 * i + p, 1 + q] = v[q]
        return carry

    lax.fori_loop(0, rows1 // 2, to_pairs, 0)

    pl.semaphore_wait(barrier, len(others))

    lanes = lax.broadcasted_iota(jnp.int16, (rows1, 128), 1) & 15
    col = pv[pl.ds(1, rows1), 8].reshape(rows1 // 16, 16, N, 128)
    packed = flat(col[:, 15])
    for k in range(15):
        packed = jnp.where(lanes == k, roll(flat(col[:, k]), k - 15), packed)
    send_x[...] = packed.reshape(rows1 // 16, N, 128)
    todo = copies(0, pv, rows1, 8, False, [send_x], [recv_x])
    for c in todo:
        c.start()
    for c in todo:
        c.wait()
    for k in range(16):
        v = roll(flat(recv_x[...]), 15 - k).reshape(rows1 // 16, N, 128)
        for i in range(rows1 // 16):
            pv[1 + 16 * i + k, 0] = v[i]

    bias1 = tiled_bias(db1)
    per = 4

    def down1(i, carry):
        row0 = i * per
        size = per * 8 * N
        sub = lax.broadcasted_iota(jnp.int16, (size, 128), 1) & 15
        own = flat(pv[pl.ds(row0 + 1, per), pl.ds(1, 8)])
        above = flat(pv[pl.ds(row0, per), pl.ds(1, 8)])
        left = flat(pv[pl.ds(row0 + 1, per), pl.ds(0, 8)])
        above_left = flat(pv[pl.ds(row0, per), pl.ds(0, 8)])
        edge = jnp.where(sub == 15, left, jnp.where(sub == 14, roll(left, 63), roll(above_left, 62)))
        second = jnp.concatenate([edge[:, :64], above[:, 64:]], axis=1)
        res = jnp.dot(jnp.concatenate([own, second], axis=1), bw1[...], preferred_element_type=F32)
        val = jnp.maximum(res + bias1, 0.0).astype(BF).reshape(per, 8, N, 256)
        for r in range(per):
            for q in range(8):
                y1[row0 + 1 + r, 1 + 2 * q] = val[r, q, :, :128]
                y1[row0 + 1 + r, 2 + 2 * q] = val[r, q, :, 128:]
        return carry

    lax.fori_loop(0, rows1 // per, down1, 0)

    def into(buf):
        def dst(row, g0, ng, val):
            buf[row + 1, pl.ds(1 + g0, ng)] = val
        return dst

    def into_out(row, g0, ng, val):
        out[row, pl.ds(g0, ng)] = val

    exchange(1, 1, y1, rows1, True)
    conv_rows(functools.partial(refine_lhs, 1, y1), br1, tiled_bias(rb1), into(z1), 0, rows1, 0, G, 2)
    exchange(2, 1, z1, rows1, False)
    conv_rows(functools.partial(down_lhs, z1), bw2, tiled_bias(db2), into(y2), 0, rows2, 0, G, 2)
    exchange(3, 2, y2, rows2, True)
    conv_rows(functools.partial(refine_lhs, 2, y2), br2, tiled_bias(rb2), into(z2), 0, rows2, 0, G, 2)
    exchange(4, 2, z2, rows2, False)
    conv_rows(functools.partial(down_lhs, z2), bw3, tiled_bias(db3), into(y3), 0, rows3, 0, G, 2)
    exchange(5, 3, y3, rows3, True)
    conv_rows(functools.partial(refine_lhs, 3, y3), br3, tiled_bias(rb3), into_out, 0, rows3, 0, G, 2)


def encode(h_count, w_count, images, *params):
    rows1 = images.shape[1] // 2
    rows2, rows3 = rows1 // 2, rows1 // 4
    x = jnp.transpose(images, (0, 1, 3, 2)).reshape(N, rows1 * 8, 128)
    args = [x, jnp.asarray(first_weight_selector(), BF)]
    for i, p in enumerate(params):
        args.append(p.reshape(1, -1) if i % 2 else (p.reshape(36, 32) if i == 0 else p))

    def act(rows, groups):
        return pltpu.VMEM((rows, groups, N, 128), BF)

    flops = 2 * 16 * rows1 * 64 * 32 * 9 * (4 + 32 + 16 + 32 + 16 + 32)
    out = pl.pallas_call(
        functools.partial(kernel, h_count, w_count, rows1),
        name='encoder',
        out_shape=jax.ShapeDtypeStruct((rows3, G, N, 128), BF),
        in_specs=[pl.BlockSpec(memory_space=pltpu.VMEM)] * len(args),
        out_specs=pl.BlockSpec(memory_space=pltpu.VMEM),
        scratch_shapes=[
            act(rows1 + 1, 9), act(rows1 + 2, G + 2), act(rows1 + 1, G + 1),
            act(rows2 + 2, G + 2), act(rows2 + 1, G + 1), act(rows3 + 2, G + 2),
            pltpu.VMEM((256, 256), BF), pltpu.VMEM((768, 256), BF), pltpu.VMEM((1024, 256), BF),
            pltpu.VMEM((1024, 256), BF), pltpu.VMEM((1024, 256), BF), pltpu.VMEM((1536, 256), BF),
            pltpu.VMEM((rows1 // 16, N, 128), BF), pltpu.VMEM((rows1 // 16, N, 128), BF),
            pltpu.VMEM((5, 2, rows1 // 4, N, 128), BF), pltpu.VMEM((5, 2, rows1 // 4, N, 128), BF),
            pltpu.SemaphoreType.DMA((6, 8)), pltpu.SemaphoreType.DMA((6, 8)),
        ],
        compiler_params=pltpu.CompilerParams(
            collective_id=0, has_side_effects=True, vmem_limit_bytes=67043328),
        cost_estimate=pl.CostEstimate(flops=flops, bytes_accessed=7 * 2**20, transcendentals=0),
    )(*args)
    return jnp.transpose(out, (2, 0, 1, 3))


def solution(mesh):
    tile_spec = P('batch', 'h', 'w', None)
    body = functools.partial(encode, mesh.shape['h'], mesh.shape['w'])
    return jax.shard_map(body, mesh=mesh, in_specs=(tile_spec,) + (P(),) * 12, out_specs=tile_spec, check_vma=False)
```

```python
import functools

import jax
import jax.numpy as jnp
import numpy as np
from jax import lax
from jax.experimental import pallas as pl
from jax.experimental.pallas import tpu as pltpu
from jax.sharding import PartitionSpec as P

BF = jnp.bfloat16
F32 = jnp.float32
N = 16
G = 16
MESH = pl.DeviceIdType.MESH


def first_weight_selector():
    sel = np.zeros((8, 256, 36), np.float32)
    for j in range(8):
        for c in range(4):
            for wi in range(16):
                b = wi - 2 * j + 1
                if 0 <= b <= 2:
                    for hi in range(2):
                        sel[j, hi * 64 + c * 16 + wi, ((hi + 1) * 3 + b) * 4 + c] = 1
                    sel[j, 128 + 64 + c * 16 + wi, (0 * 3 + b) * 4 + c] = 1
            if j == 0:
                for a, wi in ((1, 15), (2, 14), (0, 13)):
                    sel[j, 128 + c * 16 + wi, (a * 3) * 4 + c] = 1
    return sel.reshape(8 * 256, 36)


def roll(v, shift):
    shift %= 128
    return v if shift == 0 else pltpu.roll(v, shift, v.ndim - 1)


def flat(v):
    return v.reshape(-1, 128)


def build_weight(big, w, k_blocks, stride):
    cin, cout = w.shape[2], w.shape[3]
    ncols = 128 // cout
    zero = jnp.zeros((cin, cout), BF)
    for kp, pos in enumerate(k_blocks):
        for orow in range(2):
            pieces = []
            for j in range(ncols):
                piece = zero
                if pos is not None:
                    a, b = pos[0] - stride * orow, pos[1] - stride * j + 1
                    if 0 <= a <= 2 and 0 <= b <= 2:
                        piece = w[a, b]
                pieces.append(piece)
            big[kp * cin:(kp + 1) * cin, orow * 128:(orow + 1) * 128] = (
                pieces[0] if ncols == 1 else jnp.concatenate(pieces, axis=1))


REFINE1_K = ([(ir, ic) for ir in range(4) for ic in range(4)]
             + [p for e in (0, 2) for p in ((e, 4), (e + 1, -1), (e + 1, 4), (e, -1))])
REFINE2_K = ([(ir, ic) for ir in range(4) for ic in range(2)]
             + [p for ir in range(4) for p in ((ir, 2), (ir, -1))])
REFINE3_K = [(ir, ic) for ir in range(4) for ic in (-1, 0, 1)]
DOWN2_K = ([(ir, ic) for ir in range(5) for ic in range(4)]
           + [p for e in (0, 2) for p in (None, (e + 1, -1), None, (e, -1))]
           + [None, None, None, (4, -1)])
DOWN3_K = ([(ir, ic) for ir in range(5) for ic in range(2)]
           + [p for e in (0, 2) for p in ((e + 1, -1), (e, -1))] + [None, (4, -1)])


def tiled_bias(b):
    reps = 128 // b.shape[1]
    return jnp.concatenate([b[...]] * (2 * reps), axis=1)


def emit(res, bias, dst, row0, pairs, g0, ng):
    val = jnp.maximum(res + bias, 0.0).astype(BF).reshape(pairs, ng, N, 256)
    for p in range(pairs):
        for half in range(2):
            dst(row0 + 2 * p + half, g0, ng, val[p, :, :, half * 128:(half + 1) * 128])


def refine_lhs(stage, src, row0, g0, ng):
    def own(h):
        return flat(src[row0 + h, pl.ds(1 + g0, ng)])

    def left(h):
        return flat(src[row0 + h, pl.ds(g0, ng)])

    def right(h):
        return flat(src[row0 + h, pl.ds(2 + g0, ng)])

    def edge(h):
        return jnp.concatenate([right(h)[:, :64], left(h)[:, 64:]], axis=1)

    if stage == 3:
        return [f(h) for h in range(4) for f in (left, own, right)]
    if stage == 2:
        return [own(h) for h in range(4)] + [edge(h) for h in range(4)]
    ks = [own(h) for h in range(4)]
    for h in (0, 2):
        f0, f1 = edge(h), roll(edge(h + 1), 64)
        ks.append(jnp.concatenate([f0[:, :32], f1[:, 32:96], f0[:, 96:]], axis=1))
    return ks


def down_lhs(src, row0, g0, ng):
    def own(h):
        return flat(src[2 * row0 + h, pl.ds(1 + g0, ng)])

    def left(h):
        return flat(src[2 * row0 + h, pl.ds(g0, ng)])

    ks = [own(h) for h in range(5)]
    for h in (0, 2):
        ks.append(jnp.concatenate([roll(left(h + 1), 64)[:, :64], left(h)[:, 64:]], axis=1))
    return ks + [left(4)]


def conv_rows(lhs, weight, bias, dst, row_lo, row_hi, g0, ng, pairs):
    steps = (row_hi - row_lo) // (2 * pairs)

    def step(i, carry):
        row0 = row_lo + i * (2 * pairs)
        per_pair = [lhs(row0 + 2 * p, g0, ng) for p in range(pairs)]
        ks = [jnp.concatenate(part, axis=0) if pairs > 1 else part[0] for part in zip(*per_pair)]
        res = jnp.dot(jnp.concatenate(ks, axis=1), weight[...], preferred_element_type=F32)
        emit(res, bias, dst, row0, pairs, g0, ng)
        return carry

    lax.fori_loop(0, steps, step, 0)


def pack_cols(stage, buf, lo, hi, right_edge):
    rows = hi - lo
    col = buf[pl.ds(1 + lo, rows), G if right_edge else 1]
    per = 4 if stage == 1 else 2
    width = 128 // per
    col = col.reshape(rows // per, per, N, 128)
    base = 128 - width if right_edge else 0
    parts = []
    for k in range(per):
        v = roll(flat(col[:, k]), k * width - base)
        parts.append(v[:, k * width:(k + 1) * width])
    return jnp.concatenate(parts, axis=1).reshape(rows // per, N, 128)


def unpack_cols(stage, buf, lo, hi, packed, left_halo):
    per = 4 if stage == 1 else 2
    width = 128 // per
    base = 128 - width if left_halo else 0
    g = 0 if left_halo else G + 1
    tiles = flat(packed)
    for k in range(per):
        v = roll(tiles, base - k * width).reshape(-1, N, 128)
        for i in range((hi - lo) // per):
            buf[1 + lo + i * per + k, g] = v[i]


def pack_image(pv, lo, hi):
    rows = hi - lo
    col = pv[pl.ds(1 + lo, rows), 8].reshape(rows // 16, 16, N, 128)
    lanes = lax.broadcasted_iota(jnp.int16, (rows, 128), 1) & 15
    packed = flat(col[:, 15])
    for k in range(15):
        packed = jnp.where(lanes == k, roll(flat(col[:, k]), k - 15), packed)
    return packed.reshape(rows // 16, N, 128)


def unpack_image(pv, lo, hi, packed):
    tiles = flat(packed)
    for k in range(16):
        v = roll(tiles, 15 - k).reshape(-1, N, 128)
        for i in range((hi - lo) // 16):
            pv[1 + lo + 16 * i + k, 0] = v[i]


def row_blocks(rows, start, size):
    out = [(lo, min(lo + size, rows)) for lo in range(start, rows, size)]
    return out + [(lo, min(lo + size, start)) for lo in range(0, start, size)]


class Halo:
    def __init__(self, stage, buf, rows, groups, both, send_c, recv_c, sems, device):
        self.stage, self.buf, self.rows, self.groups, self.both = stage, buf, rows, groups, both
        self.send_c, self.recv_c, self.sems, self.device = send_c, recv_c, sems, device
        self.count, self.sent, self.chunks, self.top, self.bottom = 0, [], [], [], []

    def copy(self, src, dst, direction):
        send_sem, recv_sem = self.sems
        c = pltpu.make_async_remote_copy(
            src_ref=src, dst_ref=dst, send_sem=send_sem.at[self.count], recv_sem=recv_sem.at[self.count],
            device_id=self.device(*direction), device_id_type=MESH)
        self.count += 1
        self.sent.append(c)
        c.start()
        return c

    def send(self, lo, hi):
        buf, last, ng, stage = self.buf, self.rows, self.groups, self.stage
        got = []
        for side in range(2 if self.both else 1):
            direction = (0, 1) if side == 0 else (0, -1)
            if stage == 3:
                src = buf.at[pl.ds(1 + lo, hi - lo), G if side == 0 else 1]
                dst = buf.at[pl.ds(1 + lo, hi - lo), 0 if side == 0 else G + 1]
            else:
                per = {0: 16, 1: 4, 2: 2}[stage]
                part = pl.ds(lo // per, (hi - lo) // per)
                self.send_c[side, part] = (
                    pack_image(buf, lo, hi) if stage == 0 else pack_cols(stage, buf, lo, hi, side == 0))
                src, dst = self.send_c.at[side, part], self.recv_c.at[side, part]
            got.append(self.copy(src, dst, direction))
        self.chunks.append((lo, hi, got))
        if hi == self.rows:
            self.top.append(self.copy(buf.at[last, pl.ds(1, ng)], buf.at[0, pl.ds(1, ng)], (1, 0)))
            self.top.append(self.copy(buf.at[last, ng], buf.at[0, 0], (1, 1)))
            if self.both:
                self.top.append(self.copy(buf.at[last, 1], buf.at[0, ng + 1], (1, -1)))
        if lo == 0 and self.both:
            self.bottom.append(self.copy(buf.at[1, pl.ds(1, ng)], buf.at[last + 1, pl.ds(1, ng)], (-1, 0)))
            self.bottom.append(self.copy(buf.at[1, ng], buf.at[last + 1, 0], (-1, 1)))
            self.bottom.append(self.copy(buf.at[1, 1], buf.at[last + 1, ng + 1], (-1, -1)))

    def need(self, lo, hi):
        left = []
        for first, end, got in self.chunks:
            if first < hi and lo < end:
                for side, c in enumerate(got):
                    c.wait_recv()
                    if self.stage != 3:
                        per = {0: 16, 1: 4, 2: 2}[self.stage]
                        packed = self.recv_c[side, pl.ds(first // per, (end - first) // per)]
                        if self.stage == 0:
                            unpack_image(self.buf, first, end, packed)
                        else:
                            unpack_cols(self.stage, self.buf, first, end, packed, side == 0)
            else:
                left.append((first, end, got))
        self.chunks = left
        if lo < 0:
            for c in self.top:
                c.wait_recv()
            self.top = []
        if hi > self.rows:
            for c in self.bottom:
                c.wait_recv()
            self.bottom = []

    def finish(self):
        assert not (self.chunks or self.top or self.bottom)
        for c in self.sent:
            c.wait_send()


def kernel(h_count, w_count, rows1, x_hbm, sel, dw1, db1, rw1, rb1, dw2, db2, rw2, rb2, dw3, db3, rw3, rb3, out,
           x, pv, y1, z1, y2, z2, y3, bw1, br1, bw2, br2, bw3, br3,
           send_x, recv_x, send_c, recv_c, x_sem, send_sem, recv_sem):
    rows2, rows3 = rows1 // 2, rows1 // 4
    me_h, me_w = lax.axis_index('h'), lax.axis_index('w')

    image_blocks = row_blocks(rows1, 0, 32)
    loads = []
    for i, (lo, hi) in enumerate(image_blocks):
        part = pl.ds(lo * 8, (hi - lo) * 8)
        loads.append(pltpu.make_async_copy(x_hbm.at[:, part], x.at[:, part], x_sem.at[i]))
        loads[-1].start()

    def device(dh, dw):
        return {'h': lax.rem(me_h + dh + h_count, h_count), 'w': lax.rem(me_w + dw + w_count, w_count)}

    barrier = pltpu.get_barrier_semaphore()
    others = [(dh, dw) for dh in (-1, 0, 1) for dw in (-1, 0, 1) if dh or dw]
    for dh, dw in others:
        pl.semaphore_signal(barrier, inc=1, device_id=device(dh, dw), device_id_type=MESH)

    picked = jnp.dot(sel[...], dw1[...], preferred_element_type=F32).astype(BF)
    bw1[...] = jnp.concatenate([picked[j * 256:(j + 1) * 256] for j in range(8)], axis=1)
    build_weight(br1, rw1, REFINE1_K, 1)
    build_weight(bw2, dw2, DOWN2_K, 2)
    build_weight(br2, rw2, REFINE2_K, 1)
    build_weight(bw3, dw3, DOWN3_K, 2)
    build_weight(br3, rw3, REFINE3_K, 1)

    def halo(e, stage, buf, rows, groups, both):
        sems = (send_sem.at[e], recv_sem.at[e])
        if stage == 0:
            return Halo(stage, buf, rows, groups, both, send_x, recv_x, sems, device)
        if stage == 3:
            return Halo(stage, buf, rows, groups, both, None, None, sems, device)
        return Halo(stage, buf, rows, groups, both, send_c.at[e - 1], recv_c.at[e - 1], sems, device)

    pv_halo = halo(0, 0, pv, rows1, 8, False)
    y1_halo = halo(1, 1, y1, rows1, G, True)
    z1_halo = halo(2, 1, z1, rows1, G, False)
    y2_halo = halo(3, 2, y2, rows2, G, True)
    z2_halo = halo(4, 2, z2, rows2, G, False)
    y3_halo = halo(5, 3, y3, rows3, G, True)

    lane = lax.broadcasted_iota(jnp.int16, (N, 128), 1)

    def swap(v, dist, blocks):
        mask = (lane & dist) == 0
        new = list(v)
        for i in range(8):
            if not i & blocks:
                a, b = v[i], v[i + blocks]
                new[i] = jnp.where(mask, a, roll(b, dist))
                new[i + blocks] = jnp.where(mask, roll(a, -dist), b)
        return new

    def to_pairs(i, carry):
        t = jnp.transpose(x[:, pl.ds(i * 16, 16), :], (1, 0, 2))
        for p in range(2):
            v = [t[p * 8 + k] for k in range(8)]
            for dist, blocks in ((64, 4), (32, 2), (16, 1)):
                v = swap(v, dist, blocks)
            for q in range(8):
                pv[1 + 2 * i + p, 1 + q] = v[q]
        return carry

    for i, (lo, hi) in enumerate(image_blocks):
        loads[i].wait()
        lax.fori_loop(lo // 2, hi // 2, to_pairs, 0)
        if i == 0:
            pl.semaphore_wait(barrier, len(others))
        pv_halo.send(lo, hi)

    bias1 = tiled_bias(db1)
    per = 8
    size = per * 8 * N

    def down1(i, carry):
        row0 = i * per
        sub = lax.broadcasted_iota(jnp.int16, (size, 128), 1) & 15
        own = flat(pv[pl.ds(row0 + 1, per), pl.ds(1, 8)])
        above = flat(pv[pl.ds(row0, per), pl.ds(1, 8)])
        left = flat(pv[pl.ds(row0 + 1, per), pl.ds(0, 8)])
        above_left = flat(pv[pl.ds(row0, per), pl.ds(0, 8)])
        edge = jnp.where(sub == 15, left, jnp.where(sub == 14, roll(left, 63), roll(above_left, 62)))
        second = jnp.concatenate([edge[:, :64], above[:, 64:]], axis=1)
        res = jnp.dot(jnp.concatenate([own, second], axis=1), bw1[...], preferred_element_type=F32)
        val = jnp.maximum(res + bias1, 0.0).astype(BF).reshape(per, 8, N, 256)
        for r in range(per):
            for q in range(8):
                y1[row0 + 1 + r, 1 + 2 * q] = val[r, q, :, :128]
                y1[row0 + 1 + r, 2 + 2 * q] = val[r, q, :, 128:]
        return carry

    for lo, hi in row_blocks(rows1, 8, 32):
        pv_halo.need(lo - 1, hi)
        lax.fori_loop(lo // per, hi // per, down1, 0)
        y1_halo.send(lo, hi)

    def into(buf):
        def dst(row, g0, ng, val):
            buf[row + 1, pl.ds(1 + g0, ng)] = val
        return dst

    def into_out(row, g0, ng, val):
        out[row, pl.ds(g0, ng)] = val

    def refine(stage, src, src_halo, weight, bias, dst, dst_halo, blocks):
        for lo, hi in blocks:
            src_halo.need(lo - 1, hi + 1)
            conv_rows(functools.partial(refine_lhs, stage, src), weight, bias, dst, lo, hi, 0, G, 2)
            if dst_halo is not None:
                dst_halo.send(lo, hi)

    def down(src, src_halo, weight, bias, dst, dst_halo, blocks):
        for lo, hi in blocks:
            src_halo.need(2 * lo - 1, 2 * hi)
            conv_rows(functools.partial(down_lhs, src), weight, bias, dst, lo, hi, 0, G, 2)
            dst_halo.send(lo, hi)

    refine(1, y1, y1_halo, br1, tiled_bias(rb1), into(z1), z1_halo, row_blocks(rows1, 12, 32))
    down(z1, z1_halo, bw2, tiled_bias(db2), into(y2), y2_halo, row_blocks(rows2, 8, 16))
    refine(2, y2, y2_halo, br2, tiled_bias(rb2), into(z2), z2_halo, row_blocks(rows2, 12, 16))
    down(z2, z2_halo, bw3, tiled_bias(db3), into(y3), y3_halo, row_blocks(rows3, 8, 8))
    refine(3, y3, y3_halo, br3, tiled_bias(rb3), into_out, None, row_blocks(rows3, 12, 8))

    for h in (pv_halo, y1_halo, z1_halo, y2_halo, z2_halo, y3_halo):
        h.finish()


def encode(h_count, w_count, images, *params):
    rows1 = images.shape[1] // 2
    rows2, rows3 = rows1 // 2, rows1 // 4
    x = jnp.transpose(images, (0, 1, 3, 2)).reshape(N, rows1 * 8, 128)
    args = [x, jnp.asarray(first_weight_selector(), BF)]
    for i, p in enumerate(params):
        args.append(p.reshape(1, -1) if i % 2 else (p.reshape(36, 32) if i == 0 else p))

    def act(rows, groups):
        return pltpu.VMEM((rows, groups, N, 128), BF)

    flops = 2 * 16 * rows1 * 64 * 32 * 9 * (4 + 32 + 16 + 32 + 16 + 32)
    out = pl.pallas_call(
        functools.partial(kernel, h_count, w_count, rows1),
        name='encoder',
        out_shape=jax.ShapeDtypeStruct((rows3, G, N, 128), BF),
        in_specs=[pl.BlockSpec(memory_space=pl.ANY)] + [pl.BlockSpec(memory_space=pltpu.VMEM)] * (len(args) - 1),
        out_specs=pl.BlockSpec(memory_space=pltpu.VMEM),
        scratch_shapes=[
            pltpu.VMEM((N, rows1 * 8, 128), BF), act(rows1 + 1, 9), act(rows1 + 2, G + 2), act(rows1 + 1, G + 1),
            act(rows2 + 2, G + 2), act(rows2 + 1, G + 1), act(rows3 + 2, G + 2),
            pltpu.VMEM((256, 256), BF), pltpu.VMEM((768, 256), BF), pltpu.VMEM((1024, 256), BF),
            pltpu.VMEM((1024, 256), BF), pltpu.VMEM((1024, 256), BF), pltpu.VMEM((1536, 256), BF),
            pltpu.VMEM((1, rows1 // 16, N, 128), BF), pltpu.VMEM((1, rows1 // 16, N, 128), BF),
            pltpu.VMEM((4, 2, rows1 // 4, N, 128), BF), pltpu.VMEM((4, 2, rows1 // 4, N, 128), BF),
            pltpu.SemaphoreType.DMA((8,)), pltpu.SemaphoreType.DMA((6, 20)), pltpu.SemaphoreType.DMA((6, 20)),
        ],
        compiler_params=pltpu.CompilerParams(
            collective_id=0, has_side_effects=True, vmem_limit_bytes=67043328),
        cost_estimate=pl.CostEstimate(flops=flops, bytes_accessed=7 * 2**20, transcendentals=0),
    )(*args)
    return jnp.transpose(out, (2, 0, 1, 3))


def solution(mesh):
    tile_spec = P('batch', 'h', 'w', None)
    body = functools.partial(encode, mesh.shape['h'], mesh.shape['w'])
    return jax.shard_map(body, mesh=mesh, in_specs=(tile_spec,) + (P(),) * 12, out_specs=tile_spec, check_vma=False)
```

```python
import functools

import jax
import jax.numpy as jnp
import numpy as np
from jax import lax
from jax.experimental import pallas as pl
from jax.experimental.pallas import tpu as pltpu
from jax.sharding import PartitionSpec as P

BF = jnp.bfloat16
F32 = jnp.float32
N = 16
G = 16
TILES = 4
DOWN1_ROWS = 16
PAIRS = 4
MESH = pl.DeviceIdType.MESH


def first_weight_selector():
    sel = np.zeros((8, 256, 36), np.float32)
    for j in range(8):
        for c in range(4):
            for wi in range(16):
                b = wi - 2 * j + 1
                if 0 <= b <= 2:
                    for hi in range(2):
                        sel[j, hi * 64 + c * 16 + wi, ((hi + 1) * 3 + b) * 4 + c] = 1
                    sel[j, 128 + 64 + c * 16 + wi, (0 * 3 + b) * 4 + c] = 1
            if j == 0:
                for a, wi in ((1, 15), (2, 14), (0, 13)):
                    sel[j, 128 + c * 16 + wi, (a * 3) * 4 + c] = 1
    return sel.reshape(8 * 256, 36)


def roll(v, shift):
    shift %= 128
    return v if shift == 0 else pltpu.roll(v, shift, v.ndim - 1)


def flat(v):
    return v.reshape(-1, 128)


def build_weight(big, w, k_blocks, stride):
    cin, cout = w.shape[2], w.shape[3]
    ncols = 128 // cout
    zero = jnp.zeros((cin, cout), BF)
    for kp, pos in enumerate(k_blocks):
        for orow in range(2):
            pieces = []
            for j in range(ncols):
                piece = zero
                if pos is not None:
                    a, b = pos[0] - stride * orow, pos[1] - stride * j + 1
                    if 0 <= a <= 2 and 0 <= b <= 2:
                        piece = w[a, b]
                pieces.append(piece)
            big[kp * cin:(kp + 1) * cin, orow * 128:(orow + 1) * 128] = (
                pieces[0] if ncols == 1 else jnp.concatenate(pieces, axis=1))


REFINE1_K = ([(ir, ic) for ir in range(4) for ic in range(4)]
             + [p for e in (0, 2) for p in ((e, 4), (e + 1, -1), (e + 1, 4), (e, -1))])
REFINE2_K = ([(ir, ic) for ir in range(4) for ic in range(2)]
             + [p for ir in range(4) for p in ((ir, 2), (ir, -1))])
REFINE3_K = [(ir, ic) for ir in range(4) for ic in (-1, 0, 1)]
DOWN2_K = ([(ir, ic) for ir in range(5) for ic in range(4)]
           + [p for e in (0, 2) for p in (None, (e + 1, -1), None, (e, -1))]
           + [None, None, None, (4, -1)])
DOWN3_K = ([(ir, ic) for ir in range(5) for ic in range(2)]
           + [p for e in (0, 2) for p in ((e + 1, -1), (e, -1))] + [None, (4, -1)])


def tiled_bias(b):
    reps = 128 // b.shape[1]
    return jnp.concatenate([b[...]] * (2 * reps), axis=1)


def emit(res, bias, dst, row0, pairs, g0, ng):
    val = jnp.maximum(res + bias, 0.0).astype(BF).reshape(pairs, ng, N, 256)
    for p in range(pairs):
        for half in range(2):
            dst(row0 + 2 * p + half, g0, ng, val[p, :, :, half * 128:(half + 1) * 128])


def refine_lhs(stage, src, row0, g0, ng):
    def own(h):
        return flat(src[row0 + h, pl.ds(1 + g0, ng)])

    def left(h):
        return flat(src[row0 + h, pl.ds(g0, ng)])

    def right(h):
        return flat(src[row0 + h, pl.ds(2 + g0, ng)])

    def edge(h):
        return jnp.concatenate([right(h)[:, :64], left(h)[:, 64:]], axis=1)

    if stage == 3:
        return [f(h) for h in range(4) for f in (left, own, right)]
    if stage == 2:
        return [own(h) for h in range(4)] + [edge(h) for h in range(4)]
    ks = [own(h) for h in range(4)]
    for h in (0, 2):
        f0, f1 = edge(h), roll(edge(h + 1), 64)
        ks.append(jnp.concatenate([f0[:, :32], f1[:, 32:96], f0[:, 96:]], axis=1))
    return ks


def down_lhs(src, row0, g0, ng):
    def own(h):
        return flat(src[2 * row0 + h, pl.ds(1 + g0, ng)])

    def left(h):
        return flat(src[2 * row0 + h, pl.ds(g0, ng)])

    ks = [own(h) for h in range(5)]
    for h in (0, 2):
        ks.append(jnp.concatenate([roll(left(h + 1), 64)[:, :64], left(h)[:, 64:]], axis=1))
    return ks + [left(4)]


def conv_rows(lhs, weight, bias, dst, row_lo, row_hi, g0, ng, pairs):
    steps = (row_hi - row_lo) // (2 * pairs)

    def step(i, carry):
        row0 = row_lo + i * (2 * pairs)
        per_pair = [lhs(row0 + 2 * p, g0, ng) for p in range(pairs)]
        ks = [jnp.concatenate(part, axis=0) if pairs > 1 else part[0] for part in zip(*per_pair)]
        res = jnp.dot(jnp.concatenate(ks, axis=1), weight[...], preferred_element_type=F32)
        emit(res, bias, dst, row0, pairs, g0, ng)
        return carry

    lax.fori_loop(0, steps, step, 0)


def pack_cols(stage, buf, lo, hi, right_edge):
    rows = hi - lo
    col = buf[pl.ds(1 + lo, rows), G if right_edge else 1]
    per = 4 if stage == 1 else 2
    width = 128 // per
    col = col.reshape(rows // per, per, N, 128)
    base = 128 - width if right_edge else 0
    parts = []
    for k in range(per):
        v = roll(flat(col[:, k]), k * width - base)
        parts.append(v[:, k * width:(k + 1) * width])
    return jnp.concatenate(parts, axis=1).reshape(rows // per, N, 128)


def unpack_cols(stage, buf, lo, hi, packed, left_halo):
    per = 4 if stage == 1 else 2
    width = 128 // per
    base = 128 - width if left_halo else 0
    g = 0 if left_halo else G + 1
    tiles = flat(packed)
    for k in range(per):
        v = roll(tiles, base - k * width).reshape(-1, N, 128)
        for i in range((hi - lo) // per):
            buf[1 + lo + i * per + k, g] = v[i]


def pack_image(pv, lo, hi):
    rows = hi - lo
    col = pv[pl.ds(1 + lo, rows), 8].reshape(rows // 16, 16, N, 128)
    lanes = lax.broadcasted_iota(jnp.int16, (rows, 128), 1) & 15
    packed = flat(col[:, 15])
    for k in range(15):
        packed = jnp.where(lanes == k, roll(flat(col[:, k]), k - 15), packed)
    return packed.reshape(rows // 16, N, 128)


def unpack_image(pv, lo, hi, packed):
    tiles = flat(packed)
    for k in range(16):
        v = roll(tiles, 15 - k).reshape(-1, N, 128)
        for i in range((hi - lo) // 16):
            pv[1 + lo + 16 * i + k, 0] = v[i]


def row_blocks(rows, start, size):
    out = [(lo, min(lo + size, rows)) for lo in range(start, rows, size)]
    return out + [(lo, min(lo + size, start)) for lo in range(0, start, size)]


class Halo:
    def __init__(self, stage, buf, rows, groups, both, send_c, recv_c, sems, device):
        self.stage, self.buf, self.rows, self.groups, self.both = stage, buf, rows, groups, both
        self.send_c, self.recv_c, self.sems, self.device = send_c, recv_c, sems, device
        self.count, self.sent, self.chunks, self.top, self.bottom = 0, [], [], [], []

    def copy(self, src, dst, direction):
        send_sem, recv_sem = self.sems
        c = pltpu.make_async_remote_copy(
            src_ref=src, dst_ref=dst, send_sem=send_sem.at[self.count], recv_sem=recv_sem.at[self.count],
            device_id=self.device(*direction), device_id_type=MESH)
        self.count += 1
        self.sent.append(c)
        c.start()
        return c

    def send(self, lo, hi):
        buf, last, ng, stage = self.buf, self.rows, self.groups, self.stage
        got = []
        for side in range(2 if self.both else 1):
            direction = (0, 1) if side == 0 else (0, -1)
            if stage == 3:
                src = buf.at[pl.ds(1 + lo, hi - lo), G if side == 0 else 1]
                dst = buf.at[pl.ds(1 + lo, hi - lo), 0 if side == 0 else G + 1]
            else:
                per = {0: 16, 1: 4, 2: 2}[stage]
                part = pl.ds(lo // per, (hi - lo) // per)
                self.send_c[side, part] = (
                    pack_image(buf, lo, hi) if stage == 0 else pack_cols(stage, buf, lo, hi, side == 0))
                src, dst = self.send_c.at[side, part], self.recv_c.at[side, part]
            got.append(self.copy(src, dst, direction))
        self.chunks.append((lo, hi, got))
        if hi == self.rows:
            self.top.append(self.copy(buf.at[last, pl.ds(1, ng)], buf.at[0, pl.ds(1, ng)], (1, 0)))
            self.top.append(self.copy(buf.at[last, ng], buf.at[0, 0], (1, 1)))
            if self.both:
                self.top.append(self.copy(buf.at[last, 1], buf.at[0, ng + 1], (1, -1)))
        if lo == 0 and self.both:
            self.bottom.append(self.copy(buf.at[1, pl.ds(1, ng)], buf.at[last + 1, pl.ds(1, ng)], (-1, 0)))
            self.bottom.append(self.copy(buf.at[1, ng], buf.at[last + 1, 0], (-1, 1)))
            self.bottom.append(self.copy(buf.at[1, 1], buf.at[last + 1, ng + 1], (-1, -1)))

    def need(self, lo, hi):
        left = []
        for first, end, got in self.chunks:
            if first < hi and lo < end:
                for side, c in enumerate(got):
                    c.wait_recv()
                    if self.stage != 3:
                        per = {0: 16, 1: 4, 2: 2}[self.stage]
                        packed = self.recv_c[side, pl.ds(first // per, (end - first) // per)]
                        if self.stage == 0:
                            unpack_image(self.buf, first, end, packed)
                        else:
                            unpack_cols(self.stage, self.buf, first, end, packed, side == 0)
            else:
                left.append((first, end, got))
        self.chunks = left
        if lo < 0:
            for c in self.top:
                c.wait_recv()
            self.top = []
        if hi > self.rows:
            for c in self.bottom:
                c.wait_recv()
            self.bottom = []

    def finish(self):
        assert not (self.chunks or self.top or self.bottom)
        for c in self.sent:
            c.wait_send()


def kernel(h_count, w_count, rows1, x_hbm, sel, dw1, db1, rw1, rb1, dw2, db2, rw2, rb2, dw3, db3, rw3, rb3, out,
           x, pv, y1, z1, y2, z2, y3, w36, bw1, br1, bw2, br2, bw3, br3,
           send_x, recv_x, send_c, recv_c, x_sem, send_sem, recv_sem):
    rows2, rows3 = rows1 // 2, rows1 // 4
    me_h, me_w = lax.axis_index('h'), lax.axis_index('w')

    image_blocks = row_blocks(rows1, 0, 32)
    loads = []
    for i, (lo, hi) in enumerate(image_blocks):
        part = pl.ds(lo * 8, (hi - lo) * 8)
        loads.append(pltpu.make_async_copy(x_hbm.at[:, part], x.at[:, part], x_sem.at[i]))
        loads[-1].start()

    def device(dh, dw):
        return {'h': lax.rem(me_h + dh + h_count, h_count), 'w': lax.rem(me_w + dw + w_count, w_count)}

    barrier = pltpu.get_barrier_semaphore()
    others = [(dh, dw) for dh in (-1, 0, 1) for dw in (-1, 0, 1) if dh or dw]
    for dh, dw in others:
        pl.semaphore_signal(barrier, inc=1, device_id=device(dh, dw), device_id_type=MESH)

    for k in range(9):
        w36[4 * k:4 * k + 4, :] = dw1[k].astype(F32)
    picked = jnp.dot(sel[...], w36[...].astype(BF), preferred_element_type=F32).astype(BF)
    bw1[...] = jnp.concatenate([picked[j * 256:(j + 1) * 256] for j in range(8)], axis=1)
    build_weight(br1, rw1, REFINE1_K, 1)
    build_weight(bw2, dw2, DOWN2_K, 2)
    build_weight(br2, rw2, REFINE2_K, 1)
    build_weight(bw3, dw3, DOWN3_K, 2)
    build_weight(br3, rw3, REFINE3_K, 1)

    def halo(e, stage, buf, rows, groups, both):
        sems = (send_sem.at[e], recv_sem.at[e])
        if stage == 0:
            return Halo(stage, buf, rows, groups, both, send_x, recv_x, sems, device)
        if stage == 3:
            return Halo(stage, buf, rows, groups, both, None, None, sems, device)
        return Halo(stage, buf, rows, groups, both, send_c.at[e - 1], recv_c.at[e - 1], sems, device)

    pv_halo = halo(0, 0, pv, rows1, 8, False)
    y1_halo = halo(1, 1, y1, rows1, G, True)
    z1_halo = halo(2, 1, z1, rows1, G, False)
    y2_halo = halo(3, 2, y2, rows2, G, True)
    z2_halo = halo(4, 2, z2, rows2, G, False)
    y3_halo = halo(5, 3, y3, rows3, G, True)

    lane = lax.broadcasted_iota(jnp.int16, (N, 128), 1)

    def swap(v, dist, blocks):
        mask = (lane & dist) == 0
        new = list(v)
        for i in range(8):
            if not i & blocks:
                a, b = v[i], v[i + blocks]
                new[i] = jnp.where(mask, a, roll(b, dist))
                new[i + blocks] = jnp.where(mask, roll(a, -dist), b)
        return new

    def to_pairs(i, carry):
        for u in range(TILES):
            t = jnp.transpose(x[:, pl.ds((i * TILES + u) * 16, 16), :], (1, 0, 2))
            for p in range(2):
                v = [t[p * 8 + k] for k in range(8)]
                for dist, blocks in ((64, 4), (32, 2), (16, 1)):
                    v = swap(v, dist, blocks)
                for q in range(8):
                    pv[1 + 2 * (i * TILES + u) + p, 1 + q] = v[q]
        return carry

    for i, (lo, hi) in enumerate(image_blocks):
        loads[i].wait()
        lax.fori_loop(lo // 2 // TILES, hi // 2 // TILES, to_pairs, 0)
        if i == 0:
            pl.semaphore_wait(barrier, len(others))
        pv_halo.send(lo, hi)

    bias1 = tiled_bias(db1)
    per = DOWN1_ROWS
    size = per * 8 * N

    def down1(i, carry):
        row0 = i * per
        sub = lax.broadcasted_iota(jnp.int16, (size, 128), 1) & 15
        own = flat(pv[pl.ds(row0 + 1, per), pl.ds(1, 8)])
        above = flat(pv[pl.ds(row0, per), pl.ds(1, 8)])
        left = flat(pv[pl.ds(row0 + 1, per), pl.ds(0, 8)])
        above_left = flat(pv[pl.ds(row0, per), pl.ds(0, 8)])
        edge = jnp.where(sub == 15, left, jnp.where(sub == 14, roll(left, 63), roll(above_left, 62)))
        second = jnp.concatenate([edge[:, :64], above[:, 64:]], axis=1)
        res = jnp.dot(jnp.concatenate([own, second], axis=1), bw1[...], preferred_element_type=F32)
        val = jnp.maximum(res + bias1, 0.0).astype(BF).reshape(per, 8, N, 256)
        for r in range(per):
            for q in range(8):
                y1[row0 + 1 + r, 1 + 2 * q] = val[r, q, :, :128]
                y1[row0 + 1 + r, 2 + 2 * q] = val[r, q, :, 128:]
        return carry

    for lo, hi in row_blocks(rows1, 16, 32):
        pv_halo.need(lo - 1, hi)
        lax.fori_loop(lo // per, hi // per, down1, 0)
        y1_halo.send(lo, hi)

    def into(buf):
        def dst(row, g0, ng, val):
            buf[row + 1, pl.ds(1 + g0, ng)] = val
        return dst

    def into_out(row, g0, ng, val):
        out[row, pl.ds(g0, ng)] = val

    def refine(stage, src, src_halo, weight, bias, dst, dst_halo, blocks):
        for lo, hi in blocks:
            src_halo.need(lo - 1, hi + 1)
            conv_rows(functools.partial(refine_lhs, stage, src), weight, bias, dst, lo, hi, 0, G, PAIRS)
            if dst_halo is not None:
                dst_halo.send(lo, hi)

    def down(src, src_halo, weight, bias, dst, dst_halo, blocks):
        for lo, hi in blocks:
            src_halo.need(2 * lo - 1, 2 * hi)
            conv_rows(functools.partial(down_lhs, src), weight, bias, dst, lo, hi, 0, G, PAIRS)
            dst_halo.send(lo, hi)

    refine(1, y1, y1_halo, br1, tiled_bias(rb1), into(z1), z1_halo, row_blocks(rows1, 24, 32))
    down(z1, z1_halo, bw2, tiled_bias(db2), into(y2), y2_halo, row_blocks(rows2, 16, 16))
    refine(2, y2, y2_halo, br2, tiled_bias(rb2), into(z2), z2_halo, row_blocks(rows2, 24, 16))
    down(z2, z2_halo, bw3, tiled_bias(db3), into(y3), y3_halo, row_blocks(rows3, 16, 8))
    refine(3, y3, y3_halo, br3, tiled_bias(rb3), into_out, None, row_blocks(rows3, 24, 8))

    for h in (pv_halo, y1_halo, z1_halo, y2_halo, z2_halo, y3_halo):
        h.finish()


def encode(h_count, w_count, images, *params):
    rows1 = images.shape[1] // 2
    rows2, rows3 = rows1 // 2, rows1 // 4
    x = jnp.transpose(images, (0, 1, 3, 2)).reshape(N, rows1 * 8, 128)
    args = [x, jnp.asarray(first_weight_selector(), BF)]
    for i, p in enumerate(params):
        args.append(p.reshape(1, -1) if i % 2 else (p.reshape(9, 4, 32) if i == 0 else p))

    def act(rows, groups):
        return pltpu.VMEM((rows, groups, N, 128), BF)

    flops = 2 * 16 * rows1 * 64 * 32 * 9 * (4 + 32 + 16 + 32 + 16 + 32)
    out = pl.pallas_call(
        functools.partial(kernel, h_count, w_count, rows1),
        name='encoder',
        out_shape=jax.ShapeDtypeStruct((rows3, G, N, 128), BF),
        in_specs=[pl.BlockSpec(memory_space=pl.ANY)] + [pl.BlockSpec(memory_space=pltpu.VMEM)] * (len(args) - 1),
        out_specs=pl.BlockSpec(memory_space=pltpu.VMEM),
        scratch_shapes=[
            pltpu.VMEM((N, rows1 * 8, 128), BF), act(rows1 + 1, 9), act(rows1 + 2, G + 2), act(rows1 + 1, G + 1),
            act(rows2 + 2, G + 2), act(rows2 + 1, G + 1), act(rows3 + 2, G + 2),
            pltpu.VMEM((36, 32), F32), pltpu.VMEM((256, 256), BF), pltpu.VMEM((768, 256), BF), pltpu.VMEM((1024, 256), BF),
            pltpu.VMEM((1024, 256), BF), pltpu.VMEM((1024, 256), BF), pltpu.VMEM((1536, 256), BF),
            pltpu.VMEM((1, rows1 // 16, N, 128), BF), pltpu.VMEM((1, rows1 // 16, N, 128), BF),
            pltpu.VMEM((4, 2, rows1 // 4, N, 128), BF), pltpu.VMEM((4, 2, rows1 // 4, N, 128), BF),
            pltpu.SemaphoreType.DMA((8,)), pltpu.SemaphoreType.DMA((6, 20)), pltpu.SemaphoreType.DMA((6, 20)),
        ],
        compiler_params=pltpu.CompilerParams(
            collective_id=0, has_side_effects=True, vmem_limit_bytes=56 * 2**20),
        cost_estimate=pl.CostEstimate(flops=flops, bytes_accessed=7 * 2**20, transcendentals=0),
    )(*args)
    return jnp.transpose(out, (2, 0, 1, 3))


def solution(mesh):
    tile_spec = P('batch', 'h', 'w', None)
    body = functools.partial(encode, mesh.shape['h'], mesh.shape['w'])
    return jax.shard_map(body, mesh=mesh, in_specs=(tile_spec,) + (P(),) * 12, out_specs=tile_spec, check_vma=False)
```

```python
import functools

import jax
import jax.numpy as jnp
import numpy as np
from jax import lax
from jax.experimental import pallas as pl
from jax.experimental.pallas import tpu as pltpu
from jax.sharding import PartitionSpec as P

BF = jnp.bfloat16
F32 = jnp.float32
N = 16
G = 16
TILES = 4
DOWN1_ROWS = 16
PAIRS = 4
MESH = pl.DeviceIdType.MESH


def first_weight_selector():
    sel = np.zeros((8, 256, 36), np.float32)
    for j in range(8):
        for c in range(4):
            for wi in range(16):
                b = wi - 2 * j + 1
                if 0 <= b <= 2:
                    for hi in range(2):
                        sel[j, hi * 64 + c * 16 + wi, ((hi + 1) * 3 + b) * 4 + c] = 1
                    sel[j, 128 + 64 + c * 16 + wi, (0 * 3 + b) * 4 + c] = 1
            if j == 0:
                for a, wi in ((1, 15), (2, 14), (0, 13)):
                    sel[j, 128 + c * 16 + wi, (a * 3) * 4 + c] = 1
    return sel.reshape(8 * 256, 36)


def roll(v, shift):
    shift %= 128
    return v if shift == 0 else pltpu.roll(v, shift, v.ndim - 1)


def flat(v):
    return v.reshape(-1, 128)


def build_weight(big, w, k_blocks, stride):
    cin, cout = w.shape[2], w.shape[3]
    ncols = 128 // cout
    taps = [[w[a, b] for b in range(3)] for a in range(3)]
    zero = jnp.zeros((cin, cout), BF)
    for kp, pos in enumerate(k_blocks):
        pieces = []
        for orow in range(2):
            for j in range(ncols):
                piece = zero
                if pos is not None:
                    a, b = pos[0] - stride * orow, pos[1] - stride * j + 1
                    if 0 <= a <= 2 and 0 <= b <= 2:
                        piece = taps[a][b]
                pieces.append(piece)
        big[kp * cin:(kp + 1) * cin, :] = jnp.concatenate(pieces, axis=1)


REFINE1_K = ([(ir, ic) for ir in range(4) for ic in range(4)]
             + [p for e in (0, 2) for p in ((e, 4), (e + 1, -1), (e + 1, 4), (e, -1))])
REFINE2_K = ([(ir, ic) for ir in range(4) for ic in range(2)]
             + [p for ir in range(4) for p in ((ir, 2), (ir, -1))])
REFINE3_K = [(ir, ic) for ir in range(4) for ic in (-1, 0, 1)]
DOWN2_K = ([(ir, ic) for ir in range(5) for ic in range(4)]
           + [p for e in (0, 2) for p in (None, (e + 1, -1), None, (e, -1))]
           + [None, None, None, (4, -1)])
DOWN3_K = ([(ir, ic) for ir in range(5) for ic in range(2)]
           + [p for e in (0, 2) for p in ((e + 1, -1), (e, -1))] + [None, (4, -1)])


def tiled_bias(b):
    reps = 128 // b.shape[1]
    return jnp.concatenate([b[...]] * (2 * reps), axis=1)


def refine_lhs(stage, src, p0, pairs, g0, ng):
    def rows(h, g):
        return flat(src[pl.ds(p0 + (h + 1) // 2, pairs), (h + 1) % 2, pl.ds(g, ng)])

    def own(h):
        return rows(h, 1 + g0)

    def left(h):
        return rows(h, g0)

    def right(h):
        return rows(h, 2 + g0)

    def edge(h):
        return jnp.concatenate([right(h)[:, :64], left(h)[:, 64:]], axis=1)

    if stage == 3:
        return [f(h) for h in range(4) for f in (left, own, right)]
    if stage == 2:
        return [own(h) for h in range(4)] + [edge(h) for h in range(4)]
    ks = [own(h) for h in range(4)]
    for h in (0, 2):
        f0, f1 = edge(h), roll(edge(h + 1), 64)
        ks.append(jnp.concatenate([f0[:, :32], f1[:, 32:96], f0[:, 96:]], axis=1))
    return ks


def down_lhs(src, p0, pairs, g0, ng):
    def rows(h, g):
        return flat(src[pl.ds(p0 + (h + 3) // 4, pairs), (h + 3) % 4, pl.ds(g, ng)])

    def own(h):
        return rows(h, 1 + g0)

    def left(h):
        return rows(h, g0)

    ks = [own(h) for h in range(5)]
    for h in (0, 2):
        ks.append(jnp.concatenate([roll(left(h + 1), 64)[:, :64], left(h)[:, 64:]], axis=1))
    return ks + [left(4)]


def conv_rows(lhs, weight, bias, dst, lo, hi, ranges, pairs):
    pairs = min(pairs, (hi - lo) // 2)

    def step(i, carry):
        p0 = lo // 2 + i * pairs
        parts = [lhs(p0, pairs, g0, ng) for g0, ng in ranges]
        ks = [jnp.concatenate(part, axis=0) if len(ranges) > 1 else part[0] for part in zip(*parts)]
        res = jnp.dot(jnp.concatenate(ks, axis=1), weight[...], preferred_element_type=F32)
        val = jnp.maximum(res + bias, 0.0).astype(BF)
        at = 0
        for g0, ng in ranges:
            size = pairs * ng * N
            tile = val[at:at + size]
            at += size
            dst(lo // 4 + i * (pairs // 2), p0, pairs, g0, ng, tile)
        return carry

    lax.fori_loop(0, (hi - lo) // (2 * pairs), step, 0)


def into_pairs(buf, shift):
    def dst(quad0, p0, pairs, g0, ng, tile):
        for half in range(2):
            buf[pl.ds(p0 + shift, pairs), half, pl.ds(g0 + shift, ng)] = (
                tile[:, half * 128:(half + 1) * 128].reshape(pairs, ng, N, 128))
    return dst


def into_quads(buf):
    def dst(quad0, p0, pairs, g0, ng, tile):
        for half in range(2):
            v = tile[:, half * 128:(half + 1) * 128].reshape(pairs // 2, 2, ng, N, 128)
            for odd in range(2):
                buf[pl.ds(quad0 + 1, pairs // 2), 2 * odd + half, pl.ds(1 + g0, ng)] = v[:, odd]
    return dst


def pack_cols(stage, buf, lo, hi, right_edge):
    view = buf.shape[1]
    col = buf[pl.ds(lo // view + 1, (hi - lo) // view), :, G if right_edge else 1]
    per = 4 if stage == 1 else 2
    width = 128 // per
    col = col.reshape((hi - lo) // per, per, N, 128)
    base = 128 - width if right_edge else 0
    parts = []
    for k in range(per):
        v = roll(flat(col[:, k]), k * width - base)
        parts.append(v[:, k * width:(k + 1) * width])
    return jnp.concatenate(parts, axis=1).reshape((hi - lo) // per, N, 128)


def unpack_cols(stage, buf, lo, hi, packed, left_halo):
    view = buf.shape[1]
    per = 4 if stage == 1 else 2
    width = 128 // per
    base = 128 - width if left_halo else 0
    tiles = flat(packed)
    rows = [roll(tiles, base - k * width).reshape(-1, N, 128) for k in range(per)]
    buf[pl.ds(lo // view + 1, (hi - lo) // view), :, 0 if left_halo else G + 1] = (
        jnp.stack(rows, axis=1).reshape((hi - lo) // view, view, N, 128))


def pack_image(pv, lo, hi):
    rows = hi - lo
    col = pv[pl.ds(1 + lo, rows), 8].reshape(rows // 16, 16, N, 128)
    lanes = lax.broadcasted_iota(jnp.int16, (rows, 128), 1) & 15
    packed = flat(col[:, 15])
    for k in range(15):
        packed = jnp.where(lanes == k, roll(flat(col[:, k]), k - 15), packed)
    return packed.reshape(rows // 16, N, 128)


def unpack_image(pv, lo, hi, packed):
    tiles = flat(packed)
    rows = [roll(tiles, 15 - k).reshape(-1, N, 128) for k in range(16)]
    pv[pl.ds(1 + lo, hi - lo), 0] = jnp.stack(rows, axis=1).reshape(hi - lo, N, 128)


def row_blocks(rows, start, size):
    out = [(lo, min(lo + size, rows)) for lo in range(start, rows, size)]
    return out + [(lo, min(lo + size, start)) for lo in range(0, start, size)]


class Halo:
    def __init__(self, stage, buf, rows, groups, both, send_c, recv_c, sems, device):
        self.stage, self.buf, self.rows, self.groups, self.both = stage, buf, rows, groups, both
        self.send_c, self.recv_c, self.sems, self.device = send_c, recv_c, sems, device
        self.count, self.sent, self.chunks = 0, [], []
        self.slabs, self.corners = {'top': [], 'bottom': []}, {'top': [], 'bottom': []}

    def copy(self, src, dst, direction):
        send_sem, recv_sem = self.sems
        c = pltpu.make_async_remote_copy(
            src_ref=src, dst_ref=dst, send_sem=send_sem.at[self.count], recv_sem=recv_sem.at[self.count],
            device_id=self.device(*direction), device_id_type=MESH)
        self.count += 1
        self.sent.append(c)
        c.start()
        return c

    def send_cols(self, lo, hi, side):
        buf, stage = self.buf, self.stage
        if stage == 3:
            part = pl.ds(lo // 2 + 1, (hi - lo) // 2)
            src = buf.at[part, :, G if side == 0 else 1]
            dst = buf.at[part, :, 0 if side == 0 else G + 1]
        else:
            per = {0: 16, 1: 4, 2: 2}[stage]
            part = pl.ds(lo // per, (hi - lo) // per)
            self.send_c[side, part] = (
                pack_image(buf, lo, hi) if stage == 0 else pack_cols(stage, buf, lo, hi, side == 0))
            src, dst = self.send_c.at[side, part], self.recv_c.at[side, part]
        self.chunks.append((lo, hi, side, self.copy(src, dst, (0, 1 if side == 0 else -1))))

    def cells(self, row, groups):
        view = self.buf.shape[1] if self.stage else 1
        at = (row // view + 1, row % view) if self.stage else (row + 1,)
        return self.buf.at[at + (groups,)]

    def send_rows(self, lo, hi):
        last, ng, cells = self.rows - 1, self.groups, self.cells
        every = pl.ds(1, ng)
        if hi == self.rows:
            self.slabs['top'].append(self.copy(cells(last, every), cells(-1, every), (1, 0)))
            self.corners['top'].append(self.copy(cells(last, ng), cells(-1, 0), (1, 1)))
            if self.both:
                self.corners['top'].append(self.copy(cells(last, 1), cells(-1, ng + 1), (1, -1)))
        if lo == 0 and self.both:
            self.slabs['bottom'].append(self.copy(cells(0, every), cells(last + 1, every), (-1, 0)))
            self.corners['bottom'].append(self.copy(cells(0, ng), cells(last + 1, 0), (-1, 1)))
            self.corners['bottom'].append(self.copy(cells(0, 1), cells(last + 1, ng + 1), (-1, -1)))

    def ends(self, which, lo, hi):
        for end, wanted in (('top', lo < 0), ('bottom', hi > self.rows)):
            if wanted:
                for c in which[end]:
                    c.wait_recv()
                which[end] = []

    def need_rows(self, lo, hi):
        self.ends(self.slabs, lo, hi)

    def need_cols(self, lo, hi):
        left = []
        for chunk in self.chunks:
            first, end, side, c = chunk
            if first < hi and lo < end:
                c.wait_recv()
                if self.stage != 3:
                    per = {0: 16, 1: 4, 2: 2}[self.stage]
                    packed = self.recv_c[side, pl.ds(first // per, (end - first) // per)]
                    if self.stage == 0:
                        unpack_image(self.buf, first, end, packed)
                    else:
                        unpack_cols(self.stage, self.buf, first, end, packed, side == 0)
            else:
                left.append(chunk)
        self.chunks = left
        self.ends(self.corners, lo, hi)

    def finish(self):
        assert not self.chunks and not any(self.slabs.values()) and not any(self.corners.values())
        for c in self.sent:
            c.wait_send()


def schedule(blocks, delay):
    out = []
    for i in range(len(blocks) + delay):
        if i < len(blocks):
            out.append((False, blocks[i]))
        if i >= delay and i - delay < len(blocks):
            out.append((True, blocks[i - delay]))
    return out


def kernel(h_count, w_count, rows1, x_hbm, sel, dw1, db1, rw1, rb1, dw2, db2, rw2, rb2, dw3, db3, rw3, rb3, out,
           x, pv, y1, z1, y2, z2, y3, w36, bw1, br1, bw2, br2, bw3, br3,
           send_x, recv_x, send_c, recv_c, x_sem, send_sem, recv_sem):
    rows2, rows3 = rows1 // 2, rows1 // 4
    me_h, me_w = lax.axis_index('h'), lax.axis_index('w')

    image_blocks = row_blocks(rows1, 0, 32)
    loads = []
    for i, (lo, hi) in enumerate(image_blocks):
        part = pl.ds(lo * 8, (hi - lo) * 8)
        loads.append(pltpu.make_async_copy(x_hbm.at[:, part], x.at[:, part], x_sem.at[i]))
        loads[-1].start()

    def device(dh, dw):
        return {'h': lax.rem(me_h + dh + h_count, h_count), 'w': lax.rem(me_w + dw + w_count, w_count)}

    barrier = pltpu.get_barrier_semaphore()
    others = [(dh, dw) for dh in (-1, 0, 1) for dw in (-1, 0, 1) if dh or dw]
    for dh, dw in others:
        pl.semaphore_signal(barrier, inc=1, device_id=device(dh, dw), device_id_type=MESH)

    for k in range(9):
        w36[4 * k:4 * k + 4, :] = dw1[k].astype(F32)
    picked = jnp.dot(sel[...], w36[...].astype(BF), preferred_element_type=F32).astype(BF)
    bw1[...] = jnp.concatenate([picked[j * 256:(j + 1) * 256] for j in range(8)], axis=1)
    build_weight(br1, rw1, REFINE1_K, 1)
    build_weight(bw2, dw2, DOWN2_K, 2)
    build_weight(br2, rw2, REFINE2_K, 1)
    build_weight(bw3, dw3, DOWN3_K, 2)
    build_weight(br3, rw3, REFINE3_K, 1)

    def halo(e, stage, buf, rows, groups, both):
        sems = (send_sem.at[e], recv_sem.at[e])
        if stage == 0:
            return Halo(stage, buf, rows, groups, both, send_x, recv_x, sems, device)
        if stage == 3:
            return Halo(stage, buf, rows, groups, both, None, None, sems, device)
        return Halo(stage, buf, rows, groups, both, send_c.at[e - 1], recv_c.at[e - 1], sems, device)

    pv_halo = halo(0, 0, pv, rows1, 8, False)
    y1_halo = halo(1, 1, y1, rows1, G, True)
    z1_halo = halo(2, 1, z1, rows1, G, False)
    y2_halo = halo(3, 2, y2, rows2, G, True)
    z2_halo = halo(4, 2, z2, rows2, G, False)
    y3_halo = halo(5, 3, y3, rows3, G, True)

    lane = lax.broadcasted_iota(jnp.int16, (N, 128), 1)

    def swap(v, dist, blocks):
        mask = (lane & dist) == 0
        new = list(v)
        for i in range(8):
            if not i & blocks:
                a, b = v[i], v[i + blocks]
                new[i] = jnp.where(mask, a, roll(b, dist))
                new[i + blocks] = jnp.where(mask, roll(a, -dist), b)
        return new

    def to_pairs(i, carry):
        for u in range(TILES):
            t = jnp.transpose(x[:, pl.ds((i * TILES + u) * 16, 16), :], (1, 0, 2))
            for p in range(2):
                v = [t[p * 8 + k] for k in range(8)]
                for dist, blocks in ((64, 4), (32, 2), (16, 1)):
                    v = swap(v, dist, blocks)
                pv[1 + 2 * (i * TILES + u) + p, pl.ds(1, 8)] = jnp.stack(v)
        return carry

    for i, (lo, hi) in enumerate(image_blocks):
        loads[i].wait()
        lax.fori_loop(lo // 2 // TILES, hi // 2 // TILES, to_pairs, 0)
        if i == 0:
            pl.semaphore_wait(barrier, len(others))
        pv_halo.send_cols(lo, hi, 0)
        pv_halo.send_rows(lo, hi)

    bias1 = tiled_bias(db1)

    def down1(lo, hi, q0, nq, per):
        per = min(per, hi - lo)
        size = per * nq * N

        def step(i, carry):
            row0 = lo + i * per
            sub = lax.broadcasted_iota(jnp.int16, (size, 128), 1) & 15
            own = flat(pv[pl.ds(row0 + 1, per), pl.ds(1 + q0, nq)])
            above = flat(pv[pl.ds(row0, per), pl.ds(1 + q0, nq)])
            left = flat(pv[pl.ds(row0 + 1, per), pl.ds(q0, nq)])
            above_left = flat(pv[pl.ds(row0, per), pl.ds(q0, nq)])
            edge = jnp.where(sub == 15, left, jnp.where(sub == 14, roll(left, 63), roll(above_left, 62)))
            second = jnp.concatenate([edge[:, :64], above[:, 64:]], axis=1)
            res = jnp.dot(jnp.concatenate([own, second], axis=1), bw1[...], preferred_element_type=F32)
            val = jnp.maximum(res + bias1, 0.0).astype(BF)
            pairs = pl.ds(lo // 2 + i * (per // 2) + 1, per // 2)
            for half in range(2):
                v = val[:, half * 128:(half + 1) * 128].reshape(per // 2, 2, nq, N, 128)
                for q in range(nq):
                    y1[pairs, :, 1 + 2 * (q0 + q) + half] = v[:, :, q]
            return carry

        lax.fori_loop(0, (hi - lo) // per, step, 0)

    for is_edge, (lo, hi) in schedule(row_blocks(rows1, 16, 32), 1):
        if is_edge:
            pv_halo.need_cols(lo - 1, hi)
            down1(lo, hi, 0, 1, 32)
            y1_halo.send_cols(lo, hi, 1)
            y1_halo.send_rows(lo, hi)
        else:
            pv_halo.need_rows(lo - 1, hi)
            down1(lo, hi, 1, 7, DOWN1_ROWS)
            y1_halo.send_cols(lo, hi, 0)

    def refine(stage, src, src_halo, weight, bias, dst, dst_halo, blocks, delay):
        lhs = functools.partial(refine_lhs, stage, src)
        for is_edge, (lo, hi) in schedule(blocks, delay):
            if is_edge:
                src_halo.need_cols(lo - 1, hi + 1)
                conv_rows(lhs, weight, bias, dst, lo, hi, [(0, 1), (G - 1, 1)], 16)
                if dst_halo is not None:
                    dst_halo.send_cols(lo, hi, 0)
                    dst_halo.send_rows(lo, hi)
            else:
                src_halo.need_rows(lo - 1, hi + 1)
                conv_rows(lhs, weight, bias, dst, lo, hi, [(1, G - 2)], PAIRS)

    def down(src, src_halo, weight, bias, dst, dst_halo, blocks, delay):
        lhs = functools.partial(down_lhs, src)
        for is_edge, (lo, hi) in schedule(blocks, delay):
            if is_edge:
                src_halo.need_cols(2 * lo - 1, 2 * hi)
                conv_rows(lhs, weight, bias, dst, lo, hi, [(0, 1)], 16)
                dst_halo.send_cols(lo, hi, 1)
                dst_halo.send_rows(lo, hi)
            else:
                src_halo.need_rows(2 * lo - 1, 2 * hi)
                conv_rows(lhs, weight, bias, dst, lo, hi, [(1, G - 1)], PAIRS)
                dst_halo.send_cols(lo, hi, 0)

    refine(1, y1, y1_halo, br1, tiled_bias(rb1), into_quads(z1), z1_halo, row_blocks(rows1, 24, 32), 1)
    down(z1, z1_halo, bw2, tiled_bias(db2), into_pairs(y2, 1), y2_halo, row_blocks(rows2, 16, 16), 1)
    refine(2, y2, y2_halo, br2, tiled_bias(rb2), into_quads(z2), z2_halo, row_blocks(rows2, 24, 16), 1)
    down(z2, z2_halo, bw3, tiled_bias(db3), into_pairs(y3, 1), y3_halo, row_blocks(rows3, 16, 8), 4)
    refine(3, y3, y3_halo, br3, tiled_bias(rb3), into_pairs(out, 0), None,
           [(4, rows3 - 4), (rows3 - 4, rows3), (0, 4)], 3)

    for h in (pv_halo, y1_halo, z1_halo, y2_halo, z2_halo, y3_halo):
        h.finish()


def encode(h_count, w_count, images, *params):
    rows1 = images.shape[1] // 2
    rows2, rows3 = rows1 // 2, rows1 // 4
    x = jnp.transpose(images, (0, 1, 3, 2)).reshape(N, rows1 * 8, 128)
    args = [x, jnp.asarray(first_weight_selector(), BF)]
    for i, p in enumerate(params):
        args.append(p.reshape(1, -1) if i % 2 else (p.reshape(9, 4, 32) if i == 0 else p))

    def act(*shape):
        return pltpu.VMEM(shape + (N, 128), BF)

    flops = 2 * 16 * rows1 * 64 * 32 * 9 * (4 + 32 + 16 + 32 + 16 + 32)
    out = pl.pallas_call(
        functools.partial(kernel, h_count, w_count, rows1),
        name='encoder',
        out_shape=jax.ShapeDtypeStruct((rows3 // 2, 2, G, N, 128), BF),
        in_specs=[pl.BlockSpec(memory_space=pl.ANY)] + [pl.BlockSpec(memory_space=pltpu.VMEM)] * (len(args) - 1),
        out_specs=pl.BlockSpec(memory_space=pltpu.VMEM),
        scratch_shapes=[
            pltpu.VMEM((N, rows1 * 8, 128), BF), act(rows1 + 1, 9),
            act(rows1 // 2 + 2, 2, G + 2), act(rows1 // 4 + 1, 4, G + 1),
            act(rows2 // 2 + 2, 2, G + 2), act(rows2 // 4 + 1, 4, G + 1), act(rows3 // 2 + 2, 2, G + 2),
            pltpu.VMEM((36, 32), F32), pltpu.VMEM((256, 256), BF), pltpu.VMEM((768, 256), BF), pltpu.VMEM((1024, 256), BF),
            pltpu.VMEM((1024, 256), BF), pltpu.VMEM((1024, 256), BF), pltpu.VMEM((1536, 256), BF),
            pltpu.VMEM((1, rows1 // 16, N, 128), BF), pltpu.VMEM((1, rows1 // 16, N, 128), BF),
            pltpu.VMEM((4, 2, rows1 // 4, N, 128), BF), pltpu.VMEM((4, 2, rows1 // 4, N, 128), BF),
            pltpu.SemaphoreType.DMA((8,)), pltpu.SemaphoreType.DMA((6, 20)), pltpu.SemaphoreType.DMA((6, 20)),
        ],
        compiler_params=pltpu.CompilerParams(
            collective_id=0, has_side_effects=True, vmem_limit_bytes=56 * 2**20),
        cost_estimate=pl.CostEstimate(flops=flops, bytes_accessed=7 * 2**20, transcendentals=0),
    )(*args)
    return jnp.transpose(out.reshape(rows3, G, N, 128), (2, 0, 1, 3))


def solution(mesh):
    tile_spec = P('batch', 'h', 'w', None)
    body = functools.partial(encode, mesh.shape['h'], mesh.shape['w'])
    return jax.shard_map(body, mesh=mesh, in_specs=(tile_spec,) + (P(),) * 12, out_specs=tile_spec, check_vma=False)
```

```python
import functools

import jax
import jax.numpy as jnp
import numpy as np
from jax import lax
from jax.experimental import pallas as pl
from jax.experimental.pallas import tpu as pltpu
from jax.sharding import PartitionSpec as P

BF = jnp.bfloat16
F32 = jnp.float32
N = 16
G = 16
TILES = 4
DOWN1_ROWS = 8
PAIRS = 4
UNROLL = 0
MESH = pl.DeviceIdType.MESH


def first_weight_selector():
    sel = np.zeros((8, 256, 36), np.float32)
    for j in range(8):
        for c in range(4):
            for wi in range(16):
                b = wi - 2 * j + 1
                if 0 <= b <= 2:
                    for hi in range(2):
                        sel[j, hi * 64 + c * 16 + wi, ((hi + 1) * 3 + b) * 4 + c] = 1
                    sel[j, 128 + 64 + c * 16 + wi, (0 * 3 + b) * 4 + c] = 1
            if j == 0:
                for a, wi in ((1, 15), (2, 14), (0, 13)):
                    sel[j, 128 + c * 16 + wi, (a * 3) * 4 + c] = 1
    return sel.reshape(8 * 256, 36)


def roll(v, shift):
    shift %= 128
    return v if shift == 0 else pltpu.roll(v, shift, v.ndim - 1)


def flat(v):
    return v.reshape(-1, 128)


def build_weight(big, w, k_blocks, stride):
    cin, cout = w.shape[2], w.shape[3]
    ncols = 128 // cout
    taps = [[w[a, b] for b in range(3)] for a in range(3)]
    zero = jnp.zeros((cin, cout), BF)
    for kp, pos in enumerate(k_blocks):
        pieces = []
        for orow in range(2):
            for j in range(ncols):
                piece = zero
                if pos is not None:
                    a, b = pos[0] - stride * orow, pos[1] - stride * j + 1
                    if 0 <= a <= 2 and 0 <= b <= 2:
                        piece = taps[a][b]
                pieces.append(piece)
        big[kp * cin:(kp + 1) * cin, :] = jnp.concatenate(pieces, axis=1)


REFINE1_K = ([(ir, ic) for ir in range(4) for ic in range(4)]
             + [p for e in (0, 2) for p in ((e, 4), (e + 1, -1), (e + 1, 4), (e, -1))])
REFINE2_K = ([(ir, ic) for ir in range(4) for ic in range(2)]
             + [p for ir in range(4) for p in ((ir, 2), (ir, -1))])
REFINE3_K = [(ir, ic) for ir in range(4) for ic in (-1, 0, 1)]
DOWN2_K = ([(ir, ic) for ir in range(5) for ic in range(4)]
           + [p for e in (0, 2) for p in (None, (e + 1, -1), None, (e, -1))]
           + [None, None, None, (4, -1)])
DOWN3_K = ([(ir, ic) for ir in range(5) for ic in range(2)]
           + [p for e in (0, 2) for p in ((e + 1, -1), (e, -1))] + [None, (4, -1)])


def tiled_bias(b):
    reps = 128 // b.shape[1]
    return jnp.concatenate([b[...]] * (2 * reps), axis=1)


def refine_lhs(stage, src, p0, pairs, g0, ng):
    def rows(h, g):
        return flat(src[pl.ds(p0 + (h + 1) // 2, pairs), (h + 1) % 2, pl.ds(g, ng)])

    def own(h):
        return rows(h, 1 + g0)

    def left(h):
        return rows(h, g0)

    def right(h):
        return rows(h, 2 + g0)

    def edge(h):
        return jnp.concatenate([right(h)[:, :64], left(h)[:, 64:]], axis=1)

    if stage == 3:
        return [f(h) for h in range(4) for f in (left, own, right)]
    if stage == 2:
        return [own(h) for h in range(4)] + [edge(h) for h in range(4)]
    ks = [own(h) for h in range(4)]
    for h in (0, 2):
        f0, f1 = edge(h), roll(edge(h + 1), 64)
        ks.append(jnp.concatenate([f0[:, :32], f1[:, 32:96], f0[:, 96:]], axis=1))
    return ks


def down_lhs(src, p0, pairs, g0, ng):
    def rows(h, g):
        return flat(src[pl.ds(p0 + (h + 3) // 4, pairs), (h + 3) % 4, pl.ds(g, ng)])

    def own(h):
        return rows(h, 1 + g0)

    def left(h):
        return rows(h, g0)

    ks = [own(h) for h in range(5)]
    for h in (0, 2):
        ks.append(jnp.concatenate([roll(left(h + 1), 64)[:, :64], left(h)[:, 64:]], axis=1))
    return ks + [left(4)]


def unrolled(count, step):
    trips = count // UNROLL if UNROLL else 1
    each = UNROLL or count
    if trips <= 1:
        for i in range(count):
            step(i, 0)
        return

    def trip(t, carry):
        for u in range(each):
            step(t * each + u, 0)
        return carry

    lax.fori_loop(0, trips, trip, 0)
    for i in range(trips * each, count):
        step(i, 0)


def conv_rows(lhs, weight, bias, dst, lo, hi, ranges, pairs):
    pairs = min(pairs, (hi - lo) // 2)

    def step(i, carry):
        p0 = lo // 2 + i * pairs
        parts = [lhs(p0, pairs, g0, ng) for g0, ng in ranges]
        ks = [jnp.concatenate(part, axis=0) if len(ranges) > 1 else part[0] for part in zip(*parts)]
        res = jnp.dot(jnp.concatenate(ks, axis=1), weight[...], preferred_element_type=F32)
        val = jnp.maximum(res + bias, 0.0).astype(BF)
        at = 0
        for g0, ng in ranges:
            size = pairs * ng * N
            tile = val[at:at + size]
            at += size
            dst(lo // 4 + i * (pairs // 2), p0, pairs, g0, ng, tile)
        return carry

    unrolled((hi - lo) // (2 * pairs), step)


def into_pairs(buf, shift):
    def dst(quad0, p0, pairs, g0, ng, tile):
        for half in range(2):
            buf[pl.ds(p0 + shift, pairs), half, pl.ds(g0 + shift, ng)] = (
                tile[:, half * 128:(half + 1) * 128].reshape(pairs, ng, N, 128))
    return dst


def into_quads(buf):
    def dst(quad0, p0, pairs, g0, ng, tile):
        for half in range(2):
            v = tile[:, half * 128:(half + 1) * 128].reshape(pairs // 2, 2, ng, N, 128)
            for odd in range(2):
                buf[pl.ds(quad0 + 1, pairs // 2), 2 * odd + half, pl.ds(1 + g0, ng)] = v[:, odd]
    return dst


def pack_cols(stage, buf, lo, hi, right_edge):
    view = buf.shape[1]
    col = buf[pl.ds(lo // view + 1, (hi - lo) // view), :, G if right_edge else 1]
    per = 4 if stage == 1 else 2
    width = 128 // per
    col = col.reshape((hi - lo) // per, per, N, 128)
    base = 128 - width if right_edge else 0
    parts = []
    for k in range(per):
        v = roll(flat(col[:, k]), k * width - base)
        parts.append(v[:, k * width:(k + 1) * width])
    return jnp.concatenate(parts, axis=1).reshape((hi - lo) // per, N, 128)


def unpack_cols(stage, buf, lo, hi, packed, left_halo):
    view = buf.shape[1]
    per = 4 if stage == 1 else 2
    width = 128 // per
    base = 128 - width if left_halo else 0
    tiles = flat(packed)
    rows = [roll(tiles, base - k * width).reshape(-1, N, 128) for k in range(per)]
    buf[pl.ds(lo // view + 1, (hi - lo) // view), :, 0 if left_halo else G + 1] = (
        jnp.stack(rows, axis=1).reshape((hi - lo) // view, view, N, 128))


def pack_image(pv, lo, hi):
    rows = hi - lo
    col = pv[pl.ds(1 + lo, rows), 8].reshape(rows // 16, 16, N, 128)
    lanes = lax.broadcasted_iota(jnp.int16, (rows, 128), 1) & 15
    packed = flat(col[:, 15])
    for k in range(15):
        packed = jnp.where(lanes == k, roll(flat(col[:, k]), k - 15), packed)
    return packed.reshape(rows // 16, N, 128)


def unpack_image(pv, lo, hi, packed):
    tiles = flat(packed)
    rows = [roll(tiles, 15 - k).reshape(-1, N, 128) for k in range(16)]
    pv[pl.ds(1 + lo, hi - lo), 0] = jnp.stack(rows, axis=1).reshape(hi - lo, N, 128)


def row_blocks(rows, start, size):
    out = [(lo, min(lo + size, rows)) for lo in range(start, rows, size)]
    return out + [(lo, min(lo + size, start)) for lo in range(0, start, size)]


class Halo:
    def __init__(self, stage, buf, rows, groups, both, send_c, recv_c, sems, device):
        self.stage, self.buf, self.rows, self.groups, self.both = stage, buf, rows, groups, both
        self.send_c, self.recv_c, self.sems, self.device = send_c, recv_c, sems, device
        self.count, self.sent, self.chunks = 0, [], []
        self.slabs, self.corners = {'top': [], 'bottom': []}, {'top': [], 'bottom': []}

    def copy(self, src, dst, direction):
        send_sem, recv_sem = self.sems
        c = pltpu.make_async_remote_copy(
            src_ref=src, dst_ref=dst, send_sem=send_sem.at[self.count], recv_sem=recv_sem.at[self.count],
            device_id=self.device(*direction), device_id_type=MESH)
        self.count += 1
        self.sent.append(c)
        c.start()
        return c

    def send_cols(self, lo, hi, side):
        buf, stage = self.buf, self.stage
        if stage == 3:
            part = pl.ds(lo // 2 + 1, (hi - lo) // 2)
            src = buf.at[part, :, G if side == 0 else 1]
            dst = buf.at[part, :, 0 if side == 0 else G + 1]
        else:
            per = {0: 16, 1: 4, 2: 2}[stage]
            part = pl.ds(lo // per, (hi - lo) // per)
            self.send_c[side, part] = (
                pack_image(buf, lo, hi) if stage == 0 else pack_cols(stage, buf, lo, hi, side == 0))
            src, dst = self.send_c.at[side, part], self.recv_c.at[side, part]
        self.chunks.append((lo, hi, side, self.copy(src, dst, (0, 1 if side == 0 else -1))))

    def cells(self, row, groups):
        view = self.buf.shape[1] if self.stage else 1
        at = (row // view + 1, row % view) if self.stage else (row + 1,)
        return self.buf.at[at + (groups,)]

    def send_rows(self, lo, hi):
        last, ng, cells = self.rows - 1, self.groups, self.cells
        every = pl.ds(1, ng)
        if hi == self.rows:
            self.slabs['top'].append(self.copy(cells(last, every), cells(-1, every), (1, 0)))
            self.corners['top'].append(self.copy(cells(last, ng), cells(-1, 0), (1, 1)))
            if self.both:
                self.corners['top'].append(self.copy(cells(last, 1), cells(-1, ng + 1), (1, -1)))
        if lo == 0 and self.both:
            self.slabs['bottom'].append(self.copy(cells(0, every), cells(last + 1, every), (-1, 0)))
            self.corners['bottom'].append(self.copy(cells(0, ng), cells(last + 1, 0), (-1, 1)))
            self.corners['bottom'].append(self.copy(cells(0, 1), cells(last + 1, ng + 1), (-1, -1)))

    def ends(self, which, lo, hi):
        for end, wanted in (('top', lo < 0), ('bottom', hi > self.rows)):
            if wanted:
                for c in which[end]:
                    c.wait_recv()
                which[end] = []

    def need_rows(self, lo, hi):
        self.ends(self.slabs, lo, hi)

    def need_cols(self, lo, hi):
        left = []
        for chunk in self.chunks:
            first, end, side, c = chunk
            if first < hi and lo < end:
                c.wait_recv()
                if self.stage != 3:
                    per = {0: 16, 1: 4, 2: 2}[self.stage]
                    packed = self.recv_c[side, pl.ds(first // per, (end - first) // per)]
                    if self.stage == 0:
                        unpack_image(self.buf, first, end, packed)
                    else:
                        unpack_cols(self.stage, self.buf, first, end, packed, side == 0)
            else:
                left.append(chunk)
        self.chunks = left
        self.ends(self.corners, lo, hi)

    def finish(self):
        assert not self.chunks and not any(self.slabs.values()) and not any(self.corners.values())
        for c in self.sent:
            c.wait_send()


def schedule(blocks, delay):
    out = []
    for i in range(len(blocks) + delay):
        if i < len(blocks):
            out.append((False, blocks[i]))
        if i >= delay and i - delay < len(blocks):
            out.append((True, blocks[i - delay]))
    return out


def kernel(h_count, w_count, rows1, x_hbm, sel, dw1, db1, rw1, rb1, dw2, db2, rw2, rb2, dw3, db3, rw3, rb3, out,
           x, pv, y1, z1, y2, z2, y3, w36, bw1, br1, bw2, br2, bw3, br3,
           send_x, recv_x, send_c, recv_c, x_sem, send_sem, recv_sem):
    rows2, rows3 = rows1 // 2, rows1 // 4
    me_h, me_w = lax.axis_index('h'), lax.axis_index('w')

    image_blocks = row_blocks(rows1, 0, 32)
    loads = []
    for i, (lo, hi) in enumerate(image_blocks):
        part = pl.ds(lo * 8, (hi - lo) * 8)
        loads.append(pltpu.make_async_copy(x_hbm.at[:, part], x.at[:, part], x_sem.at[i]))
        loads[-1].start()

    def device(dh, dw):
        return {'h': lax.rem(me_h + dh + h_count, h_count), 'w': lax.rem(me_w + dw + w_count, w_count)}

    barrier = pltpu.get_barrier_semaphore()
    others = [(dh, dw) for dh in (-1, 0, 1) for dw in (-1, 0, 1) if dh or dw]
    for dh, dw in others:
        pl.semaphore_signal(barrier, inc=1, device_id=device(dh, dw), device_id_type=MESH)

    for k in range(9):
        w36[4 * k:4 * k + 4, :] = dw1[k].astype(F32)
    picked = jnp.dot(sel[...], w36[...].astype(BF), preferred_element_type=F32).astype(BF)
    bw1[...] = jnp.concatenate([picked[j * 256:(j + 1) * 256] for j in range(8)], axis=1)
    build_weight(br1, rw1, REFINE1_K, 1)
    build_weight(bw2, dw2, DOWN2_K, 2)
    build_weight(br2, rw2, REFINE2_K, 1)
    build_weight(bw3, dw3, DOWN3_K, 2)
    build_weight(br3, rw3, REFINE3_K, 1)

    def halo(e, stage, buf, rows, groups, both):
        sems = (send_sem.at[e], recv_sem.at[e])
        if stage == 0:
            return Halo(stage, buf, rows, groups, both, send_x, recv_x, sems, device)
        if stage == 3:
            return Halo(stage, buf, rows, groups, both, None, None, sems, device)
        return Halo(stage, buf, rows, groups, both, send_c.at[e - 1], recv_c.at[e - 1], sems, device)

    pv_halo = halo(0, 0, pv, rows1, 8, False)
    y1_halo = halo(1, 1, y1, rows1, G, True)
    z1_halo = halo(2, 1, z1, rows1, G, False)
    y2_halo = halo(3, 2, y2, rows2, G, True)
    z2_halo = halo(4, 2, z2, rows2, G, False)
    y3_halo = halo(5, 3, y3, rows3, G, True)

    lane = lax.broadcasted_iota(jnp.int16, (N, 128), 1)

    def swap(v, dist, blocks):
        mask = (lane & dist) == 0
        new = list(v)
        for i in range(8):
            if not i & blocks:
                a, b = v[i], v[i + blocks]
                new[i] = jnp.where(mask, a, roll(b, dist))
                new[i + blocks] = jnp.where(mask, roll(a, -dist), b)
        return new

    def to_pairs(i, carry):
        for u in range(TILES):
            t = jnp.transpose(x[:, pl.ds((i * TILES + u) * 16, 16), :], (1, 0, 2))
            for p in range(2):
                v = [t[p * 8 + k] for k in range(8)]
                for dist, blocks in ((64, 4), (32, 2), (16, 1)):
                    v = swap(v, dist, blocks)
                pv[1 + 2 * (i * TILES + u) + p, pl.ds(1, 8)] = jnp.stack(v)
        return carry

    for i, (lo, hi) in enumerate(image_blocks):
        loads[i].wait()
        lax.fori_loop(lo // 2 // TILES, hi // 2 // TILES, to_pairs, 0)
        if i == 0:
            pl.semaphore_wait(barrier, len(others))
        pv_halo.send_cols(lo, hi, 0)
        pv_halo.send_rows(lo, hi)

    bias1 = tiled_bias(db1)

    def down1(lo, hi, q0, nq, per):
        per = min(per, hi - lo)
        size = per * nq * N

        def step(i, carry):
            row0 = lo + i * per
            sub = lax.broadcasted_iota(jnp.int16, (size, 128), 1) & 15
            own = flat(pv[pl.ds(row0 + 1, per), pl.ds(1 + q0, nq)])
            above = flat(pv[pl.ds(row0, per), pl.ds(1 + q0, nq)])
            left = flat(pv[pl.ds(row0 + 1, per), pl.ds(q0, nq)])
            above_left = flat(pv[pl.ds(row0, per), pl.ds(q0, nq)])
            edge = jnp.where(sub == 15, left, jnp.where(sub == 14, roll(left, 63), roll(above_left, 62)))
            second = jnp.concatenate([edge[:, :64], above[:, 64:]], axis=1)
            res = jnp.dot(jnp.concatenate([own, second], axis=1), bw1[...], preferred_element_type=F32)
            val = jnp.maximum(res + bias1, 0.0).astype(BF)
            pairs = pl.ds(lo // 2 + i * (per // 2) + 1, per // 2)
            for half in range(2):
                v = val[:, half * 128:(half + 1) * 128].reshape(per // 2, 2, nq, N, 128)
                for q in range(nq):
                    y1[pairs, :, 1 + 2 * (q0 + q) + half] = v[:, :, q]
            return carry

        unrolled((hi - lo) // per, step)

    for is_edge, (lo, hi) in schedule(row_blocks(rows1, 16, 32), 1):
        if is_edge:
            pv_halo.need_cols(lo - 1, hi)
            down1(lo, hi, 0, 1, 32)
            y1_halo.send_cols(lo, hi, 1)
            y1_halo.send_rows(lo, hi)
        else:
            pv_halo.need_rows(lo - 1, hi)
            down1(lo, hi, 1, 7, DOWN1_ROWS)
            y1_halo.send_cols(lo, hi, 0)

    def refine(stage, src, src_halo, weight, bias, dst, dst_halo, blocks, delay):
        lhs = functools.partial(refine_lhs, stage, src)
        for is_edge, (lo, hi) in schedule(blocks, delay):
            if is_edge:
                src_halo.need_cols(lo - 1, hi + 1)
                conv_rows(lhs, weight, bias, dst, lo, hi, [(0, 1), (G - 1, 1)], 16)
                if dst_halo is not None:
                    dst_halo.send_cols(lo, hi, 0)
                    dst_halo.send_rows(lo, hi)
            else:
                src_halo.need_rows(lo - 1, hi + 1)
                conv_rows(lhs, weight, bias, dst, lo, hi, [(1, G - 2)], PAIRS)

    def down(src, src_halo, weight, bias, dst, dst_halo, blocks, delay):
        lhs = functools.partial(down_lhs, src)
        for is_edge, (lo, hi) in schedule(blocks, delay):
            if is_edge:
                src_halo.need_cols(2 * lo - 1, 2 * hi)
                conv_rows(lhs, weight, bias, dst, lo, hi, [(0, 1)], 16)
                dst_halo.send_cols(lo, hi, 1)
                dst_halo.send_rows(lo, hi)
            else:
                src_halo.need_rows(2 * lo - 1, 2 * hi)
                conv_rows(lhs, weight, bias, dst, lo, hi, [(1, G - 1)], PAIRS)
                dst_halo.send_cols(lo, hi, 0)

    refine(1, y1, y1_halo, br1, tiled_bias(rb1), into_quads(z1), z1_halo, row_blocks(rows1, 24, 32), 1)
    down(z1, z1_halo, bw2, tiled_bias(db2), into_pairs(y2, 1), y2_halo, row_blocks(rows2, 16, 16), 1)
    refine(2, y2, y2_halo, br2, tiled_bias(rb2), into_quads(z2), z2_halo, row_blocks(rows2, 24, 16), 1)
    down(z2, z2_halo, bw3, tiled_bias(db3), into_pairs(y3, 1), y3_halo, row_blocks(rows3, 16, 8), 4)
    refine(3, y3, y3_halo, br3, tiled_bias(rb3), into_pairs(out, 0), None,
           [(4, rows3 - 4), (rows3 - 4, rows3), (0, 4)], 3)

    for h in (pv_halo, y1_halo, z1_halo, y2_halo, z2_halo, y3_halo):
        h.finish()


def encode(h_count, w_count, images, *params):
    rows1 = images.shape[1] // 2
    rows2, rows3 = rows1 // 2, rows1 // 4
    x = jnp.transpose(images, (0, 1, 3, 2)).reshape(N, rows1 * 8, 128)
    args = [x, jnp.asarray(first_weight_selector(), BF)]
    for i, p in enumerate(params):
        args.append(p.reshape(1, -1) if i % 2 else (p.reshape(9, 4, 32) if i == 0 else p))

    def act(*shape):
        return pltpu.VMEM(shape + (N, 128), BF)

    flops = 2 * 16 * rows1 * 64 * 32 * 9 * (4 + 32 + 16 + 32 + 16 + 32)
    out = pl.pallas_call(
        functools.partial(kernel, h_count, w_count, rows1),
        name='encoder',
        out_shape=jax.ShapeDtypeStruct((rows3 // 2, 2, G, N, 128), BF),
        in_specs=[pl.BlockSpec(memory_space=pl.ANY)] + [pl.BlockSpec(memory_space=pltpu.VMEM)] * (len(args) - 1),
        out_specs=pl.BlockSpec(memory_space=pltpu.VMEM),
        scratch_shapes=[
            pltpu.VMEM((N, rows1 * 8, 128), BF), act(rows1 + 1, 9),
            act(rows1 // 2 + 2, 2, G + 2), act(rows1 // 4 + 1, 4, G + 1),
            act(rows2 // 2 + 2, 2, G + 2), act(rows2 // 4 + 1, 4, G + 1), act(rows3 // 2 + 2, 2, G + 2),
            pltpu.VMEM((36, 32), F32), pltpu.VMEM((256, 256), BF), pltpu.VMEM((768, 256), BF), pltpu.VMEM((1024, 256), BF),
            pltpu.VMEM((1024, 256), BF), pltpu.VMEM((1024, 256), BF), pltpu.VMEM((1536, 256), BF),
            pltpu.VMEM((1, rows1 // 16, N, 128), BF), pltpu.VMEM((1, rows1 // 16, N, 128), BF),
            pltpu.VMEM((4, 2, rows1 // 4, N, 128), BF), pltpu.VMEM((4, 2, rows1 // 4, N, 128), BF),
            pltpu.SemaphoreType.DMA((8,)), pltpu.SemaphoreType.DMA((6, 20)), pltpu.SemaphoreType.DMA((6, 20)),
        ],
        compiler_params=pltpu.CompilerParams(
            collective_id=0, has_side_effects=True, vmem_limit_bytes=56 * 2**20),
        cost_estimate=pl.CostEstimate(flops=flops, bytes_accessed=7 * 2**20, transcendentals=0),
    )(*args)
    return jnp.transpose(out.reshape(rows3, G, N, 128), (2, 0, 1, 3))


def solution(mesh):
    tile_spec = P('batch', 'h', 'w', None)
    body = functools.partial(encode, mesh.shape['h'], mesh.shape['w'])
    return jax.shard_map(body, mesh=mesh, in_specs=(tile_spec,) + (P(),) * 12, out_specs=tile_spec, check_vma=False)
```

```python
import functools

import jax
import jax.numpy as jnp
import numpy as np
from jax import lax
from jax.experimental import pallas as pl
from jax.experimental.pallas import tpu as pltpu
from jax.sharding import PartitionSpec as P

BF = jnp.bfloat16
F32 = jnp.float32
N = 16
G = 16
TILES = 4
DOWN1_ROWS = 8
PAIRS = 4
UNROLL = 0
MESH = pl.DeviceIdType.MESH


def first_weight_selector():
    sel = np.zeros((8, 256, 36), np.float32)
    for j in range(8):
        for c in range(4):
            for wi in range(16):
                b = wi - 2 * j + 1
                if 0 <= b <= 2:
                    for hi in range(2):
                        sel[j, hi * 64 + c * 16 + wi, ((hi + 1) * 3 + b) * 4 + c] = 1
                    sel[j, 128 + 64 + c * 16 + wi, (0 * 3 + b) * 4 + c] = 1
            if j == 0:
                for a, wi in ((1, 15), (2, 14), (0, 13)):
                    sel[j, 128 + c * 16 + wi, (a * 3) * 4 + c] = 1
    return sel.reshape(8 * 256, 36)


def roll(v, shift):
    shift %= 128
    return v if shift == 0 else pltpu.roll(v, shift, v.ndim - 1)


def flat(v):
    return v.reshape(-1, 128)


def build_weight(big, w, k_blocks, stride):
    cin, cout = w.shape[2], w.shape[3]
    ncols = 128 // cout
    taps = [[w[a, b] for b in range(3)] for a in range(3)]
    zero = jnp.zeros((cin, cout), BF)
    for kp, pos in enumerate(k_blocks):
        pieces = []
        for orow in range(2):
            for j in range(ncols):
                piece = zero
                if pos is not None:
                    a, b = pos[0] - stride * orow, pos[1] - stride * j + 1
                    if 0 <= a <= 2 and 0 <= b <= 2:
                        piece = taps[a][b]
                pieces.append(piece)
        big[kp * cin:(kp + 1) * cin, :] = jnp.concatenate(pieces, axis=1)


REFINE1_K = ([(ir, ic) for ir in range(4) for ic in range(4)]
             + [p for e in (0, 2) for p in ((e, 4), (e + 1, -1), (e + 1, 4), (e, -1))])
REFINE2_K = ([(ir, ic) for ir in range(4) for ic in range(2)]
             + [p for ir in range(4) for p in ((ir, 2), (ir, -1))])
REFINE3_K = [(ir, ic) for ir in range(4) for ic in (-1, 0, 1)]
DOWN2_K = ([(ir, ic) for ir in range(5) for ic in range(4)]
           + [p for e in (0, 2) for p in (None, (e + 1, -1), None, (e, -1))]
           + [None, None, None, (4, -1)])
DOWN3_K = ([(ir, ic) for ir in range(5) for ic in range(2)]
           + [p for e in (0, 2) for p in ((e + 1, -1), (e, -1))] + [None, (4, -1)])


def tiled_bias(b):
    reps = 128 // b.shape[1]
    return jnp.concatenate([b[...]] * (2 * reps), axis=1)


def refine_lhs(stage, src, p0, pairs, g0, ng):
    def rows(h, g):
        return flat(src[pl.ds(p0 + (h + 1) // 2, pairs), (h + 1) % 2, pl.ds(g, ng)])

    def own(h):
        return rows(h, 1 + g0)

    def left(h):
        return rows(h, g0)

    def right(h):
        return rows(h, 2 + g0)

    def edge(h):
        return jnp.concatenate([right(h)[:, :64], left(h)[:, 64:]], axis=1)

    if stage == 3:
        return [f(h) for h in range(4) for f in (left, own, right)]
    if stage == 2:
        return [own(h) for h in range(4)] + [edge(h) for h in range(4)]
    ks = [own(h) for h in range(4)]
    for h in (0, 2):
        f0, f1 = edge(h), roll(edge(h + 1), 64)
        ks.append(jnp.concatenate([f0[:, :32], f1[:, 32:96], f0[:, 96:]], axis=1))
    return ks


def down_lhs(src, p0, pairs, g0, ng):
    def rows(h, g):
        return flat(src[pl.ds(p0 + (h + 3) // 4, pairs), (h + 3) % 4, pl.ds(g, ng)])

    def own(h):
        return rows(h, 1 + g0)

    def left(h):
        return rows(h, g0)

    ks = [own(h) for h in range(5)]
    for h in (0, 2):
        ks.append(jnp.concatenate([roll(left(h + 1), 64)[:, :64], left(h)[:, 64:]], axis=1))
    return ks + [left(4)]


def divisor(count, most):
    return next(d for d in range(min(most, count), 0, -1) if count % d == 0 and d % 2 == 0)


def unrolled(count, step):
    trips = count // UNROLL if UNROLL else 1
    each = UNROLL or count
    if trips <= 1:
        for i in range(count):
            step(i, 0)
        return

    def trip(t, carry):
        for u in range(each):
            step(t * each + u, 0)
        return carry

    lax.fori_loop(0, trips, trip, 0)
    for i in range(trips * each, count):
        step(i, 0)


def conv_rows(lhs, weight, bias, dst, lo, hi, ranges, pairs):
    pairs = divisor((hi - lo) // 2, pairs)

    def step(i, carry):
        p0 = lo // 2 + i * pairs
        parts = [lhs(p0, pairs, g0, ng) for g0, ng in ranges]
        ks = [jnp.concatenate(part, axis=0) if len(ranges) > 1 else part[0] for part in zip(*parts)]
        res = jnp.dot(jnp.concatenate(ks, axis=1), weight[...], preferred_element_type=F32)
        val = jnp.maximum(res + bias, 0.0).astype(BF)
        at = 0
        for g0, ng in ranges:
            size = pairs * ng * N
            tile = val[at:at + size]
            at += size
            dst(lo // 4 + i * (pairs // 2), p0, pairs, g0, ng, tile)
        return carry

    unrolled((hi - lo) // (2 * pairs), step)


def into_pairs(buf, shift):
    def dst(quad0, p0, pairs, g0, ng, tile):
        for half in range(2):
            buf[pl.ds(p0 + shift, pairs), half, pl.ds(g0 + shift, ng)] = (
                tile[:, half * 128:(half + 1) * 128].reshape(pairs, ng, N, 128))
    return dst


def into_quads(buf):
    def dst(quad0, p0, pairs, g0, ng, tile):
        for half in range(2):
            v = tile[:, half * 128:(half + 1) * 128].reshape(pairs // 2, 2, ng, N, 128)
            for odd in range(2):
                buf[pl.ds(quad0 + 1, pairs // 2), 2 * odd + half, pl.ds(1 + g0, ng)] = v[:, odd]
    return dst


def pack_cols(stage, buf, lo, hi, right_edge):
    view = buf.shape[1]
    col = buf[pl.ds(lo // view + 1, (hi - lo) // view), :, G if right_edge else 1]
    per = 4 if stage == 1 else 2
    width = 128 // per
    col = col.reshape((hi - lo) // per, per, N, 128)
    base = 128 - width if right_edge else 0
    parts = []
    for k in range(per):
        v = roll(flat(col[:, k]), k * width - base)
        parts.append(v[:, k * width:(k + 1) * width])
    return jnp.concatenate(parts, axis=1).reshape((hi - lo) // per, N, 128)


def unpack_cols(stage, buf, lo, hi, packed, left_halo):
    view = buf.shape[1]
    per = 4 if stage == 1 else 2
    width = 128 // per
    base = 128 - width if left_halo else 0
    tiles = flat(packed)
    rows = [roll(tiles, base - k * width).reshape(-1, N, 128) for k in range(per)]
    buf[pl.ds(lo // view + 1, (hi - lo) // view), :, 0 if left_halo else G + 1] = (
        jnp.stack(rows, axis=1).reshape((hi - lo) // view, view, N, 128))


def pack_image(pv, lo, hi):
    rows = hi - lo
    col = pv[pl.ds(1 + lo, rows), 8].reshape(rows // 16, 16, N, 128)
    lanes = lax.broadcasted_iota(jnp.int16, (rows, 128), 1) & 15
    packed = flat(col[:, 15])
    for k in range(15):
        packed = jnp.where(lanes == k, roll(flat(col[:, k]), k - 15), packed)
    return packed.reshape(rows // 16, N, 128)


def unpack_image(pv, lo, hi, packed):
    tiles = flat(packed)
    rows = [roll(tiles, 15 - k).reshape(-1, N, 128) for k in range(16)]
    pv[pl.ds(1 + lo, hi - lo), 0] = jnp.stack(rows, axis=1).reshape(hi - lo, N, 128)


def row_blocks(rows, start, size):
    out = [(lo, min(lo + size, rows)) for lo in range(start, rows, size)]
    return out + [(lo, min(lo + size, start)) for lo in range(0, start, size)]


class Halo:
    def __init__(self, stage, buf, rows, groups, both, send_c, recv_c, sems, device):
        self.stage, self.buf, self.rows, self.groups, self.both = stage, buf, rows, groups, both
        self.send_c, self.recv_c, self.sems, self.device = send_c, recv_c, sems, device
        self.count, self.sent, self.chunks = 0, [], []
        self.slabs, self.corners = {'top': [], 'bottom': []}, {'top': [], 'bottom': []}

    def copy(self, src, dst, direction):
        send_sem, recv_sem = self.sems
        c = pltpu.make_async_remote_copy(
            src_ref=src, dst_ref=dst, send_sem=send_sem.at[self.count], recv_sem=recv_sem.at[self.count],
            device_id=self.device(*direction), device_id_type=MESH)
        self.count += 1
        self.sent.append(c)
        c.start()
        return c

    def send_cols(self, lo, hi, side):
        buf, stage = self.buf, self.stage
        if stage == 3:
            part = pl.ds(lo // 2 + 1, (hi - lo) // 2)
            src = buf.at[part, :, G if side == 0 else 1]
            dst = buf.at[part, :, 0 if side == 0 else G + 1]
        else:
            per = {0: 16, 1: 4, 2: 2}[stage]
            part = pl.ds(lo // per, (hi - lo) // per)
            self.send_c[side, part] = (
                pack_image(buf, lo, hi) if stage == 0 else pack_cols(stage, buf, lo, hi, side == 0))
            src, dst = self.send_c.at[side, part], self.recv_c.at[side, part]
        self.chunks.append((lo, hi, side, self.copy(src, dst, (0, 1 if side == 0 else -1))))

    def cells(self, row, groups):
        view = self.buf.shape[1] if self.stage else 1
        at = (row // view + 1, row % view) if self.stage else (row + 1,)
        return self.buf.at[at + (groups,)]

    def send_rows(self, lo, hi):
        last, ng, cells = self.rows - 1, self.groups, self.cells
        every = pl.ds(1, ng)
        if hi == self.rows:
            self.slabs['top'].append(self.copy(cells(last, every), cells(-1, every), (1, 0)))
            self.corners['top'].append(self.copy(cells(last, ng), cells(-1, 0), (1, 1)))
            if self.both:
                self.corners['top'].append(self.copy(cells(last, 1), cells(-1, ng + 1), (1, -1)))
        if lo == 0 and self.both:
            self.slabs['bottom'].append(self.copy(cells(0, every), cells(last + 1, every), (-1, 0)))
            self.corners['bottom'].append(self.copy(cells(0, ng), cells(last + 1, 0), (-1, 1)))
            self.corners['bottom'].append(self.copy(cells(0, 1), cells(last + 1, ng + 1), (-1, -1)))

    def ends(self, which, lo, hi):
        for end, wanted in (('top', lo < 0), ('bottom', hi > self.rows)):
            if wanted:
                for c in which[end]:
                    c.wait_recv()
                which[end] = []

    def need_rows(self, lo, hi):
        self.ends(self.slabs, lo, hi)

    def need_cols(self, lo, hi):
        left = []
        for chunk in self.chunks:
            first, end, side, c = chunk
            if first < hi and lo < end:
                c.wait_recv()
                if self.stage != 3:
                    per = {0: 16, 1: 4, 2: 2}[self.stage]
                    packed = self.recv_c[side, pl.ds(first // per, (end - first) // per)]
                    if self.stage == 0:
                        unpack_image(self.buf, first, end, packed)
                    else:
                        unpack_cols(self.stage, self.buf, first, end, packed, side == 0)
            else:
                left.append(chunk)
        self.chunks = left
        self.ends(self.corners, lo, hi)

    def finish(self):
        assert not self.chunks and not any(self.slabs.values()) and not any(self.corners.values())
        for c in self.sent:
            c.wait_send()


def schedule(blocks, delay):
    out = []
    for i in range(len(blocks) + delay):
        if i < len(blocks):
            out.append((False, blocks[i]))
        if i >= delay and i - delay < len(blocks):
            out.append((True, blocks[i - delay]))
    return out


def kernel(h_count, w_count, rows1, x_hbm, sel, dw1, db1, rw1, rb1, dw2, db2, rw2, rb2, dw3, db3, rw3, rb3, out,
           x, pv, y1, z1, y2, z2, y3, w36, bw1, br1, bw2, br2, bw3, br3,
           send_x, recv_x, send_c, recv_c, x_sem, send_sem, recv_sem):
    rows2, rows3 = rows1 // 2, rows1 // 4
    me_h, me_w = lax.axis_index('h'), lax.axis_index('w')

    image_blocks = row_blocks(rows1, 0, 32)
    loads = []
    for i, (lo, hi) in enumerate(image_blocks):
        part = pl.ds(lo * 8, (hi - lo) * 8)
        loads.append(pltpu.make_async_copy(x_hbm.at[:, part], x.at[:, part], x_sem.at[i]))
        loads[-1].start()

    def device(dh, dw):
        return {'h': lax.rem(me_h + dh + h_count, h_count), 'w': lax.rem(me_w + dw + w_count, w_count)}

    barrier = pltpu.get_barrier_semaphore()
    others = [(dh, dw) for dh in (-1, 0, 1) for dw in (-1, 0, 1) if dh or dw]
    for dh, dw in others:
        pl.semaphore_signal(barrier, inc=1, device_id=device(dh, dw), device_id_type=MESH)

    for k in range(9):
        w36[4 * k:4 * k + 4, :] = dw1[k].astype(F32)
    picked = jnp.dot(sel[...], w36[...].astype(BF), preferred_element_type=F32).astype(BF)
    bw1[...] = jnp.concatenate([picked[j * 256:(j + 1) * 256] for j in range(8)], axis=1)
    build_weight(br1, rw1, REFINE1_K, 1)
    build_weight(bw2, dw2, DOWN2_K, 2)
    build_weight(br2, rw2, REFINE2_K, 1)
    build_weight(bw3, dw3, DOWN3_K, 2)
    build_weight(br3, rw3, REFINE3_K, 1)

    def halo(e, stage, buf, rows, groups, both):
        sems = (send_sem.at[e], recv_sem.at[e])
        if stage == 0:
            return Halo(stage, buf, rows, groups, both, send_x, recv_x, sems, device)
        if stage == 3:
            return Halo(stage, buf, rows, groups, both, None, None, sems, device)
        return Halo(stage, buf, rows, groups, both, send_c.at[e - 1], recv_c.at[e - 1], sems, device)

    pv_halo = halo(0, 0, pv, rows1, 8, False)
    y1_halo = halo(1, 1, y1, rows1, G, True)
    z1_halo = halo(2, 1, z1, rows1, G, False)
    y2_halo = halo(3, 2, y2, rows2, G, True)
    z2_halo = halo(4, 2, z2, rows2, G, False)
    y3_halo = halo(5, 3, y3, rows3, G, True)

    lane = lax.broadcasted_iota(jnp.int16, (N, 128), 1)

    def swap(v, dist, blocks):
        mask = (lane & dist) == 0
        new = list(v)
        for i in range(8):
            if not i & blocks:
                a, b = v[i], v[i + blocks]
                new[i] = jnp.where(mask, a, roll(b, dist))
                new[i + blocks] = jnp.where(mask, roll(a, -dist), b)
        return new

    def to_pairs(i, carry):
        for u in range(TILES):
            t = jnp.transpose(x[:, pl.ds((i * TILES + u) * 16, 16), :], (1, 0, 2))
            for p in range(2):
                v = [t[p * 8 + k] for k in range(8)]
                for dist, blocks in ((64, 4), (32, 2), (16, 1)):
                    v = swap(v, dist, blocks)
                pv[1 + 2 * (i * TILES + u) + p, pl.ds(1, 8)] = jnp.stack(v)
        return carry

    for i, (lo, hi) in enumerate(image_blocks):
        loads[i].wait()
        lax.fori_loop(lo // 2 // TILES, hi // 2 // TILES, to_pairs, 0)
        if i == 1:
            pl.semaphore_wait(barrier, len(others))
        if i % 2:
            pv_halo.send_cols(image_blocks[i - 1][0], hi, 0)
        pv_halo.send_rows(lo, hi)

    bias1 = tiled_bias(db1)

    def down1(lo, hi, q0, nq, per):
        per = divisor(hi - lo, per)
        size = per * nq * N

        def step(i, carry):
            row0 = lo + i * per
            sub = lax.broadcasted_iota(jnp.int16, (size, 128), 1) & 15
            own = flat(pv[pl.ds(row0 + 1, per), pl.ds(1 + q0, nq)])
            above = flat(pv[pl.ds(row0, per), pl.ds(1 + q0, nq)])
            left = flat(pv[pl.ds(row0 + 1, per), pl.ds(q0, nq)])
            above_left = flat(pv[pl.ds(row0, per), pl.ds(q0, nq)])
            edge = jnp.where(sub == 15, left, jnp.where(sub == 14, roll(left, 63), roll(above_left, 62)))
            second = jnp.concatenate([edge[:, :64], above[:, 64:]], axis=1)
            res = jnp.dot(jnp.concatenate([own, second], axis=1), bw1[...], preferred_element_type=F32)
            val = jnp.maximum(res + bias1, 0.0).astype(BF)
            pairs = pl.ds(lo // 2 + i * (per // 2) + 1, per // 2)
            for half in range(2):
                v = val[:, half * 128:(half + 1) * 128].reshape(per // 2, 2, nq, N, 128)
                for q in range(nq):
                    y1[pairs, :, 1 + 2 * (q0 + q) + half] = v[:, :, q]
            return carry

        unrolled((hi - lo) // per, step)

    for is_edge, (lo, hi) in schedule(row_blocks(rows1, 16, 56), 1):
        if is_edge:
            pv_halo.need_cols(lo - 1, hi)
            down1(lo, hi, 0, 1, 32)
            y1_halo.send_cols(lo, hi, 1)
            y1_halo.send_rows(lo, hi)
        else:
            pv_halo.need_rows(lo - 1, hi)
            down1(lo, hi, 1, 7, DOWN1_ROWS)
            y1_halo.send_cols(lo, hi, 0)

    def refine(stage, src, src_halo, weight, bias, dst, dst_halo, blocks, delay):
        lhs = functools.partial(refine_lhs, stage, src)
        for is_edge, (lo, hi) in schedule(blocks, delay):
            if is_edge:
                src_halo.need_cols(lo - 1, hi + 1)
                conv_rows(lhs, weight, bias, dst, lo, hi, [(0, 1), (G - 1, 1)], 16)
                if dst_halo is not None:
                    dst_halo.send_cols(lo, hi, 0)
                    dst_halo.send_rows(lo, hi)
            else:
                src_halo.need_rows(lo - 1, hi + 1)
                conv_rows(lhs, weight, bias, dst, lo, hi, [(1, G - 2)], PAIRS)

    def down(src, src_halo, weight, bias, dst, dst_halo, blocks, delay):
        lhs = functools.partial(down_lhs, src)
        for is_edge, (lo, hi) in schedule(blocks, delay):
            if is_edge:
                src_halo.need_cols(2 * lo - 1, 2 * hi)
                conv_rows(lhs, weight, bias, dst, lo, hi, [(0, 1)], 16)
                dst_halo.send_cols(lo, hi, 1)
                dst_halo.send_rows(lo, hi)
            else:
                src_halo.need_rows(2 * lo - 1, 2 * hi)
                conv_rows(lhs, weight, bias, dst, lo, hi, [(1, G - 1)], PAIRS)
                dst_halo.send_cols(lo, hi, 0)

    refine(1, y1, y1_halo, br1, tiled_bias(rb1), into_quads(z1), z1_halo, row_blocks(rows1, 24, 56), 1)
    down(z1, z1_halo, bw2, tiled_bias(db2), into_pairs(y2, 1), y2_halo, row_blocks(rows2, 16, 24), 1)
    refine(2, y2, y2_halo, br2, tiled_bias(rb2), into_quads(z2), z2_halo, row_blocks(rows2, 24, 24), 1)
    down(z2, z2_halo, bw3, tiled_bias(db3), into_pairs(y3, 1), y3_halo, row_blocks(rows3, 16, 16), 4)
    refine(3, y3, y3_halo, br3, tiled_bias(rb3), into_pairs(out, 0), None,
           [(4, rows3 - 4), (rows3 - 4, rows3), (0, 4)], 3)

    for h in (pv_halo, y1_halo, z1_halo, y2_halo, z2_halo, y3_halo):
        h.finish()


def encode(h_count, w_count, images, *params):
    rows1 = images.shape[1] // 2
    rows2, rows3 = rows1 // 2, rows1 // 4
    x = jnp.transpose(images, (0, 1, 3, 2)).reshape(N, rows1 * 8, 128)
    args = [x, jnp.asarray(first_weight_selector(), BF)]
    for i, p in enumerate(params):
        args.append(p.reshape(1, -1) if i % 2 else (p.reshape(9, 4, 32) if i == 0 else p))

    def act(*shape):
        return pltpu.VMEM(shape + (N, 128), BF)

    flops = 2 * 16 * rows1 * 64 * 32 * 9 * (4 + 32 + 16 + 32 + 16 + 32)
    out = pl.pallas_call(
        functools.partial(kernel, h_count, w_count, rows1),
        name='encoder',
        out_shape=jax.ShapeDtypeStruct((rows3 // 2, 2, G, N, 128), BF),
        in_specs=[pl.BlockSpec(memory_space=pl.ANY)] + [pl.BlockSpec(memory_space=pltpu.VMEM)] * (len(args) - 1),
        out_specs=pl.BlockSpec(memory_space=pltpu.VMEM),
        scratch_shapes=[
            pltpu.VMEM((N, rows1 * 8, 128), BF), act(rows1 + 1, 9),
            act(rows1 // 2 + 2, 2, G + 2), act(rows1 // 4 + 1, 4, G + 1),
            act(rows2 // 2 + 2, 2, G + 2), act(rows2 // 4 + 1, 4, G + 1), act(rows3 // 2 + 2, 2, G + 2),
            pltpu.VMEM((36, 32), F32), pltpu.VMEM((256, 256), BF), pltpu.VMEM((768, 256), BF), pltpu.VMEM((1024, 256), BF),
            pltpu.VMEM((1024, 256), BF), pltpu.VMEM((1024, 256), BF), pltpu.VMEM((1536, 256), BF),
            pltpu.VMEM((1, rows1 // 16, N, 128), BF), pltpu.VMEM((1, rows1 // 16, N, 128), BF),
            pltpu.VMEM((4, 2, rows1 // 4, N, 128), BF), pltpu.VMEM((4, 2, rows1 // 4, N, 128), BF),
            pltpu.SemaphoreType.DMA((8,)), pltpu.SemaphoreType.DMA((6, 20)), pltpu.SemaphoreType.DMA((6, 20)),
        ],
        compiler_params=pltpu.CompilerParams(
            collective_id=0, has_side_effects=True, vmem_limit_bytes=56 * 2**20),
        cost_estimate=pl.CostEstimate(flops=flops, bytes_accessed=7 * 2**20, transcendentals=0),
    )(*args)
    return jnp.transpose(out.reshape(rows3, G, N, 128), (2, 0, 1, 3))


def solution(mesh):
    tile_spec = P('batch', 'h', 'w', None)
    body = functools.partial(encode, mesh.shape['h'], mesh.shape['w'])
    return jax.shard_map(body, mesh=mesh, in_specs=(tile_spec,) + (P(),) * 12, out_specs=tile_spec, check_vma=False)
```

```python
import functools

import jax
import jax.numpy as jnp
import numpy as np
from jax import lax
from jax.experimental import pallas as pl
from jax.experimental.pallas import tpu as pltpu
from jax.sharding import PartitionSpec as P

BF = jnp.bfloat16
F32 = jnp.float32
N = 16
G = 16
TILES = 4
DOWN1_ROWS = 8
PAIRS = 4
UNROLL = 0
MESH = pl.DeviceIdType.MESH


def first_weight_selector():
    sel = np.zeros((8, 256, 36), np.float32)
    for j in range(8):
        for c in range(4):
            for wi in range(16):
                b = wi - 2 * j + 1
                if 0 <= b <= 2:
                    for hi in range(2):
                        sel[j, hi * 64 + c * 16 + wi, ((hi + 1) * 3 + b) * 4 + c] = 1
                    sel[j, 128 + 64 + c * 16 + wi, (0 * 3 + b) * 4 + c] = 1
            if j == 0:
                for a, wi in ((1, 15), (2, 14), (0, 13)):
                    sel[j, 128 + c * 16 + wi, (a * 3) * 4 + c] = 1
    return sel.reshape(8 * 256, 36)


def roll(v, shift):
    shift %= 128
    return v if shift == 0 else pltpu.roll(v, shift, v.ndim - 1)


def flat(v):
    return v.reshape(-1, 128)


def build_weight(big, w, k_blocks, stride):
    cin, cout = w.shape[2], w.shape[3]
    ncols = 128 // cout
    taps = [[w[a, b] for b in range(3)] for a in range(3)]
    zero = jnp.zeros((cin, cout), BF)
    for kp, pos in enumerate(k_blocks):
        pieces = []
        for orow in range(2):
            for j in range(ncols):
                piece = zero
                if pos is not None:
                    a, b = pos[0] - stride * orow, pos[1] - stride * j + 1
                    if 0 <= a <= 2 and 0 <= b <= 2:
                        piece = taps[a][b]
                pieces.append(piece)
        big[kp * cin:(kp + 1) * cin, :] = jnp.concatenate(pieces, axis=1)


REFINE1_K = ([(ir, ic) for ir in range(4) for ic in range(4)]
             + [p for e in (0, 2) for p in ((e, 4), (e + 1, -1), (e + 1, 4), (e, -1))])
REFINE2_K = ([(ir, ic) for ir in range(4) for ic in range(2)]
             + [p for ir in range(4) for p in ((ir, 2), (ir, -1))])
REFINE3_K = [(ir, ic) for ir in range(4) for ic in (-1, 0, 1)]
DOWN2_K = ([(ir, ic) for ir in range(5) for ic in range(4)]
           + [p for e in (0, 2) for p in (None, (e + 1, -1), None, (e, -1))]
           + [None, None, None, (4, -1)])
DOWN3_K = ([(ir, ic) for ir in range(5) for ic in range(2)]
           + [p for e in (0, 2) for p in ((e + 1, -1), (e, -1))] + [None, (4, -1)])


def tiled_bias(b):
    reps = 128 // b.shape[1]
    return jnp.concatenate([b[...]] * (2 * reps), axis=1)


def refine_lhs(stage, src, p0, pairs, g0, ng):
    def rows(h, g):
        return flat(src[pl.ds(p0 + (h + 1) // 2, pairs), (h + 1) % 2, pl.ds(g, ng)])

    def own(h):
        return rows(h, 1 + g0)

    def left(h):
        return rows(h, g0)

    def right(h):
        return rows(h, 2 + g0)

    def edge(h):
        return jnp.concatenate([right(h)[:, :64], left(h)[:, 64:]], axis=1)

    if stage == 3:
        return [f(h) for h in range(4) for f in (left, own, right)]
    if stage == 2:
        return [own(h) for h in range(4)] + [edge(h) for h in range(4)]
    ks = [own(h) for h in range(4)]
    for h in (0, 2):
        f0, f1 = edge(h), roll(edge(h + 1), 64)
        ks.append(jnp.concatenate([f0[:, :32], f1[:, 32:96], f0[:, 96:]], axis=1))
    return ks


def down_lhs(src, p0, pairs, g0, ng):
    def rows(h, g):
        return flat(src[pl.ds(p0 + (h + 3) // 4, pairs), (h + 3) % 4, pl.ds(g, ng)])

    def own(h):
        return rows(h, 1 + g0)

    def left(h):
        return rows(h, g0)

    ks = [own(h) for h in range(5)]
    for h in (0, 2):
        ks.append(jnp.concatenate([roll(left(h + 1), 64)[:, :64], left(h)[:, 64:]], axis=1))
    return ks + [left(4)]


def divisor(count, most):
    return next(d for d in range(min(most, count), 0, -1) if count % d == 0 and d % 2 == 0)


def unrolled(count, step):
    trips = count // UNROLL if UNROLL else 1
    each = UNROLL or count
    if trips <= 1:
        for i in range(count):
            step(i, 0)
        return

    def trip(t, carry):
        for u in range(each):
            step(t * each + u, 0)
        return carry

    lax.fori_loop(0, trips, trip, 0)
    for i in range(trips * each, count):
        step(i, 0)


def conv_rows(lhs, weight, bias, dst, lo, hi, ranges, pairs):
    pairs = divisor((hi - lo) // 2, pairs)

    def step(i, carry):
        p0 = lo // 2 + i * pairs
        parts = [lhs(p0, pairs, g0, ng) for g0, ng in ranges]
        ks = [jnp.concatenate(part, axis=0) if len(ranges) > 1 else part[0] for part in zip(*parts)]
        res = jnp.dot(jnp.concatenate(ks, axis=1), weight[...], preferred_element_type=F32)
        val = jnp.maximum(res + bias, 0.0).astype(BF)
        at = 0
        for g0, ng in ranges:
            size = pairs * ng * N
            tile = val[at:at + size]
            at += size
            dst(lo // 4 + i * (pairs // 2), p0, pairs, g0, ng, tile)
        return carry

    unrolled((hi - lo) // (2 * pairs), step)


def into_pairs(buf, shift):
    def dst(quad0, p0, pairs, g0, ng, tile):
        for half in range(2):
            buf[pl.ds(p0 + shift, pairs), half, pl.ds(g0 + shift, ng)] = (
                tile[:, half * 128:(half + 1) * 128].reshape(pairs, ng, N, 128))
    return dst


def into_quads(buf):
    def dst(quad0, p0, pairs, g0, ng, tile):
        for half in range(2):
            v = tile[:, half * 128:(half + 1) * 128].reshape(pairs // 2, 2, ng, N, 128)
            for odd in range(2):
                buf[pl.ds(quad0 + 1, pairs // 2), 2 * odd + half, pl.ds(1 + g0, ng)] = v[:, odd]
    return dst


def pack_cols(stage, buf, lo, hi, right_edge):
    view = buf.shape[1]
    col = buf[pl.ds(lo // view + 1, (hi - lo) // view), :, G if right_edge else 1]
    per = 4 if stage == 1 else 2
    width = 128 // per
    col = col.reshape((hi - lo) // per, per, N, 128)
    base = 128 - width if right_edge else 0
    parts = []
    for k in range(per):
        v = roll(flat(col[:, k]), k * width - base)
        parts.append(v[:, k * width:(k + 1) * width])
    return jnp.concatenate(parts, axis=1).reshape((hi - lo) // per, N, 128)


def unpack_cols(stage, buf, lo, hi, packed, left_halo):
    view = buf.shape[1]
    per = 4 if stage == 1 else 2
    width = 128 // per
    base = 128 - width if left_halo else 0
    tiles = flat(packed)
    rows = [roll(tiles, base - k * width).reshape(-1, N, 128) for k in range(per)]
    buf[pl.ds(lo // view + 1, (hi - lo) // view), :, 0 if left_halo else G + 1] = (
        jnp.stack(rows, axis=1).reshape((hi - lo) // view, view, N, 128))


def pack_image(pv, lo, hi):
    rows = hi - lo
    col = pv[pl.ds(1 + lo, rows), 8].reshape(rows // 16, 16, N, 128)
    lanes = lax.broadcasted_iota(jnp.int16, (rows, 128), 1) & 15
    packed = flat(col[:, 15])
    for k in range(15):
        packed = jnp.where(lanes == k, roll(flat(col[:, k]), k - 15), packed)
    return packed.reshape(rows // 16, N, 128)


def unpack_image(pv, lo, hi, packed):
    tiles = flat(packed)
    rows = [roll(tiles, 15 - k).reshape(-1, N, 128) for k in range(16)]
    pv[pl.ds(1 + lo, hi - lo), 0] = jnp.stack(rows, axis=1).reshape(hi - lo, N, 128)


def row_blocks(rows, start, size):
    out = [(lo, min(lo + size, rows)) for lo in range(start, rows, size)]
    return out + [(lo, min(lo + size, start)) for lo in range(0, start, size)]


class Halo:
    def __init__(self, stage, buf, rows, groups, both, send_c, recv_c, sems, device):
        self.stage, self.buf, self.rows, self.groups, self.both = stage, buf, rows, groups, both
        self.send_c, self.recv_c, self.sems, self.device = send_c, recv_c, sems, device
        self.count, self.sent, self.chunks = 0, [], []
        self.slabs, self.corners = {'top': [], 'bottom': []}, {'top': [], 'bottom': []}

    def copy(self, src, dst, direction):
        send_sem, recv_sem = self.sems
        c = pltpu.make_async_remote_copy(
            src_ref=src, dst_ref=dst, send_sem=send_sem.at[self.count], recv_sem=recv_sem.at[self.count],
            device_id=self.device(*direction), device_id_type=MESH)
        self.count += 1
        self.sent.append(c)
        c.start()
        return c

    def send_cols(self, lo, hi, side):
        buf, stage = self.buf, self.stage
        if stage == 3:
            part = pl.ds(lo // 2 + 1, (hi - lo) // 2)
            src = buf.at[part, :, G if side == 0 else 1]
            dst = buf.at[part, :, 0 if side == 0 else G + 1]
        else:
            per = {0: 16, 1: 4, 2: 2}[stage]
            part = pl.ds(lo // per, (hi - lo) // per)
            self.send_c[side, part] = (
                pack_image(buf, lo, hi) if stage == 0 else pack_cols(stage, buf, lo, hi, side == 0))
            src, dst = self.send_c.at[side, part], self.recv_c.at[side, part]
        self.chunks.append((lo, hi, side, self.copy(src, dst, (0, 1 if side == 0 else -1))))

    def cells(self, row, groups):
        view = self.buf.shape[1] if self.stage else 1
        at = (row // view + 1, row % view) if self.stage else (row + 1,)
        return self.buf.at[at + (groups,)]

    def send_rows(self, lo, hi):
        last, ng, cells = self.rows - 1, self.groups, self.cells
        every = pl.ds(1, ng)
        if hi == self.rows:
            self.slabs['top'].append(self.copy(cells(last, every), cells(-1, every), (1, 0)))
            self.corners['top'].append(self.copy(cells(last, ng), cells(-1, 0), (1, 1)))
            if self.both:
                self.corners['top'].append(self.copy(cells(last, 1), cells(-1, ng + 1), (1, -1)))
        if lo == 0 and self.both:
            self.slabs['bottom'].append(self.copy(cells(0, every), cells(last + 1, every), (-1, 0)))
            self.corners['bottom'].append(self.copy(cells(0, ng), cells(last + 1, 0), (-1, 1)))
            self.corners['bottom'].append(self.copy(cells(0, 1), cells(last + 1, ng + 1), (-1, -1)))

    def ends(self, which, lo, hi):
        for end, wanted in (('top', lo < 0), ('bottom', hi > self.rows)):
            if wanted:
                for c in which[end]:
                    c.wait_recv()
                which[end] = []

    def need_rows(self, lo, hi):
        self.ends(self.slabs, lo, hi)

    def need_cols(self, lo, hi):
        left = []
        for chunk in self.chunks:
            first, end, side, c = chunk
            if first < hi and lo < end:
                c.wait_recv()
                if self.stage != 3:
                    per = {0: 16, 1: 4, 2: 2}[self.stage]
                    packed = self.recv_c[side, pl.ds(first // per, (end - first) // per)]
                    if self.stage == 0:
                        unpack_image(self.buf, first, end, packed)
                    else:
                        unpack_cols(self.stage, self.buf, first, end, packed, side == 0)
            else:
                left.append(chunk)
        self.chunks = left
        self.ends(self.corners, lo, hi)

    def finish(self):
        assert not self.chunks and not any(self.slabs.values()) and not any(self.corners.values())
        for c in self.sent:
            c.wait_send()


def schedule(blocks, delay):
    out = []
    for i in range(len(blocks) + delay):
        if i < len(blocks):
            out.append((False, blocks[i]))
        if i >= delay and i - delay < len(blocks):
            out.append((True, blocks[i - delay]))
    return out


def kernel(h_count, w_count, rows1, x_hbm, sel, dw1, db1, rw1, rb1, dw2, db2, rw2, rb2, dw3, db3, rw3, rb3, out,
           x, pv, y1, z1, y2, z2, y3, w36, bw1, br1, bw2, br2, bw3, br3,
           send_x, recv_x, send_c, recv_c, x_sem, send_sem, recv_sem):
    rows2, rows3 = rows1 // 2, rows1 // 4
    me_h, me_w = lax.axis_index('h'), lax.axis_index('w')

    image_blocks = row_blocks(rows1, 0, 32)
    loads = []
    for i, (lo, hi) in enumerate(image_blocks):
        part = pl.ds(lo * 8, (hi - lo) * 8)
        loads.append(pltpu.make_async_copy(x_hbm.at[:, part], x.at[:, part], x_sem.at[i]))
        loads[-1].start()

    def device(dh, dw):
        return {'h': lax.rem(me_h + dh + h_count, h_count), 'w': lax.rem(me_w + dw + w_count, w_count)}

    barrier = pltpu.get_barrier_semaphore()
    others = [(dh, dw) for dh in (-1, 0, 1) for dw in (-1, 0, 1) if dh or dw]
    for dh, dw in others:
        pl.semaphore_signal(barrier, inc=1, device_id=device(dh, dw), device_id_type=MESH)

    for k in range(9):
        w36[4 * k:4 * k + 4, :] = dw1[k].astype(F32)
    picked = jnp.dot(sel[...], w36[...].astype(BF), preferred_element_type=F32).astype(BF)
    bw1[...] = jnp.concatenate([picked[j * 256:(j + 1) * 256] for j in range(8)], axis=1)
    build_weight(br1, rw1, REFINE1_K, 1)
    build_weight(bw2, dw2, DOWN2_K, 2)
    build_weight(br2, rw2, REFINE2_K, 1)
    build_weight(bw3, dw3, DOWN3_K, 2)
    build_weight(br3, rw3, REFINE3_K, 1)

    def halo(e, stage, buf, rows, groups, both):
        sems = (send_sem.at[e], recv_sem.at[e])
        if stage == 0:
            return Halo(stage, buf, rows, groups, both, send_x, recv_x, sems, device)
        if stage == 3:
            return Halo(stage, buf, rows, groups, both, None, None, sems, device)
        return Halo(stage, buf, rows, groups, both, send_c.at[e - 1], recv_c.at[e - 1], sems, device)

    pv_halo = halo(0, 0, pv, rows1, 8, False)
    y1_halo = halo(1, 1, y1, rows1, G, True)
    z1_halo = halo(2, 1, z1, rows1, G, False)
    y2_halo = halo(3, 2, y2, rows2, G, True)
    z2_halo = halo(4, 2, z2, rows2, G, False)
    y3_halo = halo(5, 3, y3, rows3, G, True)

    lane = lax.broadcasted_iota(jnp.int16, (N, 128), 1)

    def to_groups(v):
        v = [roll(t, 16 * i) for i, t in enumerate(v)]
        for k in range(3):
            mask = (lane & (16 << k)) == 0
            v = [jnp.where(mask, v[j], v[(j + (1 << k)) % 8]) for j in range(8)]
        return [roll(v[-q % 8], -16 * q) for q in range(8)]

    def to_pairs(i, carry):
        for u in range(TILES):
            t = jnp.transpose(x[:, pl.ds((i * TILES + u) * 16, 16), :], (1, 0, 2))
            for p in range(2):
                v = to_groups([t[p * 8 + k] for k in range(8)])
                pv[1 + 2 * (i * TILES + u) + p, pl.ds(1, 8)] = jnp.stack(v)
        return carry

    for i, (lo, hi) in enumerate(image_blocks):
        loads[i].wait()
        lax.fori_loop(lo // 2 // TILES, hi // 2 // TILES, to_pairs, 0)
        if i == 1:
            pl.semaphore_wait(barrier, len(others))
        if i % 2:
            pv_halo.send_cols(image_blocks[i - 1][0], hi, 0)
        pv_halo.send_rows(lo, hi)

    bias1 = tiled_bias(db1)

    def down1(lo, hi, q0, nq, per):
        per = divisor(hi - lo, per)
        size = per * nq * N

        def step(i, carry):
            row0 = lo + i * per
            sub = lax.broadcasted_iota(jnp.int16, (size, 128), 1) & 15
            own = flat(pv[pl.ds(row0 + 1, per), pl.ds(1 + q0, nq)])
            above = flat(pv[pl.ds(row0, per), pl.ds(1 + q0, nq)])
            left = flat(pv[pl.ds(row0 + 1, per), pl.ds(q0, nq)])
            above_left = flat(pv[pl.ds(row0, per), pl.ds(q0, nq)])
            edge = jnp.where(sub == 15, left, jnp.where(sub == 14, roll(left, 63), roll(above_left, 62)))
            second = jnp.concatenate([edge[:, :64], above[:, 64:]], axis=1)
            res = jnp.dot(jnp.concatenate([own, second], axis=1), bw1[...], preferred_element_type=F32)
            val = jnp.maximum(res + bias1, 0.0).astype(BF)
            pairs = pl.ds(lo // 2 + i * (per // 2) + 1, per // 2)
            for half in range(2):
                v = val[:, half * 128:(half + 1) * 128].reshape(per // 2, 2, nq, N, 128)
                for q in range(nq):
                    y1[pairs, :, 1 + 2 * (q0 + q) + half] = v[:, :, q]
            return carry

        unrolled((hi - lo) // per, step)

    for is_edge, (lo, hi) in schedule(row_blocks(rows1, 16, 56), 1):
        if is_edge:
            pv_halo.need_cols(lo - 1, hi)
            down1(lo, hi, 0, 1, 32)
            y1_halo.send_cols(lo, hi, 1)
            y1_halo.send_rows(lo, hi)
        else:
            pv_halo.need_rows(lo - 1, hi)
            down1(lo, hi, 1, 7, DOWN1_ROWS)
            y1_halo.send_cols(lo, hi, 0)

    def refine(stage, src, src_halo, weight, bias, dst, dst_halo, blocks, delay):
        lhs = functools.partial(refine_lhs, stage, src)
        for is_edge, (lo, hi) in schedule(blocks, delay):
            if is_edge:
                src_halo.need_cols(lo - 1, hi + 1)
                conv_rows(lhs, weight, bias, dst, lo, hi, [(0, 1), (G - 1, 1)], 16)
                if dst_halo is not None:
                    dst_halo.send_cols(lo, hi, 0)
                    dst_halo.send_rows(lo, hi)
            else:
                src_halo.need_rows(lo - 1, hi + 1)
                conv_rows(lhs, weight, bias, dst, lo, hi, [(1, G - 2)], PAIRS)

    def down(src, src_halo, weight, bias, dst, dst_halo, blocks, delay):
        lhs = functools.partial(down_lhs, src)
        for is_edge, (lo, hi) in schedule(blocks, delay):
            if is_edge:
                src_halo.need_cols(2 * lo - 1, 2 * hi)
                conv_rows(lhs, weight, bias, dst, lo, hi, [(0, 1)], 16)
                dst_halo.send_cols(lo, hi, 1)
                dst_halo.send_rows(lo, hi)
            else:
                src_halo.need_rows(2 * lo - 1, 2 * hi)
                conv_rows(lhs, weight, bias, dst, lo, hi, [(1, G - 1)], PAIRS)
                dst_halo.send_cols(lo, hi, 0)

    refine(1, y1, y1_halo, br1, tiled_bias(rb1), into_quads(z1), z1_halo, row_blocks(rows1, 24, 56), 1)
    down(z1, z1_halo, bw2, tiled_bias(db2), into_pairs(y2, 1), y2_halo, row_blocks(rows2, 16, 24), 1)
    refine(2, y2, y2_halo, br2, tiled_bias(rb2), into_quads(z2), z2_halo, row_blocks(rows2, 24, 24), 1)
    down(z2, z2_halo, bw3, tiled_bias(db3), into_pairs(y3, 1), y3_halo, row_blocks(rows3, 16, 16), 4)
    refine(3, y3, y3_halo, br3, tiled_bias(rb3), into_pairs(out, 0), None,
           [(4, rows3 - 4), (rows3 - 4, rows3), (0, 4)], 3)

    for h in (pv_halo, y1_halo, z1_halo, y2_halo, z2_halo, y3_halo):
        h.finish()


def encode(h_count, w_count, images, *params):
    rows1 = images.shape[1] // 2
    rows2, rows3 = rows1 // 2, rows1 // 4
    x = jnp.transpose(images, (0, 1, 3, 2)).reshape(N, rows1 * 8, 128)
    args = [x, jnp.asarray(first_weight_selector(), BF)]
    for i, p in enumerate(params):
        args.append(p.reshape(1, -1) if i % 2 else (p.reshape(9, 4, 32) if i == 0 else p))

    def act(*shape):
        return pltpu.VMEM(shape + (N, 128), BF)

    flops = 2 * 16 * rows1 * 64 * 32 * 9 * (4 + 32 + 16 + 32 + 16 + 32)
    out = pl.pallas_call(
        functools.partial(kernel, h_count, w_count, rows1),
        name='encoder',
        out_shape=pltpu.VMEM((rows3 // 2, 2, G, N, 128), BF),
        in_specs=[pl.BlockSpec(memory_space=pl.ANY)] + [pl.BlockSpec(memory_space=pltpu.VMEM)] * (len(args) - 1),
        out_specs=pl.BlockSpec(memory_space=pltpu.VMEM),
        scratch_shapes=[
            pltpu.VMEM((N, rows1 * 8 + 16, 128), BF), act(rows1 + 1, 9),
            act(rows1 // 2 + 2, 2, G + 3), act(rows1 // 4 + 1, 4, G + 1),
            act(rows2 // 2 + 2, 2, G + 3), act(rows2 // 4 + 1, 4, G + 1), act(rows3 // 2 + 2, 2, G + 3),
            pltpu.VMEM((36, 32), F32), pltpu.VMEM((256, 256), BF), pltpu.VMEM((768, 256), BF), pltpu.VMEM((1024, 256), BF),
            pltpu.VMEM((1024, 256), BF), pltpu.VMEM((1024, 256), BF), pltpu.VMEM((1536, 256), BF),
            pltpu.VMEM((1, rows1 // 16, N, 128), BF), pltpu.VMEM((1, rows1 // 16, N, 128), BF),
            pltpu.VMEM((4, 2, rows1 // 4, N, 128), BF), pltpu.VMEM((4, 2, rows1 // 4, N, 128), BF),
            pltpu.SemaphoreType.DMA((8,)), pltpu.SemaphoreType.DMA((6, 20)), pltpu.SemaphoreType.DMA((6, 20)),
        ],
        compiler_params=pltpu.CompilerParams(
            collective_id=0, has_side_effects=True, vmem_limit_bytes=56 * 2**20),
        cost_estimate=pl.CostEstimate(flops=flops, bytes_accessed=7 * 2**20, transcendentals=0),
    )(*args)
    return jnp.transpose(out.reshape(rows3, G, N, 128), (2, 0, 1, 3))


def solution(mesh):
    tile_spec = P('batch', 'h', 'w', None)
    body = functools.partial(encode, mesh.shape['h'], mesh.shape['w'])
    return jax.shard_map(body, mesh=mesh, in_specs=(tile_spec,) + (P(),) * 12, out_specs=tile_spec, check_vma=False)
```

```python
import functools

import jax
import jax.numpy as jnp
import numpy as np
from jax import lax
from jax.experimental import pallas as pl
from jax.experimental.pallas import tpu as pltpu
from jax.sharding import PartitionSpec as P

BF = jnp.bfloat16
F32 = jnp.float32
N = 16
G = 16
TILES = 4
DOWN1_ROWS = 8
PAIRS = 4
UNROLL = 0
MESH = pl.DeviceIdType.MESH


def first_weight_selector():
    sel = np.zeros((8, 256, 36), np.float32)
    for j in range(8):
        for c in range(4):
            for wi in range(16):
                b = wi - 2 * j + 1
                if 0 <= b <= 2:
                    for hi in range(2):
                        sel[j, hi * 64 + c * 16 + wi, ((hi + 1) * 3 + b) * 4 + c] = 1
                    sel[j, 128 + 64 + c * 16 + wi, (0 * 3 + b) * 4 + c] = 1
            if j == 0:
                for a, wi in ((1, 15), (2, 14), (0, 13)):
                    sel[j, 128 + c * 16 + wi, (a * 3) * 4 + c] = 1
    return sel.reshape(8 * 256, 36)


def roll(v, shift):
    shift %= 128
    return v if shift == 0 else pltpu.roll(v, shift, v.ndim - 1)


def flat(v):
    return v.reshape(-1, 128)


def build_weight(big, w, k_blocks, stride):
    cin, cout = w.shape[2], w.shape[3]
    ncols = 128 // cout
    taps = [[w[a, b] for b in range(3)] for a in range(3)]
    zero = jnp.zeros((cin, cout), BF)
    for kp, pos in enumerate(k_blocks):
        pieces = []
        for orow in range(2):
            for j in range(ncols):
                piece = zero
                if pos is not None:
                    a, b = pos[0] - stride * orow, pos[1] - stride * j + 1
                    if 0 <= a <= 2 and 0 <= b <= 2:
                        piece = taps[a][b]
                pieces.append(piece)
        big[kp * cin:(kp + 1) * cin, :] = jnp.concatenate(pieces, axis=1)


REFINE1_K = ([(ir, ic) for ir in range(4) for ic in range(4)]
             + [p for e in (0, 2) for p in ((e, 4), (e + 1, -1), (e + 1, 4), (e, -1))])
REFINE2_K = ([(ir, ic) for ir in range(4) for ic in range(2)]
             + [p for ir in range(4) for p in ((ir, 2), (ir, -1))])
REFINE3_K = [(ir, ic) for ir in range(4) for ic in (-1, 0, 1)]
DOWN2_K = ([(ir, ic) for ir in range(5) for ic in range(4)]
           + [p for e in (0, 2) for p in (None, (e + 1, -1), None, (e, -1))]
           + [None, None, None, (4, -1)])
DOWN3_K = ([(ir, ic) for ir in range(5) for ic in range(2)]
           + [p for e in (0, 2) for p in ((e + 1, -1), (e, -1))] + [None, (4, -1)])


def tiled_bias(b):
    reps = 128 // b.shape[1]
    return jnp.concatenate([b[...]] * (2 * reps), axis=1)


def refine_lhs(stage, src, p0, pairs, g0, ng):
    def rows(h, g):
        return flat(src[pl.ds(p0 + (h + 1) // 2, pairs), (h + 1) % 2, pl.ds(g, ng)])

    def own(h):
        return rows(h, 1 + g0)

    def left(h):
        return rows(h, g0)

    def right(h):
        return rows(h, 2 + g0)

    def edge(h):
        return jnp.concatenate([right(h)[:, :64], left(h)[:, 64:]], axis=1)

    if stage == 3:
        return [f(h) for h in range(4) for f in (left, own, right)]
    if stage == 2:
        return [own(h) for h in range(4)] + [edge(h) for h in range(4)]
    ks = [own(h) for h in range(4)]
    for h in (0, 2):
        f0, f1 = edge(h), roll(edge(h + 1), 64)
        ks.append(jnp.concatenate([f0[:, :32], f1[:, 32:96], f0[:, 96:]], axis=1))
    return ks


def down_lhs(src, p0, pairs, g0, ng):
    def rows(h, g):
        return flat(src[pl.ds(p0 + (h + 3) // 4, pairs), (h + 3) % 4, pl.ds(g, ng)])

    def own(h):
        return rows(h, 1 + g0)

    def left(h):
        return rows(h, g0)

    ks = [own(h) for h in range(5)]
    for h in (0, 2):
        ks.append(jnp.concatenate([roll(left(h + 1), 64)[:, :64], left(h)[:, 64:]], axis=1))
    return ks + [left(4)]


def divisor(count, most):
    return next(d for d in range(min(most, count), 0, -1) if count % d == 0 and d % 2 == 0)


def unrolled(count, step):
    trips = count // UNROLL if UNROLL else 1
    each = UNROLL or count
    if trips <= 1:
        for i in range(count):
            step(i, 0)
        return

    def trip(t, carry):
        for u in range(each):
            step(t * each + u, 0)
        return carry

    lax.fori_loop(0, trips, trip, 0)
    for i in range(trips * each, count):
        step(i, 0)


def conv_rows(lhs, weight, bias, dst, lo, hi, ranges, pairs):
    pairs = divisor((hi - lo) // 2, pairs)

    def step(i, carry):
        p0 = lo // 2 + i * pairs
        parts = [lhs(p0, pairs, g0, ng) for g0, ng in ranges]
        ks = [jnp.concatenate(part, axis=0) if len(ranges) > 1 else part[0] for part in zip(*parts)]
        res = jnp.dot(jnp.concatenate(ks, axis=1), weight[...], preferred_element_type=F32)
        val = jnp.maximum(res + bias, 0.0).astype(BF)
        at = 0
        for g0, ng in ranges:
            size = pairs * ng * N
            tile = val[at:at + size]
            at += size
            dst(lo // 4 + i * (pairs // 2), p0, pairs, g0, ng, tile)
        return carry

    unrolled((hi - lo) // (2 * pairs), step)


def into_pairs(buf, shift):
    def dst(quad0, p0, pairs, g0, ng, tile):
        for half in range(2):
            buf[pl.ds(p0 + shift, pairs), half, pl.ds(g0 + shift, ng)] = (
                tile[:, half * 128:(half + 1) * 128].reshape(pairs, ng, N, 128))
    return dst


def into_quads(buf):
    def dst(quad0, p0, pairs, g0, ng, tile):
        for half in range(2):
            v = tile[:, half * 128:(half + 1) * 128].reshape(pairs // 2, 2, ng, N, 128)
            for odd in range(2):
                buf[pl.ds(quad0 + 1, pairs // 2), 2 * odd + half, pl.ds(1 + g0, ng)] = v[:, odd]
    return dst


def pack_cols(stage, buf, lo, hi, right_edge):
    view = buf.shape[1]
    col = buf[pl.ds(lo // view + 1, (hi - lo) // view), :, G if right_edge else 1]
    per = 4 if stage == 1 else 2
    width = 128 // per
    col = col.reshape((hi - lo) // per, per, N, 128)
    base = 128 - width if right_edge else 0
    parts = []
    for k in range(per):
        v = roll(flat(col[:, k]), k * width - base)
        parts.append(v[:, k * width:(k + 1) * width])
    return jnp.concatenate(parts, axis=1).reshape((hi - lo) // per, N, 128)


def unpack_cols(stage, buf, lo, hi, packed, left_halo):
    view = buf.shape[1]
    per = 4 if stage == 1 else 2
    width = 128 // per
    base = 128 - width if left_halo else 0
    tiles = flat(packed)
    rows = [roll(tiles, base - k * width).reshape(-1, N, 128) for k in range(per)]
    buf[pl.ds(lo // view + 1, (hi - lo) // view), :, 0 if left_halo else G + 1] = (
        jnp.stack(rows, axis=1).reshape((hi - lo) // view, view, N, 128))


def pack_image(pv, lo, hi):
    rows = hi - lo
    col = pv[pl.ds(1 + lo, rows), 8].reshape(rows // 16, 16, N, 128)
    lanes = lax.broadcasted_iota(jnp.int16, (rows, 128), 1) & 15
    packed = flat(col[:, 15])
    for k in range(15):
        packed = jnp.where(lanes == k, roll(flat(col[:, k]), k - 15), packed)
    return packed.reshape(rows // 16, N, 128)


def unpack_image(pv, lo, hi, packed):
    tiles = flat(packed)
    rows = [roll(tiles, 15 - k).reshape(-1, N, 128) for k in range(16)]
    pv[pl.ds(1 + lo, hi - lo), 0] = jnp.stack(rows, axis=1).reshape(hi - lo, N, 128)


def row_blocks(rows, start, size):
    out = [(lo, min(lo + size, rows)) for lo in range(start, rows, size)]
    return out + [(lo, min(lo + size, start)) for lo in range(0, start, size)]


BLOCKS = {
    'y1': [(16, 96), (96, 128), (0, 16)],
    'z1': [(24, 88), (88, 120), (120, 128), (0, 24)],
    'y2': [(16, 40), (40, 56), (56, 64), (0, 16)],
    'z2': [(24, 32), (32, 48), (48, 64), (0, 24)],
    'y3': [(16, 24), (24, 32), (0, 16)],
    'z3': [(4, 28), (28, 32), (0, 4)],
}


class Halo:
    def __init__(self, stage, buf, rows, groups, both, send_c, recv_c, sems, device):
        self.stage, self.buf, self.rows, self.groups, self.both = stage, buf, rows, groups, both
        self.send_c, self.recv_c, self.sems, self.device = send_c, recv_c, sems, device
        self.count, self.sent, self.chunks = 0, [], []
        self.slabs, self.corners = {'top': [], 'bottom': []}, {'top': [], 'bottom': []}

    def copy(self, src, dst, direction):
        send_sem, recv_sem = self.sems
        c = pltpu.make_async_remote_copy(
            src_ref=src, dst_ref=dst, send_sem=send_sem.at[self.count], recv_sem=recv_sem.at[self.count],
            device_id=self.device(*direction), device_id_type=MESH)
        self.count += 1
        self.sent.append(c)
        c.start()
        return c

    def send_cols(self, lo, hi, side):
        buf, stage = self.buf, self.stage
        if stage == 3:
            part = pl.ds(lo // 2 + 1, (hi - lo) // 2)
            src = buf.at[part, :, G if side == 0 else 1]
            dst = buf.at[part, :, 0 if side == 0 else G + 1]
        else:
            per = {0: 16, 1: 4, 2: 2}[stage]
            part = pl.ds(lo // per, (hi - lo) // per)
            self.send_c[side, part] = (
                pack_image(buf, lo, hi) if stage == 0 else pack_cols(stage, buf, lo, hi, side == 0))
            src, dst = self.send_c.at[side, part], self.recv_c.at[side, part]
        self.chunks.append((lo, hi, side, self.copy(src, dst, (0, 1 if side == 0 else -1))))

    def cells(self, row, groups):
        view = self.buf.shape[1] if self.stage else 1
        at = (row // view + 1, row % view) if self.stage else (row + 1,)
        return self.buf.at[at + (groups,)]

    def send_rows(self, lo, hi):
        last, ng, cells = self.rows - 1, self.groups, self.cells
        every = pl.ds(1, ng)
        if hi == self.rows:
            self.slabs['top'].append(self.copy(cells(last, every), cells(-1, every), (1, 0)))
            self.corners['top'].append(self.copy(cells(last, ng), cells(-1, 0), (1, 1)))
            if self.both:
                self.corners['top'].append(self.copy(cells(last, 1), cells(-1, ng + 1), (1, -1)))
        if lo == 0 and self.both:
            self.slabs['bottom'].append(self.copy(cells(0, every), cells(last + 1, every), (-1, 0)))
            self.corners['bottom'].append(self.copy(cells(0, ng), cells(last + 1, 0), (-1, 1)))
            self.corners['bottom'].append(self.copy(cells(0, 1), cells(last + 1, ng + 1), (-1, -1)))

    def ends(self, which, lo, hi):
        for end, wanted in (('top', lo < 0), ('bottom', hi > self.rows)):
            if wanted:
                for c in which[end]:
                    c.wait_recv()
                which[end] = []

    def need_rows(self, lo, hi):
        self.ends(self.slabs, lo, hi)

    def need_cols(self, lo, hi):
        left = []
        for chunk in self.chunks:
            first, end, side, c = chunk
            if first < hi and lo < end:
                c.wait_recv()
                if self.stage != 3:
                    per = {0: 16, 1: 4, 2: 2}[self.stage]
                    packed = self.recv_c[side, pl.ds(first // per, (end - first) // per)]
                    if self.stage == 0:
                        unpack_image(self.buf, first, end, packed)
                    else:
                        unpack_cols(self.stage, self.buf, first, end, packed, side == 0)
            else:
                left.append(chunk)
        self.chunks = left
        self.ends(self.corners, lo, hi)

    def finish(self):
        assert not self.chunks and not any(self.slabs.values()) and not any(self.corners.values())
        for c in self.sent:
            c.wait_send()


def schedule(blocks, delay):
    out = []
    for i in range(len(blocks) + delay):
        if i < len(blocks):
            out.append((False, blocks[i]))
        if i >= delay and i - delay < len(blocks):
            out.append((True, blocks[i - delay]))
    return out


def kernel(h_count, w_count, rows1, x_hbm, sel, dw1, db1, rw1, rb1, dw2, db2, rw2, rb2, dw3, db3, rw3, rb3, out,
           x, pv, y1, z1, y2, z2, y3, w36, bw1, br1, bw2, br2, bw3, br3,
           send_x, recv_x, send_c, recv_c, x_sem, send_sem, recv_sem):
    rows2, rows3 = rows1 // 2, rows1 // 4
    me_h, me_w = lax.axis_index('h'), lax.axis_index('w')

    image_blocks = row_blocks(rows1, 0, 32)
    loads = []
    for i, (lo, hi) in enumerate(image_blocks):
        part = pl.ds(lo * 8, (hi - lo) * 8)
        loads.append(pltpu.make_async_copy(x_hbm.at[:, part], x.at[:, part], x_sem.at[i]))
        loads[-1].start()

    def device(dh, dw):
        return {'h': lax.rem(me_h + dh + h_count, h_count), 'w': lax.rem(me_w + dw + w_count, w_count)}

    barrier = pltpu.get_barrier_semaphore()
    others = [(dh, dw) for dh in (-1, 0, 1) for dw in (-1, 0, 1) if dh or dw]
    for dh, dw in others:
        pl.semaphore_signal(barrier, inc=1, device_id=device(dh, dw), device_id_type=MESH)

    for k in range(9):
        w36[4 * k:4 * k + 4, :] = dw1[k].astype(F32)
    picked = jnp.dot(sel[...], w36[...].astype(BF), preferred_element_type=F32).astype(BF)
    bw1[...] = jnp.concatenate([picked[j * 256:(j + 1) * 256] for j in range(8)], axis=1)
    build_weight(br1, rw1, REFINE1_K, 1)
    build_weight(bw2, dw2, DOWN2_K, 2)
    build_weight(br2, rw2, REFINE2_K, 1)
    build_weight(bw3, dw3, DOWN3_K, 2)
    build_weight(br3, rw3, REFINE3_K, 1)

    def halo(e, stage, buf, rows, groups, both):
        sems = (send_sem.at[e], recv_sem.at[e])
        if stage == 0:
            return Halo(stage, buf, rows, groups, both, send_x, recv_x, sems, device)
        if stage == 3:
            return Halo(stage, buf, rows, groups, both, None, None, sems, device)
        return Halo(stage, buf, rows, groups, both, send_c.at[e - 1], recv_c.at[e - 1], sems, device)

    pv_halo = halo(0, 0, pv, rows1, 8, False)
    y1_halo = halo(1, 1, y1, rows1, G, True)
    z1_halo = halo(2, 1, z1, rows1, G, False)
    y2_halo = halo(3, 2, y2, rows2, G, True)
    z2_halo = halo(4, 2, z2, rows2, G, False)
    y3_halo = halo(5, 3, y3, rows3, G, True)

    lane = lax.broadcasted_iota(jnp.int16, (N, 128), 1)

    def to_groups(v):
        v = [roll(t, 16 * i) for i, t in enumerate(v)]
        for k in range(3):
            mask = (lane & (16 << k)) == 0
            v = [jnp.where(mask, v[j], v[(j + (1 << k)) % 8]) for j in range(8)]
        return [roll(v[-q % 8], -16 * q) for q in range(8)]

    def to_pairs(i, carry):
        for u in range(TILES):
            t = jnp.transpose(x[:, pl.ds((i * TILES + u) * 16, 16), :], (1, 0, 2))
            for p in range(2):
                v = to_groups([t[p * 8 + k] for k in range(8)])
                pv[1 + 2 * (i * TILES + u) + p, pl.ds(1, 8)] = jnp.stack(v)
        return carry

    for i, (lo, hi) in enumerate(image_blocks):
        loads[i].wait()
        lax.fori_loop(lo // 2 // TILES, hi // 2 // TILES, to_pairs, 0)
        if i == 1:
            pl.semaphore_wait(barrier, len(others))
        if i % 2:
            pv_halo.send_cols(image_blocks[i - 1][0], hi, 0)
        pv_halo.send_rows(lo, hi)

    bias1 = tiled_bias(db1)

    def down1(lo, hi, q0, nq, per):
        per = divisor(hi - lo, per)
        size = per * nq * N

        def step(i, carry):
            row0 = lo + i * per
            sub = lax.broadcasted_iota(jnp.int16, (size, 128), 1) & 15
            own = flat(pv[pl.ds(row0 + 1, per), pl.ds(1 + q0, nq)])
            above = flat(pv[pl.ds(row0, per), pl.ds(1 + q0, nq)])
            left = flat(pv[pl.ds(row0 + 1, per), pl.ds(q0, nq)])
            above_left = flat(pv[pl.ds(row0, per), pl.ds(q0, nq)])
            edge = jnp.where(sub == 15, left, jnp.where(sub == 14, roll(left, 63), roll(above_left, 62)))
            second = jnp.concatenate([edge[:, :64], above[:, 64:]], axis=1)
            res = jnp.dot(jnp.concatenate([own, second], axis=1), bw1[...], preferred_element_type=F32)
            val = jnp.maximum(res + bias1, 0.0).astype(BF)
            pairs = pl.ds(lo // 2 + i * (per // 2) + 1, per // 2)
            for half in range(2):
                v = val[:, half * 128:(half + 1) * 128].reshape(per // 2, 2, nq, N, 128)
                for q in range(nq):
                    y1[pairs, :, 1 + 2 * (q0 + q) + half] = v[:, :, q]
            return carry

        unrolled((hi - lo) // per, step)

    for is_edge, (lo, hi) in schedule(BLOCKS['y1'], 1):
        if is_edge:
            pv_halo.need_cols(lo - 1, hi)
            down1(lo, hi, 0, 1, 32)
            y1_halo.send_cols(lo, hi, 1)
            y1_halo.send_rows(lo, hi)
        else:
            pv_halo.need_rows(lo - 1, hi)
            down1(lo, hi, 1, 7, DOWN1_ROWS)
            y1_halo.send_cols(lo, hi, 0)

    def refine(stage, src, src_halo, weight, bias, dst, dst_halo, blocks, delay):
        lhs = functools.partial(refine_lhs, stage, src)
        for is_edge, (lo, hi) in schedule(blocks, delay):
            if is_edge:
                if dst_halo is None and lo == blocks[0][0]:
                    for h in (pv_halo, y1_halo, z1_halo, y2_halo, z2_halo):
                        h.finish()
                src_halo.need_cols(lo - 1, hi + 1)
                conv_rows(lhs, weight, bias, dst, lo, hi, [(0, 1), (G - 1, 1)], 16)
                if dst_halo is not None:
                    dst_halo.send_cols(lo, hi, 0)
                    dst_halo.send_rows(lo, hi)
            else:
                src_halo.need_rows(lo - 1, hi + 1)
                conv_rows(lhs, weight, bias, dst, lo, hi, [(1, G - 2)], PAIRS)

    def down(src, src_halo, weight, bias, dst, dst_halo, blocks, delay):
        lhs = functools.partial(down_lhs, src)
        for is_edge, (lo, hi) in schedule(blocks, delay):
            if is_edge:
                src_halo.need_cols(2 * lo - 1, 2 * hi)
                conv_rows(lhs, weight, bias, dst, lo, hi, [(0, 1)], 16)
                dst_halo.send_cols(lo, hi, 1)
                dst_halo.send_rows(lo, hi)
            else:
                src_halo.need_rows(2 * lo - 1, 2 * hi)
                conv_rows(lhs, weight, bias, dst, lo, hi, [(1, G - 1)], PAIRS)
                dst_halo.send_cols(lo, hi, 0)

    refine(1, y1, y1_halo, br1, tiled_bias(rb1), into_quads(z1), z1_halo, BLOCKS['z1'], 1)
    down(z1, z1_halo, bw2, tiled_bias(db2), into_pairs(y2, 1), y2_halo, BLOCKS['y2'], 1)
    refine(2, y2, y2_halo, br2, tiled_bias(rb2), into_quads(z2), z2_halo, BLOCKS['z2'], 1)
    down(z2, z2_halo, bw3, tiled_bias(db3), into_pairs(y3, 1), y3_halo, BLOCKS['y3'], 3)
    refine(3, y3, y3_halo, br3, tiled_bias(rb3), into_pairs(out, 0), None,
           BLOCKS['z3'], 3)

    y3_halo.finish()


def encode(h_count, w_count, images, *params):
    rows1 = images.shape[1] // 2
    rows2, rows3 = rows1 // 2, rows1 // 4
    x = jnp.transpose(images, (0, 1, 3, 2)).reshape(N, rows1 * 8, 128)
    args = [x, jnp.asarray(first_weight_selector(), BF)]
    for i, p in enumerate(params):
        args.append(p.reshape(1, -1) if i % 2 else (p.reshape(9, 4, 32) if i == 0 else p))

    def act(*shape):
        return pltpu.VMEM(shape + (N, 128), BF)

    flops = 2 * 16 * rows1 * 64 * 32 * 9 * (4 + 32 + 16 + 32 + 16 + 32)
    out = pl.pallas_call(
        functools.partial(kernel, h_count, w_count, rows1),
        name='encoder',
        out_shape=pltpu.VMEM((rows3 // 2, 2, G, N, 128), BF),
        in_specs=[pl.BlockSpec(memory_space=pl.ANY)] + [pl.BlockSpec(memory_space=pltpu.VMEM)] * (len(args) - 1),
        out_specs=pl.BlockSpec(memory_space=pltpu.VMEM),
        scratch_shapes=[
            pltpu.VMEM((N, rows1 * 8 + 16, 128), BF), act(rows1 + 1, 9),
            act(rows1 // 2 + 2, 2, G + 3), act(rows1 // 4 + 1, 4, G + 1),
            act(rows2 // 2 + 2, 2, G + 3), act(rows2 // 4 + 1, 4, G + 1), act(rows3 // 2 + 2, 2, G + 3),
            pltpu.VMEM((36, 32), F32), pltpu.VMEM((256, 256), BF), pltpu.VMEM((768, 256), BF), pltpu.VMEM((1024, 256), BF),
            pltpu.VMEM((1024, 256), BF), pltpu.VMEM((1024, 256), BF), pltpu.VMEM((1536, 256), BF),
            pltpu.VMEM((1, rows1 // 16, N, 128), BF), pltpu.VMEM((1, rows1 // 16, N, 128), BF),
            pltpu.VMEM((4, 2, rows1 // 4, N, 128), BF), pltpu.VMEM((4, 2, rows1 // 4, N, 128), BF),
            pltpu.SemaphoreType.DMA((8,)), pltpu.SemaphoreType.DMA((6, 20)), pltpu.SemaphoreType.DMA((6, 20)),
        ],
        compiler_params=pltpu.CompilerParams(
            collective_id=0, has_side_effects=True, vmem_limit_bytes=56 * 2**20),
        cost_estimate=pl.CostEstimate(flops=flops, bytes_accessed=7 * 2**20, transcendentals=0),
    )(*args)
    return jnp.transpose(out.reshape(rows3, G, N, 128), (2, 0, 1, 3))


def solution(mesh):
    tile_spec = P('batch', 'h', 'w', None)
    body = functools.partial(encode, mesh.shape['h'], mesh.shape['w'])
    return jax.shard_map(body, mesh=mesh, in_specs=(tile_spec,) + (P(),) * 12, out_specs=tile_spec, check_vma=False)
```

```python
import functools

import jax
import jax.numpy as jnp
import numpy as np
from jax import lax
from jax.experimental import pallas as pl
from jax.experimental.pallas import tpu as pltpu
from jax.sharding import PartitionSpec as P

BF = jnp.bfloat16
F32 = jnp.float32
N = 16
G = 16
TILES = 4
DOWN1_ROWS = 8
PAIRS = 4
UNROLL = 1
MESH = pl.DeviceIdType.MESH


def first_weight_selector():
    sel = np.zeros((8, 256, 36), np.float32)
    for j in range(8):
        for c in range(4):
            for wi in range(16):
                b = wi - 2 * j + 1
                if 0 <= b <= 2:
                    for hi in range(2):
                        sel[j, hi * 64 + c * 16 + wi, ((hi + 1) * 3 + b) * 4 + c] = 1
                    sel[j, 128 + 64 + c * 16 + wi, (0 * 3 + b) * 4 + c] = 1
            if j == 0:
                for a, wi in ((1, 15), (2, 14), (0, 13)):
                    sel[j, 128 + c * 16 + wi, (a * 3) * 4 + c] = 1
    return sel.reshape(8 * 256, 36)


def roll(v, shift):
    shift %= 128
    return v if shift == 0 else pltpu.roll(v, shift, v.ndim - 1)


def flat(v):
    return v.reshape(-1, 128)


def build_weight(big, w, k_blocks, stride):
    cin, cout = w.shape[2], w.shape[3]
    ncols = 128 // cout
    taps = [[w[a, b] for b in range(3)] for a in range(3)]
    zero = jnp.zeros((cin, cout), BF)
    for kp, pos in enumerate(k_blocks):
        pieces = []
        for orow in range(2):
            for j in range(ncols):
                piece = zero
                if pos is not None:
                    a, b = pos[0] - stride * orow, pos[1] - stride * j + 1
                    if 0 <= a <= 2 and 0 <= b <= 2:
                        piece = taps[a][b]
                pieces.append(piece)
        big[kp * cin:(kp + 1) * cin, :] = jnp.concatenate(pieces, axis=1)


REFINE1_K = ([(ir, ic) for ir in range(4) for ic in range(4)]
             + [p for e in (0, 2) for p in ((e, 4), (e + 1, -1), (e + 1, 4), (e, -1))])
REFINE2_K = ([(ir, ic) for ir in range(4) for ic in range(2)]
             + [p for ir in range(4) for p in ((ir, 2), (ir, -1))])
REFINE3_K = [(ir, ic) for ir in range(4) for ic in (-1, 0, 1)]
DOWN2_K = ([(ir, ic) for ir in range(5) for ic in range(4)]
           + [p for e in (0, 2) for p in (None, (e + 1, -1), None, (e, -1))]
           + [None, None, None, (4, -1)])
DOWN3_K = ([(ir, ic) for ir in range(5) for ic in range(2)]
           + [p for e in (0, 2) for p in ((e + 1, -1), (e, -1))] + [None, (4, -1)])


def tiled_bias(b):
    reps = 128 // b.shape[1]
    return jnp.concatenate([b[...]] * (2 * reps), axis=1)


def refine_lhs(stage, src, p0, pairs, g0, ng):
    def rows(h, g):
        return flat(src[pl.ds(p0 + (h + 1) // 2, pairs), (h + 1) % 2, pl.ds(g, ng)])

    def own(h):
        return rows(h, 1 + g0)

    def left(h):
        return rows(h, g0)

    def right(h):
        return rows(h, 2 + g0)

    def edge(h):
        return jnp.concatenate([right(h)[:, :64], left(h)[:, 64:]], axis=1)

    if stage == 3:
        return [f(h) for h in range(4) for f in (left, own, right)]
    if stage == 2:
        return [own(h) for h in range(4)] + [edge(h) for h in range(4)]
    ks = [own(h) for h in range(4)]
    for h in (0, 2):
        f0, f1 = edge(h), roll(edge(h + 1), 64)
        ks.append(jnp.concatenate([f0[:, :32], f1[:, 32:96], f0[:, 96:]], axis=1))
    return ks


def down_lhs(src, p0, pairs, g0, ng):
    def rows(h, g):
        return flat(src[pl.ds(p0 + (h + 3) // 4, pairs), (h + 3) % 4, pl.ds(g, ng)])

    def own(h):
        return rows(h, 1 + g0)

    def left(h):
        return rows(h, g0)

    ks = [own(h) for h in range(5)]
    for h in (0, 2):
        ks.append(jnp.concatenate([roll(left(h + 1), 64)[:, :64], left(h)[:, 64:]], axis=1))
    return ks + [left(4)]


def divisor(count, most):
    return next(d for d in range(min(most, count), 0, -1) if count % d == 0 and d % 2 == 0)


def unrolled(count, step):
    trips = count // UNROLL if UNROLL else 1
    each = UNROLL or count
    if trips <= 1:
        for i in range(count):
            step(i, 0)
        return

    def trip(t, carry):
        for u in range(each):
            step(t * each + u, 0)
        return carry

    lax.fori_loop(0, trips, trip, 0)
    for i in range(trips * each, count):
        step(i, 0)


def conv_rows(lhs, weight, bias, dst, lo, hi, ranges, pairs):
    pairs = divisor((hi - lo) // 2, pairs)

    def step(i, carry):
        p0 = lo // 2 + i * pairs
        parts = [lhs(p0, pairs, g0, ng) for g0, ng in ranges]
        ks = [jnp.concatenate(part, axis=0) if len(ranges) > 1 else part[0] for part in zip(*parts)]
        res = jnp.dot(jnp.concatenate(ks, axis=1), weight[...], preferred_element_type=F32)
        val = jnp.maximum(res + bias, 0.0).astype(BF)
        at = 0
        for g0, ng in ranges:
            size = pairs * ng * N
            tile = val[at:at + size]
            at += size
            dst(lo // 4 + i * (pairs // 2), p0, pairs, g0, ng, tile)
        return carry

    unrolled((hi - lo) // (2 * pairs), step)


def into_pairs(buf, shift):
    def dst(quad0, p0, pairs, g0, ng, tile):
        for half in range(2):
            buf[pl.ds(p0 + shift, pairs), half, pl.ds(g0 + shift, ng)] = (
                tile[:, half * 128:(half + 1) * 128].reshape(pairs, ng, N, 128))
    return dst


def into_quads(buf):
    def dst(quad0, p0, pairs, g0, ng, tile):
        for half in range(2):
            v = tile[:, half * 128:(half + 1) * 128].reshape(pairs // 2, 2, ng, N, 128)
            for odd in range(2):
                buf[pl.ds(quad0 + 1, pairs // 2), 2 * odd + half, pl.ds(1 + g0, ng)] = v[:, odd]
    return dst


def pack_cols(stage, buf, lo, hi, right_edge):
    view = buf.shape[1]
    col = buf[pl.ds(lo // view + 1, (hi - lo) // view), :, G if right_edge else 1]
    per = 4 if stage == 1 else 2
    width = 128 // per
    col = col.reshape((hi - lo) // per, per, N, 128)
    base = 128 - width if right_edge else 0
    parts = []
    for k in range(per):
        v = roll(flat(col[:, k]), k * width - base)
        parts.append(v[:, k * width:(k + 1) * width])
    return jnp.concatenate(parts, axis=1).reshape((hi - lo) // per, N, 128)


def unpack_cols(stage, buf, lo, hi, packed, left_halo):
    view = buf.shape[1]
    per = 4 if stage == 1 else 2
    width = 128 // per
    base = 128 - width if left_halo else 0
    tiles = flat(packed)
    rows = [roll(tiles, base - k * width).reshape(-1, N, 128) for k in range(per)]
    buf[pl.ds(lo // view + 1, (hi - lo) // view), :, 0 if left_halo else G + 1] = (
        jnp.stack(rows, axis=1).reshape((hi - lo) // view, view, N, 128))


def pack_image(pv, lo, hi):
    rows = hi - lo
    col = pv[pl.ds(1 + lo, rows), 8].reshape(rows // 16, 16, N, 128)
    lanes = lax.broadcasted_iota(jnp.int16, (rows, 128), 1) & 15
    packed = flat(col[:, 15])
    for k in range(15):
        packed = jnp.where(lanes == k, roll(flat(col[:, k]), k - 15), packed)
    return packed.reshape(rows // 16, N, 128)


def unpack_image(pv, lo, hi, packed):
    tiles = flat(packed)
    rows = [roll(tiles, 15 - k).reshape(-1, N, 128) for k in range(16)]
    pv[pl.ds(1 + lo, hi - lo), 0] = jnp.stack(rows, axis=1).reshape(hi - lo, N, 128)


def row_blocks(rows, start, size):
    out = [(lo, min(lo + size, rows)) for lo in range(start, rows, size)]
    return out + [(lo, min(lo + size, start)) for lo in range(0, start, size)]


class Halo:
    def __init__(self, stage, buf, rows, groups, both, send_c, recv_c, sems, device):
        self.stage, self.buf, self.rows, self.groups, self.both = stage, buf, rows, groups, both
        self.send_c, self.recv_c, self.sems, self.device = send_c, recv_c, sems, device
        self.count, self.sent, self.chunks = 0, [], []
        self.slabs, self.corners = {'top': [], 'bottom': []}, {'top': [], 'bottom': []}

    def copy(self, src, dst, direction):
        send_sem, recv_sem = self.sems
        c = pltpu.make_async_remote_copy(
            src_ref=src, dst_ref=dst, send_sem=send_sem.at[self.count], recv_sem=recv_sem.at[self.count],
            device_id=self.device(*direction), device_id_type=MESH)
        self.count += 1
        self.sent.append(c)
        c.start()
        return c

    def send_cols(self, lo, hi, side):
        buf, stage = self.buf, self.stage
        if stage == 3:
            part = pl.ds(lo // 2 + 1, (hi - lo) // 2)
            src = buf.at[part, :, G if side == 0 else 1]
            dst = buf.at[part, :, 0 if side == 0 else G + 1]
        else:
            per = {0: 16, 1: 4, 2: 2}[stage]
            part = pl.ds(lo // per, (hi - lo) // per)
            self.send_c[side, part] = (
                pack_image(buf, lo, hi) if stage == 0 else pack_cols(stage, buf, lo, hi, side == 0))
            src, dst = self.send_c.at[side, part], self.recv_c.at[side, part]
        self.chunks.append((lo, hi, side, self.copy(src, dst, (0, 1 if side == 0 else -1))))

    def cells(self, row, groups):
        view = self.buf.shape[1] if self.stage else 1
        at = (row // view + 1, row % view) if self.stage else (row + 1,)
        return self.buf.at[at + (groups,)]

    def send_rows(self, lo, hi):
        last, ng, cells = self.rows - 1, self.groups, self.cells
        every = pl.ds(1, ng)
        if hi == self.rows:
            self.slabs['top'].append(self.copy(cells(last, every), cells(-1, every), (1, 0)))
            self.corners['top'].append(self.copy(cells(last, ng), cells(-1, 0), (1, 1)))
            if self.both:
                self.corners['top'].append(self.copy(cells(last, 1), cells(-1, ng + 1), (1, -1)))
        if lo == 0 and self.both:
            self.slabs['bottom'].append(self.copy(cells(0, every), cells(last + 1, every), (-1, 0)))
            self.corners['bottom'].append(self.copy(cells(0, ng), cells(last + 1, 0), (-1, 1)))
            self.corners['bottom'].append(self.copy(cells(0, 1), cells(last + 1, ng + 1), (-1, -1)))

    def ends(self, which, lo, hi):
        for end, wanted in (('top', lo < 0), ('bottom', hi > self.rows)):
            if wanted:
                for c in which[end]:
                    c.wait_recv()
                which[end] = []

    def need_rows(self, lo, hi):
        self.ends(self.slabs, lo, hi)

    def need_cols(self, lo, hi):
        left = []
        for chunk in self.chunks:
            first, end, side, c = chunk
            if first < hi and lo < end:
                c.wait_recv()
                if self.stage != 3:
                    per = {0: 16, 1: 4, 2: 2}[self.stage]
                    packed = self.recv_c[side, pl.ds(first // per, (end - first) // per)]
                    if self.stage == 0:
                        unpack_image(self.buf, first, end, packed)
                    else:
                        unpack_cols(self.stage, self.buf, first, end, packed, side == 0)
            else:
                left.append(chunk)
        self.chunks = left
        self.ends(self.corners, lo, hi)

    def finish(self):
        assert not self.chunks and not any(self.slabs.values()) and not any(self.corners.values())
        for c in self.sent:
            c.wait_send()


def schedule(blocks, delay):
    out = []
    for i in range(len(blocks) + delay):
        if i < len(blocks):
            out.append((False, blocks[i]))
        if i >= delay and i - delay < len(blocks):
            out.append((True, blocks[i - delay]))
    return out


def kernel(h_count, w_count, rows1, x_hbm, sel, dw1, db1, rw1, rb1, dw2, db2, rw2, rb2, dw3, db3, rw3, rb3, out,
           x, pv, y1, z1, y2, z2, y3, w36, bw1, br1, bw2, br2, bw3, br3,
           send_x, recv_x, send_c, recv_c, x_sem, send_sem, recv_sem):
    rows2, rows3 = rows1 // 2, rows1 // 4
    me_h, me_w = lax.axis_index('h'), lax.axis_index('w')

    image_blocks = row_blocks(rows1, 0, 32)
    loads = []
    for i, (lo, hi) in enumerate(image_blocks):
        part = pl.ds(lo * 8, (hi - lo) * 8)
        loads.append(pltpu.make_async_copy(x_hbm.at[:, part], x.at[:, part], x_sem.at[i]))
        loads[-1].start()

    def device(dh, dw):
        return {'h': lax.rem(me_h + dh + h_count, h_count), 'w': lax.rem(me_w + dw + w_count, w_count)}

    barrier = pltpu.get_barrier_semaphore()
    others = [(dh, dw) for dh in (-1, 0, 1) for dw in (-1, 0, 1) if dh or dw]
    for dh, dw in others:
        pl.semaphore_signal(barrier, inc=1, device_id=device(dh, dw), device_id_type=MESH)

    for k in range(9):
        w36[4 * k:4 * k + 4, :] = dw1[k].astype(F32)
    picked = jnp.dot(sel[...], w36[...].astype(BF), preferred_element_type=F32).astype(BF)
    bw1[...] = jnp.concatenate([picked[j * 256:(j + 1) * 256] for j in range(8)], axis=1)
    build_weight(br1, rw1, REFINE1_K, 1)
    build_weight(bw2, dw2, DOWN2_K, 2)
    build_weight(br2, rw2, REFINE2_K, 1)
    build_weight(bw3, dw3, DOWN3_K, 2)
    build_weight(br3, rw3, REFINE3_K, 1)

    def halo(e, stage, buf, rows, groups, both):
        sems = (send_sem.at[e], recv_sem.at[e])
        if stage == 0:
            return Halo(stage, buf, rows, groups, both, send_x, recv_x, sems, device)
        if stage == 3:
            return Halo(stage, buf, rows, groups, both, None, None, sems, device)
        return Halo(stage, buf, rows, groups, both, send_c.at[e - 1], recv_c.at[e - 1], sems, device)

    pv_halo = halo(0, 0, pv, rows1, 8, False)
    y1_halo = halo(1, 1, y1, rows1, G, True)
    z1_halo = halo(2, 1, z1, rows1, G, False)
    y2_halo = halo(3, 2, y2, rows2, G, True)
    z2_halo = halo(4, 2, z2, rows2, G, False)
    y3_halo = halo(5, 3, y3, rows3, G, True)

    lane = lax.broadcasted_iota(jnp.int16, (N, 128), 1)

    def to_groups(v):
        v = [roll(t, 16 * i) for i, t in enumerate(v)]
        for k in range(3):
            mask = (lane & (16 << k)) == 0
            v = [jnp.where(mask, v[j], v[(j + (1 << k)) % 8]) for j in range(8)]
        return [roll(v[-q % 8], -16 * q) for q in range(8)]

    def to_pairs(i, carry):
        for u in range(TILES):
            t = jnp.transpose(x[:, pl.ds((i * TILES + u) * 16, 16), :], (1, 0, 2))
            for p in range(2):
                v = to_groups([t[p * 8 + k] for k in range(8)])
                pv[1 + 2 * (i * TILES + u) + p, pl.ds(1, 8)] = jnp.stack(v)
        return carry

    for i, (lo, hi) in enumerate(image_blocks):
        loads[i].wait()
        lax.fori_loop(lo // 2 // TILES, hi // 2 // TILES, to_pairs, 0)
        if i == 1:
            pl.semaphore_wait(barrier, len(others))
        if i % 2:
            pv_halo.send_cols(image_blocks[i - 1][0], hi, 0)
        pv_halo.send_rows(lo, hi)

    bias1 = tiled_bias(db1)

    def down1(lo, hi, q0, nq, per):
        per = divisor(hi - lo, per)
        size = per * nq * N

        def step(i, carry):
            row0 = lo + i * per
            sub = lax.broadcasted_iota(jnp.int16, (size, 128), 1) & 15
            own = flat(pv[pl.ds(row0 + 1, per), pl.ds(1 + q0, nq)])
            above = flat(pv[pl.ds(row0, per), pl.ds(1 + q0, nq)])
            left = flat(pv[pl.ds(row0 + 1, per), pl.ds(q0, nq)])
            above_left = flat(pv[pl.ds(row0, per), pl.ds(q0, nq)])
            edge = jnp.where(sub == 15, left, jnp.where(sub == 14, roll(left, 63), roll(above_left, 62)))
            second = jnp.concatenate([edge[:, :64], above[:, 64:]], axis=1)
            res = jnp.dot(jnp.concatenate([own, second], axis=1), bw1[...], preferred_element_type=F32)
            val = jnp.maximum(res + bias1, 0.0).astype(BF)
            pairs = pl.ds(lo // 2 + i * (per // 2) + 1, per // 2)
            for half in range(2):
                v = val[:, half * 128:(half + 1) * 128].reshape(per // 2, 2, nq, N, 128)
                for q in range(nq):
                    y1[pairs, :, 1 + 2 * (q0 + q) + half] = v[:, :, q]
            return carry

        unrolled((hi - lo) // per, step)

    for is_edge, (lo, hi) in schedule(row_blocks(rows1, 16, 56), 1):
        if is_edge:
            pv_halo.need_cols(lo - 1, hi)
            down1(lo, hi, 0, 1, 32)
            y1_halo.send_cols(lo, hi, 1)
            y1_halo.send_rows(lo, hi)
        else:
            pv_halo.need_rows(lo - 1, hi)
            down1(lo, hi, 1, 7, DOWN1_ROWS)
            y1_halo.send_cols(lo, hi, 0)

    def refine(stage, src, src_halo, weight, bias, dst, dst_halo, blocks, delay):
        lhs = functools.partial(refine_lhs, stage, src)
        for is_edge, (lo, hi) in schedule(blocks, delay):
            if is_edge:
                src_halo.need_cols(lo - 1, hi + 1)
                conv_rows(lhs, weight, bias, dst, lo, hi, [(0, 1), (G - 1, 1)], 16)
                if dst_halo is not None:
                    dst_halo.send_cols(lo, hi, 0)
                    dst_halo.send_rows(lo, hi)
            else:
                src_halo.need_rows(lo - 1, hi + 1)
                conv_rows(lhs, weight, bias, dst, lo, hi, [(1, G - 2)], PAIRS)

    def down(src, src_halo, weight, bias, dst, dst_halo, blocks, delay):
        lhs = functools.partial(down_lhs, src)
        for is_edge, (lo, hi) in schedule(blocks, delay):
            if is_edge:
                src_halo.need_cols(2 * lo - 1, 2 * hi)
                conv_rows(lhs, weight, bias, dst, lo, hi, [(0, 1)], 16)
                dst_halo.send_cols(lo, hi, 1)
                dst_halo.send_rows(lo, hi)
            else:
                src_halo.need_rows(2 * lo - 1, 2 * hi)
                conv_rows(lhs, weight, bias, dst, lo, hi, [(1, G - 1)], PAIRS)
                dst_halo.send_cols(lo, hi, 0)

    refine(1, y1, y1_halo, br1, tiled_bias(rb1), into_quads(z1), z1_halo, row_blocks(rows1, 24, 56), 1)
    down(z1, z1_halo, bw2, tiled_bias(db2), into_pairs(y2, 1), y2_halo, row_blocks(rows2, 16, 24), 1)
    refine(2, y2, y2_halo, br2, tiled_bias(rb2), into_quads(z2), z2_halo, row_blocks(rows2, 24, 24), 1)
    down(z2, z2_halo, bw3, tiled_bias(db3), into_pairs(y3, 1), y3_halo, row_blocks(rows3, 16, 16), 4)
    refine(3, y3, y3_halo, br3, tiled_bias(rb3), into_pairs(out, 0), None,
           [(4, rows3 - 4), (rows3 - 4, rows3), (0, 4)], 3)

    for h in (pv_halo, y1_halo, z1_halo, y2_halo, z2_halo, y3_halo):
        h.finish()


def encode(h_count, w_count, images, *params):
    rows1 = images.shape[1] // 2
    rows2, rows3 = rows1 // 2, rows1 // 4
    x = jnp.transpose(images, (0, 1, 3, 2)).reshape(N, rows1 * 8, 128)
    args = [x, jnp.asarray(first_weight_selector(), BF)]
    for i, p in enumerate(params):
        args.append(p.reshape(1, -1) if i % 2 else (p.reshape(9, 4, 32) if i == 0 else p))

    def act(*shape):
        return pltpu.VMEM(shape + (N, 128), BF)

    flops = 2 * 16 * rows1 * 64 * 32 * 9 * (4 + 32 + 16 + 32 + 16 + 32)
    out = pl.pallas_call(
        functools.partial(kernel, h_count, w_count, rows1),
        name='encoder',
        out_shape=pltpu.VMEM((rows3 // 2, 2, G, N, 128), BF),
        in_specs=[pl.BlockSpec(memory_space=pl.ANY)] + [pl.BlockSpec(memory_space=pltpu.VMEM)] * (len(args) - 1),
        out_specs=pl.BlockSpec(memory_space=pltpu.VMEM),
        scratch_shapes=[
            pltpu.VMEM((N, rows1 * 8 + 16, 128), BF), act(rows1 + 1, 9),
            act(rows1 // 2 + 2, 2, G + 3), act(rows1 // 4 + 1, 4, G + 1),
            act(rows2 // 2 + 2, 2, G + 3), act(rows2 // 4 + 1, 4, G + 1), act(rows3 // 2 + 2, 2, G + 3),
            pltpu.VMEM((36, 32), F32), pltpu.VMEM((256, 256), BF), pltpu.VMEM((768, 256), BF), pltpu.VMEM((1024, 256), BF),
            pltpu.VMEM((1024, 256), BF), pltpu.VMEM((1024, 256), BF), pltpu.VMEM((1536, 256), BF),
            pltpu.VMEM((1, rows1 // 16, N, 128), BF), pltpu.VMEM((1, rows1 // 16, N, 128), BF),
            pltpu.VMEM((4, 2, rows1 // 4, N, 128), BF), pltpu.VMEM((4, 2, rows1 // 4, N, 128), BF),
            pltpu.SemaphoreType.DMA((8,)), pltpu.SemaphoreType.DMA((6, 20)), pltpu.SemaphoreType.DMA((6, 20)),
        ],
        compiler_params=pltpu.CompilerParams(
            collective_id=0, has_side_effects=True, vmem_limit_bytes=56 * 2**20),
        cost_estimate=pl.CostEstimate(flops=flops, bytes_accessed=7 * 2**20, transcendentals=0),
    )(*args)
    return jnp.transpose(out.reshape(rows3, G, N, 128), (2, 0, 1, 3))


def solution(mesh):
    tile_spec = P('batch', 'h', 'w', None)
    body = functools.partial(encode, mesh.shape['h'], mesh.shape['w'])
    return jax.shard_map(body, mesh=mesh, in_specs=(tile_spec,) + (P(),) * 12, out_specs=tile_spec, check_vma=False)
```

```python
import functools

import jax
import jax.numpy as jnp
import numpy as np
from jax import lax
from jax.experimental import pallas as pl
from jax.experimental.pallas import tpu as pltpu
from jax.sharding import PartitionSpec as P

BF = jnp.bfloat16
F32 = jnp.float32
N = 16
G = 16
TILES = 4
DOWN1_ROWS = 16
PAIRS = 4
UNROLL = 0
MESH = pl.DeviceIdType.MESH


def first_weight_selector():
    sel = np.zeros((8, 256, 36), np.float32)
    for j in range(8):
        for c in range(4):
            for wi in range(16):
                b = wi - 2 * j + 1
                if 0 <= b <= 2:
                    for hi in range(2):
                        sel[j, hi * 64 + c * 16 + wi, ((hi + 1) * 3 + b) * 4 + c] = 1
                    sel[j, 128 + 64 + c * 16 + wi, (0 * 3 + b) * 4 + c] = 1
            if j == 0:
                for a, wi in ((1, 15), (2, 14), (0, 13)):
                    sel[j, 128 + c * 16 + wi, (a * 3) * 4 + c] = 1
    return sel.reshape(8 * 256, 36)


def roll(v, shift):
    shift %= 128
    return v if shift == 0 else pltpu.roll(v, shift, v.ndim - 1)


def flat(v):
    return v.reshape(-1, 128)


def build_weight(big, w, k_blocks, stride):
    cin, cout = w.shape[2], w.shape[3]
    ncols = 128 // cout
    taps = [[w[a, b] for b in range(3)] for a in range(3)]
    zero = jnp.zeros((cin, cout), BF)
    for kp, pos in enumerate(k_blocks):
        pieces = []
        for orow in range(2):
            for j in range(ncols):
                piece = zero
                if pos is not None:
                    a, b = pos[0] - stride * orow, pos[1] - stride * j + 1
                    if 0 <= a <= 2 and 0 <= b <= 2:
                        piece = taps[a][b]
                pieces.append(piece)
        big[kp * cin:(kp + 1) * cin, :] = jnp.concatenate(pieces, axis=1)


REFINE1_K = ([(ir, ic) for ir in range(4) for ic in range(4)]
             + [p for e in (0, 2) for p in ((e, 4), (e + 1, -1), (e + 1, 4), (e, -1))])
REFINE2_K = ([(ir, ic) for ir in range(4) for ic in range(2)]
             + [p for ir in range(4) for p in ((ir, 2), (ir, -1))])
REFINE3_K = [(ir, ic) for ir in range(4) for ic in (-1, 0, 1)]
DOWN2_K = ([(ir, ic) for ir in range(5) for ic in range(4)]
           + [p for e in (0, 2) for p in (None, (e + 1, -1), None, (e, -1))]
           + [None, None, None, (4, -1)])
DOWN3_K = ([(ir, ic) for ir in range(5) for ic in range(2)]
           + [p for e in (0, 2) for p in ((e + 1, -1), (e, -1))] + [None, (4, -1)])


def tiled_bias(b):
    reps = 128 // b.shape[1]
    return jnp.concatenate([b[...]] * (2 * reps), axis=1)


def refine_lhs(stage, src, p0, pairs, g0, ng):
    def rows(h, g):
        return flat(src[pl.ds(p0 + (h + 1) // 2, pairs), (h + 1) % 2, pl.ds(g, ng)])

    def own(h):
        return rows(h, 1 + g0)

    def left(h):
        return rows(h, g0)

    def right(h):
        return rows(h, 2 + g0)

    def edge(h):
        return jnp.concatenate([right(h)[:, :64], left(h)[:, 64:]], axis=1)

    if stage == 3:
        return [f(h) for h in range(4) for f in (left, own, right)]
    if stage == 2:
        return [own(h) for h in range(4)] + [edge(h) for h in range(4)]
    ks = [own(h) for h in range(4)]
    for h in (0, 2):
        f0, f1 = edge(h), roll(edge(h + 1), 64)
        ks.append(jnp.concatenate([f0[:, :32], f1[:, 32:96], f0[:, 96:]], axis=1))
    return ks


def down_lhs(src, p0, pairs, g0, ng):
    def rows(h, g):
        return flat(src[pl.ds(p0 + (h + 3) // 4, pairs), (h + 3) % 4, pl.ds(g, ng)])

    def own(h):
        return rows(h, 1 + g0)

    def left(h):
        return rows(h, g0)

    ks = [own(h) for h in range(5)]
    for h in (0, 2):
        ks.append(jnp.concatenate([roll(left(h + 1), 64)[:, :64], left(h)[:, 64:]], axis=1))
    return ks + [left(4)]


def divisor(count, most):
    return next(d for d in range(min(most, count), 0, -1) if count % d == 0 and d % 2 == 0)


def unrolled(count, step):
    trips = count // UNROLL if UNROLL else 1
    each = UNROLL or count
    if trips <= 1:
        for i in range(count):
            step(i, 0)
        return

    def trip(t, carry):
        for u in range(each):
            step(t * each + u, 0)
        return carry

    lax.fori_loop(0, trips, trip, 0)
    for i in range(trips * each, count):
        step(i, 0)


def conv_rows(lhs, weight, bias, dst, lo, hi, ranges, pairs):
    pairs = divisor((hi - lo) // 2, pairs)

    def step(i, carry):
        p0 = lo // 2 + i * pairs
        parts = [lhs(p0, pairs, g0, ng) for g0, ng in ranges]
        ks = [jnp.concatenate(part, axis=0) if len(ranges) > 1 else part[0] for part in zip(*parts)]
        res = jnp.dot(jnp.concatenate(ks, axis=1), weight[...], preferred_element_type=F32)
        val = jnp.maximum(res + bias, 0.0).astype(BF)
        at = 0
        for g0, ng in ranges:
            size = pairs * ng * N
            tile = val[at:at + size]
            at += size
            dst(lo // 4 + i * (pairs // 2), p0, pairs, g0, ng, tile)
        return carry

    unrolled((hi - lo) // (2 * pairs), step)


def into_pairs(buf, shift):
    def dst(quad0, p0, pairs, g0, ng, tile):
        for half in range(2):
            buf[pl.ds(p0 + shift, pairs), half, pl.ds(g0 + shift, ng)] = (
                tile[:, half * 128:(half + 1) * 128].reshape(pairs, ng, N, 128))
    return dst


def into_quads(buf):
    def dst(quad0, p0, pairs, g0, ng, tile):
        for half in range(2):
            v = tile[:, half * 128:(half + 1) * 128].reshape(pairs // 2, 2, ng, N, 128)
            for odd in range(2):
                buf[pl.ds(quad0 + 1, pairs // 2), 2 * odd + half, pl.ds(1 + g0, ng)] = v[:, odd]
    return dst


def pack_cols(stage, buf, lo, hi, right_edge):
    view = buf.shape[1]
    col = buf[pl.ds(lo // view + 1, (hi - lo) // view), :, G if right_edge else 1]
    per = 4 if stage == 1 else 2
    width = 128 // per
    col = col.reshape((hi - lo) // per, per, N, 128)
    base = 128 - width if right_edge else 0
    parts = []
    for k in range(per):
        v = roll(flat(col[:, k]), k * width - base)
        parts.append(v[:, k * width:(k + 1) * width])
    return jnp.concatenate(parts, axis=1).reshape((hi - lo) // per, N, 128)


def unpack_cols(stage, buf, lo, hi, packed, left_halo):
    view = buf.shape[1]
    per = 4 if stage == 1 else 2
    width = 128 // per
    base = 128 - width if left_halo else 0
    tiles = flat(packed)
    rows = [roll(tiles, base - k * width).reshape(-1, N, 128) for k in range(per)]
    buf[pl.ds(lo // view + 1, (hi - lo) // view), :, 0 if left_halo else G + 1] = (
        jnp.stack(rows, axis=1).reshape((hi - lo) // view, view, N, 128))


def pack_image(pv, lo, hi):
    rows = hi - lo
    col = pv[pl.ds(1 + lo, rows), 8].reshape(rows // 16, 16, N, 128)
    lanes = lax.broadcasted_iota(jnp.int16, (rows, 128), 1) & 15
    packed = flat(col[:, 15])
    for k in range(15):
        packed = jnp.where(lanes == k, roll(flat(col[:, k]), k - 15), packed)
    return packed.reshape(rows // 16, N, 128)


def unpack_image(pv, lo, hi, packed):
    tiles = flat(packed)
    rows = [roll(tiles, 15 - k).reshape(-1, N, 128) for k in range(16)]
    pv[pl.ds(1 + lo, hi - lo), 0] = jnp.stack(rows, axis=1).reshape(hi - lo, N, 128)


def row_blocks(rows, start, size):
    out = [(lo, min(lo + size, rows)) for lo in range(start, rows, size)]
    return out + [(lo, min(lo + size, start)) for lo in range(0, start, size)]


class Halo:
    def __init__(self, stage, buf, rows, groups, both, send_c, recv_c, sems, device):
        self.stage, self.buf, self.rows, self.groups, self.both = stage, buf, rows, groups, both
        self.send_c, self.recv_c, self.sems, self.device = send_c, recv_c, sems, device
        self.count, self.sent, self.chunks = 0, [], []
        self.slabs, self.corners = {'top': [], 'bottom': []}, {'top': [], 'bottom': []}

    def copy(self, src, dst, direction):
        send_sem, recv_sem = self.sems
        c = pltpu.make_async_remote_copy(
            src_ref=src, dst_ref=dst, send_sem=send_sem.at[self.count], recv_sem=recv_sem.at[self.count],
            device_id=self.device(*direction), device_id_type=MESH)
        self.count += 1
        self.sent.append(c)
        c.start()
        return c

    def send_cols(self, lo, hi, side):
        buf, stage = self.buf, self.stage
        if stage == 3:
            part = pl.ds(lo // 2 + 1, (hi - lo) // 2)
            src = buf.at[part, :, G if side == 0 else 1]
            dst = buf.at[part, :, 0 if side == 0 else G + 1]
        else:
            per = {0: 16, 1: 4, 2: 2}[stage]
            part = pl.ds(lo // per, (hi - lo) // per)
            self.send_c[side, part] = (
                pack_image(buf, lo, hi) if stage == 0 else pack_cols(stage, buf, lo, hi, side == 0))
            src, dst = self.send_c.at[side, part], self.recv_c.at[side, part]
        self.chunks.append((lo, hi, side, self.copy(src, dst, (0, 1 if side == 0 else -1))))

    def cells(self, row, groups):
        view = self.buf.shape[1] if self.stage else 1
        at = (row // view + 1, row % view) if self.stage else (row + 1,)
        return self.buf.at[at + (groups,)]

    def send_rows(self, lo, hi):
        last, ng, cells = self.rows - 1, self.groups, self.cells
        every = pl.ds(1, ng)
        if hi == self.rows:
            self.slabs['top'].append(self.copy(cells(last, every), cells(-1, every), (1, 0)))
            self.corners['top'].append(self.copy(cells(last, ng), cells(-1, 0), (1, 1)))
            if self.both:
                self.corners['top'].append(self.copy(cells(last, 1), cells(-1, ng + 1), (1, -1)))
        if lo == 0 and self.both:
            self.slabs['bottom'].append(self.copy(cells(0, every), cells(last + 1, every), (-1, 0)))
            self.corners['bottom'].append(self.copy(cells(0, ng), cells(last + 1, 0), (-1, 1)))
            self.corners['bottom'].append(self.copy(cells(0, 1), cells(last + 1, ng + 1), (-1, -1)))

    def ends(self, which, lo, hi):
        for end, wanted in (('top', lo < 0), ('bottom', hi > self.rows)):
            if wanted:
                for c in which[end]:
                    c.wait_recv()
                which[end] = []

    def need_rows(self, lo, hi):
        self.ends(self.slabs, lo, hi)

    def need_cols(self, lo, hi):
        left = []
        for chunk in self.chunks:
            first, end, side, c = chunk
            if first < hi and lo < end:
                c.wait_recv()
                if self.stage != 3:
                    per = {0: 16, 1: 4, 2: 2}[self.stage]
                    packed = self.recv_c[side, pl.ds(first // per, (end - first) // per)]
                    if self.stage == 0:
                        unpack_image(self.buf, first, end, packed)
                    else:
                        unpack_cols(self.stage, self.buf, first, end, packed, side == 0)
            else:
                left.append(chunk)
        self.chunks = left
        self.ends(self.corners, lo, hi)

    def finish(self):
        assert not self.chunks and not any(self.slabs.values()) and not any(self.corners.values())
        for c in self.sent:
            c.wait_send()


def schedule(blocks, delay):
    out = []
    for i in range(len(blocks) + delay):
        if i < len(blocks):
            out.append((False, blocks[i]))
        if i >= delay and i - delay < len(blocks):
            out.append((True, blocks[i - delay]))
    return out


def kernel(h_count, w_count, rows1, x_hbm, sel, dw1, db1, rw1, rb1, dw2, db2, rw2, rb2, dw3, db3, rw3, rb3, out,
           x, pv, y1, z1, y2, z2, y3, w36, bw1, br1, bw2, br2, bw3, br3,
           send_x, recv_x, send_c, recv_c, x_sem, send_sem, recv_sem):
    rows2, rows3 = rows1 // 2, rows1 // 4
    me_h, me_w = lax.axis_index('h'), lax.axis_index('w')

    image_blocks = row_blocks(rows1, 0, 32)
    loads = []
    for i, (lo, hi) in enumerate(image_blocks):
        part = pl.ds(lo * 8, (hi - lo) * 8)
        loads.append(pltpu.make_async_copy(x_hbm.at[:, part], x.at[:, part], x_sem.at[i]))
        loads[-1].start()

    def device(dh, dw):
        return {'h': lax.rem(me_h + dh + h_count, h_count), 'w': lax.rem(me_w + dw + w_count, w_count)}

    barrier = pltpu.get_barrier_semaphore()
    others = [(dh, dw) for dh in (-1, 0, 1) for dw in (-1, 0, 1) if dh or dw]
    for dh, dw in others:
        pl.semaphore_signal(barrier, inc=1, device_id=device(dh, dw), device_id_type=MESH)

    for k in range(9):
        w36[4 * k:4 * k + 4, :] = dw1[k].astype(F32)
    picked = jnp.dot(sel[...], w36[...].astype(BF), preferred_element_type=F32).astype(BF)
    bw1[...] = jnp.concatenate([picked[j * 256:(j + 1) * 256] for j in range(8)], axis=1)
    build_weight(br1, rw1, REFINE1_K, 1)
    build_weight(bw2, dw2, DOWN2_K, 2)
    build_weight(br2, rw2, REFINE2_K, 1)
    build_weight(bw3, dw3, DOWN3_K, 2)
    build_weight(br3, rw3, REFINE3_K, 1)

    def halo(e, stage, buf, rows, groups, both):
        sems = (send_sem.at[e], recv_sem.at[e])
        if stage == 0:
            return Halo(stage, buf, rows, groups, both, send_x, recv_x, sems, device)
        if stage == 3:
            return Halo(stage, buf, rows, groups, both, None, None, sems, device)
        return Halo(stage, buf, rows, groups, both, send_c.at[e - 1], recv_c.at[e - 1], sems, device)

    pv_halo = halo(0, 0, pv, rows1, 8, False)
    y1_halo = halo(1, 1, y1, rows1, G, True)
    z1_halo = halo(2, 1, z1, rows1, G, False)
    y2_halo = halo(3, 2, y2, rows2, G, True)
    z2_halo = halo(4, 2, z2, rows2, G, False)
    y3_halo = halo(5, 3, y3, rows3, G, True)

    lane = lax.broadcasted_iota(jnp.int16, (N, 128), 1)

    def to_groups(v):
        v = [roll(t, 16 * i) for i, t in enumerate(v)]
        for k in range(3):
            mask = (lane & (16 << k)) == 0
            v = [jnp.where(mask, v[j], v[(j + (1 << k)) % 8]) for j in range(8)]
        return [roll(v[-q % 8], -16 * q) for q in range(8)]

    def to_pairs(i, carry):
        for u in range(TILES):
            t = jnp.transpose(x[:, pl.ds((i * TILES + u) * 16, 16), :], (1, 0, 2))
            for p in range(2):
                v = to_groups([t[p * 8 + k] for k in range(8)])
                pv[1 + 2 * (i * TILES + u) + p, pl.ds(1, 8)] = jnp.stack(v)
        return carry

    for i, (lo, hi) in enumerate(image_blocks):
        loads[i].wait()
        lax.fori_loop(lo // 2 // TILES, hi // 2 // TILES, to_pairs, 0)
        if i == 1:
            pl.semaphore_wait(barrier, len(others))
        if i % 2:
            pv_halo.send_cols(image_blocks[i - 1][0], hi, 0)
        pv_halo.send_rows(lo, hi)

    bias1 = tiled_bias(db1)

    def down1(lo, hi, q0, nq, per):
        per = divisor(hi - lo, per)
        size = per * nq * N

        def step(i, carry):
            row0 = lo + i * per
            sub = lax.broadcasted_iota(jnp.int16, (size, 128), 1) & 15
            own = flat(pv[pl.ds(row0 + 1, per), pl.ds(1 + q0, nq)])
            above = flat(pv[pl.ds(row0, per), pl.ds(1 + q0, nq)])
            left = flat(pv[pl.ds(row0 + 1, per), pl.ds(q0, nq)])
            above_left = flat(pv[pl.ds(row0, per), pl.ds(q0, nq)])
            edge = jnp.where(sub == 15, left, jnp.where(sub == 14, roll(left, 63), roll(above_left, 62)))
            second = jnp.concatenate([edge[:, :64], above[:, 64:]], axis=1)
            res = jnp.dot(jnp.concatenate([own, second], axis=1), bw1[...], preferred_element_type=F32)
            val = jnp.maximum(res + bias1, 0.0).astype(BF)
            pairs = pl.ds(lo // 2 + i * (per // 2) + 1, per // 2)
            for half in range(2):
                v = val[:, half * 128:(half + 1) * 128].reshape(per // 2, 2, nq, N, 128)
                for q in range(nq):
                    y1[pairs, :, 1 + 2 * (q0 + q) + half] = v[:, :, q]
            return carry

        lax.fori_loop(0, (hi - lo) // per, step, 0)

    for is_edge, (lo, hi) in schedule([(16, 80), (80, 128), (0, 16)], 1):
        if is_edge:
            pv_halo.need_cols(lo - 1, hi)
            down1(lo, hi, 0, 1, 32)
            y1_halo.send_cols(lo, hi, 1)
            y1_halo.send_rows(lo, hi)
        else:
            pv_halo.need_rows(lo - 1, hi)
            down1(lo, hi, 1, 7, DOWN1_ROWS)
            y1_halo.send_cols(lo, hi, 0)

    def refine(stage, src, src_halo, weight, bias, dst, dst_halo, blocks, delay):
        lhs = functools.partial(refine_lhs, stage, src)
        for is_edge, (lo, hi) in schedule(blocks, delay):
            if is_edge:
                if dst_halo is None and lo == blocks[0][0]:
                    for h in (pv_halo, y1_halo, z1_halo, y2_halo, z2_halo):
                        h.finish()
                src_halo.need_cols(lo - 1, hi + 1)
                conv_rows(lhs, weight, bias, dst, lo, hi, [(0, 1), (G - 1, 1)], 16)
                if dst_halo is not None:
                    dst_halo.send_cols(lo, hi, 0)
                    dst_halo.send_rows(lo, hi)
            else:
                src_halo.need_rows(lo - 1, hi + 1)
                conv_rows(lhs, weight, bias, dst, lo, hi, [(1, G - 2)], PAIRS)

    def down(src, src_halo, weight, bias, dst, dst_halo, blocks, delay):
        lhs = functools.partial(down_lhs, src)
        for is_edge, (lo, hi) in schedule(blocks, delay):
            if is_edge:
                src_halo.need_cols(2 * lo - 1, 2 * hi)
                conv_rows(lhs, weight, bias, dst, lo, hi, [(0, 1)], 16)
                dst_halo.send_cols(lo, hi, 1)
                dst_halo.send_rows(lo, hi)
            else:
                src_halo.need_rows(2 * lo - 1, 2 * hi)
                conv_rows(lhs, weight, bias, dst, lo, hi, [(1, G - 1)], PAIRS)
                dst_halo.send_cols(lo, hi, 0)

    refine(1, y1, y1_halo, br1, tiled_bias(rb1), into_quads(z1), z1_halo, row_blocks(rows1, 24, 56), 1)
    down(z1, z1_halo, bw2, tiled_bias(db2), into_pairs(y2, 1), y2_halo, row_blocks(rows2, 16, 24), 1)
    refine(2, y2, y2_halo, br2, tiled_bias(rb2), into_quads(z2), z2_halo, row_blocks(rows2, 24, 24), 1)
    down(z2, z2_halo, bw3, tiled_bias(db3), into_pairs(y3, 1), y3_halo, row_blocks(rows3, 16, 16), 4)
    refine(3, y3, y3_halo, br3, tiled_bias(rb3), into_pairs(out, 0), None,
           [(4, rows3 - 4), (rows3 - 4, rows3), (0, 4)], 3)

    y3_halo.finish()


def encode(h_count, w_count, images, *params):
    rows1 = images.shape[1] // 2
    rows2, rows3 = rows1 // 2, rows1 // 4
    x = jnp.transpose(images, (0, 1, 3, 2)).reshape(N, rows1 * 8, 128)
    args = [x, jnp.asarray(first_weight_selector(), BF)]
    for i, p in enumerate(params):
        args.append(p.reshape(1, -1) if i % 2 else (p.reshape(9, 4, 32) if i == 0 else p))

    def act(*shape):
        return pltpu.VMEM(shape + (N, 128), BF)

    flops = 2 * 16 * rows1 * 64 * 32 * 9 * (4 + 32 + 16 + 32 + 16 + 32)
    out = pl.pallas_call(
        functools.partial(kernel, h_count, w_count, rows1),
        name='encoder',
        out_shape=pltpu.VMEM((rows3 // 2, 2, G, N, 128), BF),
        in_specs=[pl.BlockSpec(memory_space=pl.ANY)] + [pl.BlockSpec(memory_space=pltpu.VMEM)] * (len(args) - 1),
        out_specs=pl.BlockSpec(memory_space=pltpu.VMEM),
        scratch_shapes=[
            pltpu.VMEM((N, rows1 * 8 + 16, 128), BF), act(rows1 + 1, 9),
            act(rows1 // 2 + 2, 2, G + 3), act(rows1 // 4 + 1, 4, G + 1),
            act(rows2 // 2 + 2, 2, G + 3), act(rows2 // 4 + 1, 4, G + 1), act(rows3 // 2 + 2, 2, G + 3),
            pltpu.VMEM((36, 32), F32), pltpu.VMEM((256, 256), BF), pltpu.VMEM((768, 256), BF), pltpu.VMEM((1024, 256), BF),
            pltpu.VMEM((1024, 256), BF), pltpu.VMEM((1024, 256), BF), pltpu.VMEM((1536, 256), BF),
            pltpu.VMEM((1, rows1 // 16, N, 128), BF), pltpu.VMEM((1, rows1 // 16, N, 128), BF),
            pltpu.VMEM((4, 2, rows1 // 4, N, 128), BF), pltpu.VMEM((4, 2, rows1 // 4, N, 128), BF),
            pltpu.SemaphoreType.DMA((8,)), pltpu.SemaphoreType.DMA((6, 20)), pltpu.SemaphoreType.DMA((6, 20)),
        ],
        compiler_params=pltpu.CompilerParams(
            collective_id=0, has_side_effects=True, vmem_limit_bytes=56 * 2**20),
        cost_estimate=pl.CostEstimate(flops=flops, bytes_accessed=7 * 2**20, transcendentals=0),
    )(*args)
    return jnp.transpose(out.reshape(rows3, G, N, 128), (2, 0, 1, 3))


def solution(mesh):
    tile_spec = P('batch', 'h', 'w', None)
    body = functools.partial(encode, mesh.shape['h'], mesh.shape['w'])
    return jax.shard_map(body, mesh=mesh, in_specs=(tile_spec,) + (P(),) * 12, out_specs=tile_spec, check_vma=False)
```

```python
import functools

import jax
import jax.numpy as jnp
import numpy as np
from jax import lax
from jax.experimental import pallas as pl
from jax.experimental.pallas import tpu as pltpu
from jax.sharding import PartitionSpec as P

BF = jnp.bfloat16
F32 = jnp.float32
N = 16
G = 16
TILES = 4
DOWN1_ROWS = 4
PAIRS = 4
UNROLL = 0
MESH = pl.DeviceIdType.MESH


def first_weight_selector():
    sel = np.zeros((8, 256, 36), np.float32)
    for j in range(8):
        for c in range(4):
            for wi in range(16):
                b = wi - 2 * j + 1
                if 0 <= b <= 2:
                    for hi in range(2):
                        sel[j, hi * 64 + c * 16 + wi, ((hi + 1) * 3 + b) * 4 + c] = 1
                    sel[j, 128 + 64 + c * 16 + wi, (0 * 3 + b) * 4 + c] = 1
            if j == 0:
                for a, wi in ((1, 15), (2, 14), (0, 13)):
                    sel[j, 128 + c * 16 + wi, (a * 3) * 4 + c] = 1
    return sel.reshape(8 * 256, 36)


def roll(v, shift):
    shift %= 128
    return v if shift == 0 else pltpu.roll(v, shift, v.ndim - 1)


def flat(v):
    return v.reshape(-1, 128)


def build_weight(big, w, k_blocks, stride):
    cin, cout = w.shape[2], w.shape[3]
    ncols = 128 // cout
    taps = [[w[a, b] for b in range(3)] for a in range(3)]
    zero = jnp.zeros((cin, cout), BF)
    for kp, pos in enumerate(k_blocks):
        pieces = []
        for orow in range(2):
            for j in range(ncols):
                piece = zero
                if pos is not None:
                    a, b = pos[0] - stride * orow, pos[1] - stride * j + 1
                    if 0 <= a <= 2 and 0 <= b <= 2:
                        piece = taps[a][b]
                pieces.append(piece)
        big[kp * cin:(kp + 1) * cin, :] = jnp.concatenate(pieces, axis=1)


REFINE1_K = ([(ir, ic) for ir in range(4) for ic in range(4)]
             + [p for e in (0, 2) for p in ((e, 4), (e + 1, -1), (e + 1, 4), (e, -1))])
REFINE2_K = ([(ir, ic) for ir in range(4) for ic in range(2)]
             + [p for ir in range(4) for p in ((ir, 2), (ir, -1))])
REFINE3_K = [(ir, ic) for ir in range(4) for ic in (-1, 0, 1)]
DOWN2_K = ([(ir, ic) for ir in range(5) for ic in range(4)]
           + [p for e in (0, 2) for p in (None, (e + 1, -1), None, (e, -1))]
           + [None, None, None, (4, -1)])
DOWN3_K = ([(ir, ic) for ir in range(5) for ic in range(2)]
           + [p for e in (0, 2) for p in ((e + 1, -1), (e, -1))] + [None, (4, -1)])


def tiled_bias(b):
    reps = 128 // b.shape[1]
    return jnp.concatenate([b[...]] * (2 * reps), axis=1)


def refine_lhs(stage, src, p0, pairs, g0, ng):
    def rows(h, g):
        return flat(src[pl.ds(p0 + (h + 1) // 2, pairs), (h + 1) % 2, pl.ds(g, ng)])

    def own(h):
        return rows(h, 1 + g0)

    def left(h):
        return rows(h, g0)

    def right(h):
        return rows(h, 2 + g0)

    def edge(h):
        return jnp.concatenate([right(h)[:, :64], left(h)[:, 64:]], axis=1)

    if stage == 3:
        return [f(h) for h in range(4) for f in (left, own, right)]
    if stage == 2:
        return [own(h) for h in range(4)] + [edge(h) for h in range(4)]
    ks = [own(h) for h in range(4)]
    for h in (0, 2):
        f0, f1 = edge(h), roll(edge(h + 1), 64)
        ks.append(jnp.concatenate([f0[:, :32], f1[:, 32:96], f0[:, 96:]], axis=1))
    return ks


def down_lhs(src, p0, pairs, g0, ng):
    def rows(h, g):
        return flat(src[pl.ds(p0 + (h + 3) // 4, pairs), (h + 3) % 4, pl.ds(g, ng)])

    def own(h):
        return rows(h, 1 + g0)

    def left(h):
        return rows(h, g0)

    ks = [own(h) for h in range(5)]
    for h in (0, 2):
        ks.append(jnp.concatenate([roll(left(h + 1), 64)[:, :64], left(h)[:, 64:]], axis=1))
    return ks + [left(4)]


def divisor(count, most):
    return next(d for d in range(min(most, count), 0, -1) if count % d == 0 and d % 2 == 0)


def unrolled(count, step):
    trips = count // UNROLL if UNROLL else 1
    each = UNROLL or count
    if trips <= 1:
        for i in range(count):
            step(i, 0)
        return

    def trip(t, carry):
        for u in range(each):
            step(t * each + u, 0)
        return carry

    lax.fori_loop(0, trips, trip, 0)
    for i in range(trips * each, count):
        step(i, 0)


def conv_rows(lhs, weight, bias, dst, lo, hi, ranges, pairs):
    pairs = divisor((hi - lo) // 2, pairs)

    def step(i, carry):
        p0 = lo // 2 + i * pairs
        parts = [lhs(p0, pairs, g0, ng) for g0, ng in ranges]
        ks = [jnp.concatenate(part, axis=0) if len(ranges) > 1 else part[0] for part in zip(*parts)]
        res = jnp.dot(jnp.concatenate(ks, axis=1), weight[...], preferred_element_type=F32)
        val = jnp.maximum(res + bias, 0.0).astype(BF)
        at = 0
        for g0, ng in ranges:
            size = pairs * ng * N
            tile = val[at:at + size]
            at += size
            dst(lo // 4 + i * (pairs // 2), p0, pairs, g0, ng, tile)
        return carry

    unrolled((hi - lo) // (2 * pairs), step)


def into_pairs(buf, shift):
    def dst(quad0, p0, pairs, g0, ng, tile):
        for half in range(2):
            buf[pl.ds(p0 + shift, pairs), half, pl.ds(g0 + shift, ng)] = (
                tile[:, half * 128:(half + 1) * 128].reshape(pairs, ng, N, 128))
    return dst


def into_quads(buf):
    def dst(quad0, p0, pairs, g0, ng, tile):
        for half in range(2):
            v = tile[:, half * 128:(half + 1) * 128].reshape(pairs // 2, 2, ng, N, 128)
            for odd in range(2):
                buf[pl.ds(quad0 + 1, pairs // 2), 2 * odd + half, pl.ds(1 + g0, ng)] = v[:, odd]
    return dst


def pack_cols(stage, buf, lo, hi, right_edge):
    view = buf.shape[1]
    col = buf[pl.ds(lo // view + 1, (hi - lo) // view), :, G if right_edge else 1]
    per = 4 if stage == 1 else 2
    width = 128 // per
    col = col.reshape((hi - lo) // per, per, N, 128)
    base = 128 - width if right_edge else 0
    parts = []
    for k in range(per):
        v = roll(flat(col[:, k]), k * width - base)
        parts.append(v[:, k * width:(k + 1) * width])
    return jnp.concatenate(parts, axis=1).reshape((hi - lo) // per, N, 128)


def unpack_cols(stage, buf, lo, hi, packed, left_halo):
    view = buf.shape[1]
    per = 4 if stage == 1 else 2
    width = 128 // per
    base = 128 - width if left_halo else 0
    tiles = flat(packed)
    rows = [roll(tiles, base - k * width).reshape(-1, N, 128) for k in range(per)]
    buf[pl.ds(lo // view + 1, (hi - lo) // view), :, 0 if left_halo else G + 1] = (
        jnp.stack(rows, axis=1).reshape((hi - lo) // view, view, N, 128))


def pack_image(pv, lo, hi):
    rows = hi - lo
    col = pv[pl.ds(1 + lo, rows), 8].reshape(rows // 16, 16, N, 128)
    lanes = lax.broadcasted_iota(jnp.int16, (rows, 128), 1) & 15
    packed = flat(col[:, 15])
    for k in range(15):
        packed = jnp.where(lanes == k, roll(flat(col[:, k]), k - 15), packed)
    return packed.reshape(rows // 16, N, 128)


def unpack_image(pv, lo, hi, packed):
    tiles = flat(packed)
    rows = [roll(tiles, 15 - k).reshape(-1, N, 128) for k in range(16)]
    pv[pl.ds(1 + lo, hi - lo), 0] = jnp.stack(rows, axis=1).reshape(hi - lo, N, 128)


def row_blocks(rows, start, size):
    out = [(lo, min(lo + size, rows)) for lo in range(start, rows, size)]
    return out + [(lo, min(lo + size, start)) for lo in range(0, start, size)]


class Halo:
    def __init__(self, stage, buf, rows, groups, both, send_c, recv_c, sems, device):
        self.stage, self.buf, self.rows, self.groups, self.both = stage, buf, rows, groups, both
        self.send_c, self.recv_c, self.sems, self.device = send_c, recv_c, sems, device
        self.count, self.sent, self.chunks = 0, [], []
        self.slabs, self.corners = {'top': [], 'bottom': []}, {'top': [], 'bottom': []}

    def copy(self, src, dst, direction):
        send_sem, recv_sem = self.sems
        c = pltpu.make_async_remote_copy(
            src_ref=src, dst_ref=dst, send_sem=send_sem.at[self.count], recv_sem=recv_sem.at[self.count],
            device_id=self.device(*direction), device_id_type=MESH)
        self.count += 1
        self.sent.append(c)
        c.start()
        return c

    def send_cols(self, lo, hi, side):
        buf, stage = self.buf, self.stage
        if stage == 3:
            part = pl.ds(lo // 2 + 1, (hi - lo) // 2)
            src = buf.at[part, :, G if side == 0 else 1]
            dst = buf.at[part, :, 0 if side == 0 else G + 1]
        else:
            per = {0: 16, 1: 4, 2: 2}[stage]
            part = pl.ds(lo // per, (hi - lo) // per)
            self.send_c[side, part] = (
                pack_image(buf, lo, hi) if stage == 0 else pack_cols(stage, buf, lo, hi, side == 0))
            src, dst = self.send_c.at[side, part], self.recv_c.at[side, part]
        self.chunks.append((lo, hi, side, self.copy(src, dst, (0, 1 if side == 0 else -1))))

    def cells(self, row, groups):
        view = self.buf.shape[1] if self.stage else 1
        at = (row // view + 1, row % view) if self.stage else (row + 1,)
        return self.buf.at[at + (groups,)]

    def send_rows(self, lo, hi):
        last, ng, cells = self.rows - 1, self.groups, self.cells
        every = pl.ds(1, ng)
        if hi == self.rows:
            self.slabs['top'].append(self.copy(cells(last, every), cells(-1, every), (1, 0)))
            self.corners['top'].append(self.copy(cells(last, ng), cells(-1, 0), (1, 1)))
            if self.both:
                self.corners['top'].append(self.copy(cells(last, 1), cells(-1, ng + 1), (1, -1)))
        if lo == 0 and self.both:
            self.slabs['bottom'].append(self.copy(cells(0, every), cells(last + 1, every), (-1, 0)))
            self.corners['bottom'].append(self.copy(cells(0, ng), cells(last + 1, 0), (-1, 1)))
            self.corners['bottom'].append(self.copy(cells(0, 1), cells(last + 1, ng + 1), (-1, -1)))

    def ends(self, which, lo, hi):
        for end, wanted in (('top', lo < 0), ('bottom', hi > self.rows)):
            if wanted:
                for c in which[end]:
                    c.wait_recv()
                which[end] = []

    def need_rows(self, lo, hi):
        self.ends(self.slabs, lo, hi)

    def need_cols(self, lo, hi):
        left = []
        for chunk in self.chunks:
            first, end, side, c = chunk
            if first < hi and lo < end:
                c.wait_recv()
                if self.stage != 3:
                    per = {0: 16, 1: 4, 2: 2}[self.stage]
                    packed = self.recv_c[side, pl.ds(first // per, (end - first) // per)]
                    if self.stage == 0:
                        unpack_image(self.buf, first, end, packed)
                    else:
                        unpack_cols(self.stage, self.buf, first, end, packed, side == 0)
            else:
                left.append(chunk)
        self.chunks = left
        self.ends(self.corners, lo, hi)

    def finish(self):
        assert not self.chunks and not any(self.slabs.values()) and not any(self.corners.values())
        for c in self.sent:
            c.wait_send()


def schedule(blocks, delay):
    out = []
    for i in range(len(blocks) + delay):
        if i < len(blocks):
            out.append((False, blocks[i]))
        if i >= delay and i - delay < len(blocks):
            out.append((True, blocks[i - delay]))
    return out


def kernel(h_count, w_count, rows1, x_hbm, sel, dw1, db1, rw1, rb1, dw2, db2, rw2, rb2, dw3, db3, rw3, rb3, out,
           x, pv, y1, z1, y2, z2, y3, w36, bw1, br1, bw2, br2, bw3, br3,
           send_x, recv_x, send_c, recv_c, x_sem, send_sem, recv_sem):
    rows2, rows3 = rows1 // 2, rows1 // 4
    me_h, me_w = lax.axis_index('h'), lax.axis_index('w')

    image_blocks = row_blocks(rows1, 0, 32)
    loads = []
    for i, (lo, hi) in enumerate(image_blocks):
        part = pl.ds(lo * 8, (hi - lo) * 8)
        loads.append(pltpu.make_async_copy(x_hbm.at[:, part], x.at[:, part], x_sem.at[i]))
        loads[-1].start()

    def device(dh, dw):
        return {'h': lax.rem(me_h + dh + h_count, h_count), 'w': lax.rem(me_w + dw + w_count, w_count)}

    barrier = pltpu.get_barrier_semaphore()
    others = [(dh, dw) for dh in (-1, 0, 1) for dw in (-1, 0, 1) if dh or dw]
    for dh, dw in others:
        pl.semaphore_signal(barrier, inc=1, device_id=device(dh, dw), device_id_type=MESH)

    for k in range(9):
        w36[4 * k:4 * k + 4, :] = dw1[k].astype(F32)
    picked = jnp.dot(sel[...], w36[...].astype(BF), preferred_element_type=F32).astype(BF)
    bw1[...] = jnp.concatenate([picked[j * 256:(j + 1) * 256] for j in range(8)], axis=1)
    build_weight(br1, rw1, REFINE1_K, 1)
    build_weight(bw2, dw2, DOWN2_K, 2)
    build_weight(br2, rw2, REFINE2_K, 1)
    build_weight(bw3, dw3, DOWN3_K, 2)
    build_weight(br3, rw3, REFINE3_K, 1)

    def halo(e, stage, buf, rows, groups, both):
        sems = (send_sem.at[e], recv_sem.at[e])
        if stage == 0:
            return Halo(stage, buf, rows, groups, both, send_x, recv_x, sems, device)
        if stage == 3:
            return Halo(stage, buf, rows, groups, both, None, None, sems, device)
        return Halo(stage, buf, rows, groups, both, send_c.at[e - 1], recv_c.at[e - 1], sems, device)

    pv_halo = halo(0, 0, pv, rows1, 8, False)
    y1_halo = halo(1, 1, y1, rows1, G, True)
    z1_halo = halo(2, 1, z1, rows1, G, False)
    y2_halo = halo(3, 2, y2, rows2, G, True)
    z2_halo = halo(4, 2, z2, rows2, G, False)
    y3_halo = halo(5, 3, y3, rows3, G, True)

    lane = lax.broadcasted_iota(jnp.int16, (N, 128), 1)

    def to_groups(v):
        v = [roll(t, 16 * i) for i, t in enumerate(v)]
        for k in range(3):
            mask = (lane & (16 << k)) == 0
            v = [jnp.where(mask, v[j], v[(j + (1 << k)) % 8]) for j in range(8)]
        return [roll(v[-q % 8], -16 * q) for q in range(8)]

    def to_pairs(i, carry):
        for u in range(TILES):
            t = jnp.transpose(x[:, pl.ds((i * TILES + u) * 16, 16), :], (1, 0, 2))
            for p in range(2):
                v = to_groups([t[p * 8 + k] for k in range(8)])
                pv[1 + 2 * (i * TILES + u) + p, pl.ds(1, 8)] = jnp.stack(v)
        return carry

    for i, (lo, hi) in enumerate(image_blocks):
        loads[i].wait()
        lax.fori_loop(lo // 2 // TILES, hi // 2 // TILES, to_pairs, 0)
        if i == 1:
            pl.semaphore_wait(barrier, len(others))
        if i % 2:
            pv_halo.send_cols(image_blocks[i - 1][0], hi, 0)
        pv_halo.send_rows(lo, hi)

    bias1 = tiled_bias(db1)

    def down1(lo, hi, q0, nq, per):
        per = divisor(hi - lo, per)
        size = per * nq * N

        def step(i, carry):
            row0 = lo + i * per
            sub = lax.broadcasted_iota(jnp.int16, (size, 128), 1) & 15
            own = flat(pv[pl.ds(row0 + 1, per), pl.ds(1 + q0, nq)])
            above = flat(pv[pl.ds(row0, per), pl.ds(1 + q0, nq)])
            left = flat(pv[pl.ds(row0 + 1, per), pl.ds(q0, nq)])
            above_left = flat(pv[pl.ds(row0, per), pl.ds(q0, nq)])
            edge = jnp.where(sub == 15, left, jnp.where(sub == 14, roll(left, 63), roll(above_left, 62)))
            second = jnp.concatenate([edge[:, :64], above[:, 64:]], axis=1)
            res = jnp.dot(jnp.concatenate([own, second], axis=1), bw1[...], preferred_element_type=F32)
            val = jnp.maximum(res + bias1, 0.0).astype(BF)
            pairs = pl.ds(lo // 2 + i * (per // 2) + 1, per // 2)
            for half in range(2):
                v = val[:, half * 128:(half + 1) * 128].reshape(per // 2, 2, nq, N, 128)
                for q in range(nq):
                    y1[pairs, :, 1 + 2 * (q0 + q) + half] = v[:, :, q]
            return carry

        unrolled((hi - lo) // per, step)

    for is_edge, (lo, hi) in schedule(row_blocks(rows1, 16, 56), 1):
        if is_edge:
            pv_halo.need_cols(lo - 1, hi)
            down1(lo, hi, 0, 1, 32)
            y1_halo.send_cols(lo, hi, 1)
            y1_halo.send_rows(lo, hi)
        else:
            pv_halo.need_rows(lo - 1, hi)
            down1(lo, hi, 1, 7, DOWN1_ROWS)
            y1_halo.send_cols(lo, hi, 0)

    def refine(stage, src, src_halo, weight, bias, dst, dst_halo, blocks, delay):
        lhs = functools.partial(refine_lhs, stage, src)
        for is_edge, (lo, hi) in schedule(blocks, delay):
            if is_edge:
                src_halo.need_cols(lo - 1, hi + 1)
                conv_rows(lhs, weight, bias, dst, lo, hi, [(0, 1), (G - 1, 1)], 16)
                if dst_halo is not None:
                    dst_halo.send_cols(lo, hi, 0)
                    dst_halo.send_rows(lo, hi)
            else:
                src_halo.need_rows(lo - 1, hi + 1)
                conv_rows(lhs, weight, bias, dst, lo, hi, [(1, G - 2)], PAIRS)

    def down(src, src_halo, weight, bias, dst, dst_halo, blocks, delay):
        lhs = functools.partial(down_lhs, src)
        for is_edge, (lo, hi) in schedule(blocks, delay):
            if is_edge:
                src_halo.need_cols(2 * lo - 1, 2 * hi)
                conv_rows(lhs, weight, bias, dst, lo, hi, [(0, 1)], 16)
                dst_halo.send_cols(lo, hi, 1)
                dst_halo.send_rows(lo, hi)
            else:
                src_halo.need_rows(2 * lo - 1, 2 * hi)
                conv_rows(lhs, weight, bias, dst, lo, hi, [(1, G - 1)], PAIRS)
                dst_halo.send_cols(lo, hi, 0)

    refine(1, y1, y1_halo, br1, tiled_bias(rb1), into_quads(z1), z1_halo, row_blocks(rows1, 24, 56), 1)
    down(z1, z1_halo, bw2, tiled_bias(db2), into_pairs(y2, 1), y2_halo, row_blocks(rows2, 16, 24), 1)
    refine(2, y2, y2_halo, br2, tiled_bias(rb2), into_quads(z2), z2_halo, row_blocks(rows2, 24, 24), 1)
    down(z2, z2_halo, bw3, tiled_bias(db3), into_pairs(y3, 1), y3_halo, row_blocks(rows3, 16, 16), 4)
    refine(3, y3, y3_halo, br3, tiled_bias(rb3), into_pairs(out, 0), None,
           [(4, rows3 - 4), (rows3 - 4, rows3), (0, 4)], 3)

    for h in (pv_halo, y1_halo, z1_halo, y2_halo, z2_halo, y3_halo):
        h.finish()


def encode(h_count, w_count, images, *params):
    rows1 = images.shape[1] // 2
    rows2, rows3 = rows1 // 2, rows1 // 4
    x = jnp.transpose(images, (0, 1, 3, 2)).reshape(N, rows1 * 8, 128)
    args = [x, jnp.asarray(first_weight_selector(), BF)]
    for i, p in enumerate(params):
        args.append(p.reshape(1, -1) if i % 2 else (p.reshape(9, 4, 32) if i == 0 else p))

    def act(*shape):
        return pltpu.VMEM(shape + (N, 128), BF)

    flops = 2 * 16 * rows1 * 64 * 32 * 9 * (4 + 32 + 16 + 32 + 16 + 32)
    out = pl.pallas_call(
        functools.partial(kernel, h_count, w_count, rows1),
        name='encoder',
        out_shape=pltpu.VMEM((rows3 // 2, 2, G, N, 128), BF),
        in_specs=[pl.BlockSpec(memory_space=pl.ANY)] + [pl.BlockSpec(memory_space=pltpu.VMEM)] * (len(args) - 1),
        out_specs=pl.BlockSpec(memory_space=pltpu.VMEM),
        scratch_shapes=[
            pltpu.VMEM((N, rows1 * 8 + 16, 128), BF), act(rows1 + 1, 9),
            act(rows1 // 2 + 2, 2, G + 3), act(rows1 // 4 + 1, 4, G + 1),
            act(rows2 // 2 + 2, 2, G + 3), act(rows2 // 4 + 1, 4, G + 1), act(rows3 // 2 + 2, 2, G + 3),
            pltpu.VMEM((36, 32), F32), pltpu.VMEM((256, 256), BF), pltpu.VMEM((768, 256), BF), pltpu.VMEM((1024, 256), BF),
            pltpu.VMEM((1024, 256), BF), pltpu.VMEM((1024, 256), BF), pltpu.VMEM((1536, 256), BF),
            pltpu.VMEM((1, rows1 // 16, N, 128), BF), pltpu.VMEM((1, rows1 // 16, N, 128), BF),
            pltpu.VMEM((4, 2, rows1 // 4, N, 128), BF), pltpu.VMEM((4, 2, rows1 // 4, N, 128), BF),
            pltpu.SemaphoreType.DMA((8,)), pltpu.SemaphoreType.DMA((6, 20)), pltpu.SemaphoreType.DMA((6, 20)),
        ],
        compiler_params=pltpu.CompilerParams(
            collective_id=0, has_side_effects=True, vmem_limit_bytes=56 * 2**20),
        cost_estimate=pl.CostEstimate(flops=flops, bytes_accessed=7 * 2**20, transcendentals=0),
    )(*args)
    return jnp.transpose(out.reshape(rows3, G, N, 128), (2, 0, 1, 3))


def solution(mesh):
    tile_spec = P('batch', 'h', 'w', None)
    body = functools.partial(encode, mesh.shape['h'], mesh.shape['w'])
    return jax.shard_map(body, mesh=mesh, in_specs=(tile_spec,) + (P(),) * 12, out_specs=tile_spec, check_vma=False)
```
